256 devices in a mesh: rep: 16 (over x, y_hi, core), shard: 16 (over z, y_lo).
Axes of the slice: x: 4, y: 4 (y_hi: 2, y_lo: 2; y = y_hi * 2 + y_lo), z: 8, core: 2. Of those that a mesh axis runs over, the one named last changes fastest.
Arguments:
- activations: bfloat16 [6, 32768, 2048], P(None, ('rep', 'shard')), may hold values from -50 to 50
- cotangents: bfloat16 [6, 32768, 512], P(None, ('rep', 'shard')), may hold values from -120 to 120
- momentum: float32 [12, 256, 2048], P(None, None, 'shard'), may hold values from -6 to 6
- owners: int32 [12], replicated, may hold values from 0 to 15, as said below
- bucket_starts: int32 [2], replicated, may hold values from 1 to 11, as said below
Outputs:
- momentum_out: float32 [12, 256, 2048], P(None, None, 'shard')
- update: float32 [12, 256, 2048], P(None, None, 'shard')
- owned: bfloat16 [32, 256, 2048], P('shard')
The draws below stay inside these ranges and needn't reach their ends.
Inputs may be any that keep to these rules, and one draw needn't show every extreme that they name: `owners`: no owner is named more than 2 times, and some owner exactly 2 times. `bucket_starts`: strictly increasing.
All inputs are finite; a program needn't handle non-finite values.
Results may differ from the reference program's by a relative error of at most 0.033.
Values may be sent and summed in bfloat16 or wider, within the bound.
A program may use at most 128 MiB of HBM per device.

```python
import math
import jax
import jax.numpy as jnp
from jax import lax

D = 2048
KV = 256
LAYERS = 6
ITERS = 5
BUCKETS = 3
MATS = 12
SLOTS = 2
TOKENS = 32768
N_SHARD = 16


def bucket_layout(key):
    key_starts = jax.random.fold_in(key, 31)
    chosen = jax.random.permutation(key_starts, MATS - 2)[:BUCKETS - 2] + 1
    last_start = jnp.full((1,), MATS - 1, dtype=jnp.int32)
    return jnp.sort(jnp.concatenate([chosen.astype(jnp.int32), last_start])).astype(jnp.int32)


def draw_activations(key, part):
    key_values = jax.random.fold_in(key, 41)
    shape_full = (LAYERS, TOKENS, D)
    values = jnp.clip(jax.random.normal(key_values, shape_full, jnp.float32), -4.5, 4.5)
    ratio = 6.0
    position = jnp.arange(D, dtype=jnp.float32) / D
    rising = jnp.exp(math.log(ratio) * position)
    mean_energy = (ratio * ratio - 1.0) / (2.0 * math.log(ratio))
    column_scale = rising / math.sqrt(mean_energy)
    return (values * column_scale[None, None, :]).astype(jnp.bfloat16)


def draw_cotangents(key, part):
    key_normal = jax.random.fold_in(key, 11)
    key_quiet_scale = jax.random.fold_in(key, 12)
    key_column = jax.random.fold_in(key, 13)
    key_quiet = jax.random.fold_in(key, 14)
    key_loud_scale = jax.random.fold_in(key, 15)
    shape_full = (LAYERS, TOKENS, 2 * KV)
    normal_part = jnp.clip(jax.random.normal(key_normal, shape_full, jnp.float32), -5.0, 5.0)
    starts = bucket_layout(key)
    indices = jnp.arange(MATS, dtype=jnp.int32)
    buckets = jnp.sum((indices[:, None] >= starts[None, :]).astype(jnp.int32), axis=1)
    quiet_bucket = jax.random.randint(key_quiet, (), 0, BUCKETS, dtype=jnp.int32)
    quiet_log = jax.random.uniform(key_quiet_scale, (MATS,), jnp.float32, math.log(0.03), math.log(0.1))
    loud_log = jax.random.uniform(key_loud_scale, (MATS,), jnp.float32, 0.0, math.log(8.0))
    matrix_scale = jnp.exp(jnp.where(buckets == quiet_bucket, quiet_log, loud_log))
    matrix_scale = jnp.repeat(matrix_scale.reshape(LAYERS, 1, 2), KV, axis=2)
    column_scale = jnp.exp(jax.random.uniform(key_column, (LAYERS, 1, 2 * KV), jnp.float32, 0.0, math.log(3.0)))
    return (normal_part * matrix_scale * column_scale).astype(jnp.bfloat16)


def draw_owners(key, part):
    key_first = jax.random.fold_in(key, 21)
    key_second = jax.random.fold_in(key, 22)
    key_third = jax.random.fold_in(key, 23)
    shuffled = jax.random.permutation(key_first, N_SHARD).astype(jnp.int32)
    filled = jnp.full((SLOTS,), shuffled[0], dtype=jnp.int32)
    others = jax.random.permutation(key_second, jnp.repeat(shuffled[1:], SLOTS))
    candidates = jnp.concatenate([filled, others])[:MATS]
    return jax.random.permutation(key_third, candidates).astype(jnp.int32)


def draw_bucket_starts(key, part):
    return bucket_layout(key)


def block_scale(rng, shape, pieces, smallest, largest):
    level = 1.0
    for axis_at, shards_of in pieces:
        steps = jax.random.uniform(jax.random.fold_in(jax.random.fold_in(rng, 6), axis_at), (shards_of,), jnp.float32, smallest / len(pieces), largest / len(pieces))
        level = level * jnp.repeat(jnp.exp(steps), shape[axis_at] // shards_of).reshape((-1,) + (1,) * (len(shape) - 1 - axis_at))
    return level


def bell_draw(stream_key, extent, deviation, limit, shards=(), kind=jnp.bfloat16):
    drawn = jax.random.normal(stream_key, extent, jnp.float32) * deviation
    if len(shards) > 0:
        drawn = block_scale(stream_key, extent, shards, -0.22, 0.18) * drawn
    return jnp.clip(drawn, min=-limit, max=limit).astype(kind)


def setup_inputs(seed: int = 0) -> dict:
    key_list = jax.random.split(jax.random.key(seed), 6)
    activations = draw_activations(jax.random.fold_in(key_list[5], 71), 0)
    cotangents = draw_cotangents(jax.random.fold_in(key_list[5], 71), 0)
    momentum = bell_draw(key_list[2], (MATS, KV, D), 1.0, 6.0, ((2, 16),), jnp.float32)
    owners = draw_owners(jax.random.fold_in(key_list[5], 71), 0)
    bucket_starts = draw_bucket_starts(jax.random.fold_in(key_list[5], 71), 0)
    return {"activations": activations, "cotangents": cotangents, "momentum": momentum, "owners": owners, "bucket_starts": bucket_starts}


coef_a = 3.4445
coef_b = -4.775
coef_c = 2.0315
momentum_rate = 0.95
clip_level = 0.5
epsilon = 1e-06

def orthogonal(update_in):
    values = update_in.astype(jnp.float32)
    frobenius = jnp.sqrt(jnp.sum(values * values))
    matrix = (values / (frobenius + epsilon)).astype(jnp.bfloat16)
    for iteration in range(ITERS):
        gram_matrix = jnp.dot(matrix, matrix.T, preferred_element_type=jnp.float32).astype(jnp.bfloat16)
        square = jnp.dot(gram_matrix, gram_matrix, preferred_element_type=jnp.float32)
        mixing = (coef_b * gram_matrix.astype(jnp.float32) + coef_c * square).astype(jnp.bfloat16)
        matrix = (coef_a * matrix.astype(jnp.float32) + jnp.dot(mixing, matrix, preferred_element_type=jnp.float32)).astype(jnp.bfloat16)
    return matrix

def clip_factors(square_sums, bucket_starts):
    indices = jnp.arange(MATS, dtype=jnp.int32)
    buckets = lax.optimization_barrier(jnp.sum((indices[:, None] >= bucket_starts[None, :]).astype(jnp.int32), axis=1))
    together = (buckets[:, None] == buckets[None, :]).astype(jnp.float32)
    totals = lax.optimization_barrier(jnp.sum(together * square_sums[None, :], axis=1))
    members = lax.optimization_barrier(jnp.sum(together, axis=1))
    root_mean = jnp.sqrt(totals / (members * KV * D) + epsilon)
    return jnp.minimum(1.0, clip_level / root_mean)

def slot_numbers(owners):
    indices = jnp.arange(MATS, dtype=jnp.int32)
    earlier = (indices[None, :] < indices[:, None]) & (owners[None, :] == owners[:, None])
    return lax.optimization_barrier(jnp.sum(earlier.astype(jnp.int32), axis=1)).astype(jnp.int32)

def reference(activations, cotangents, momentum, owners, bucket_starts):
    layer_grads = []
    for layer_index in range(LAYERS):
        layer_grads.append(lax.dot_general(cotangents[layer_index], activations[layer_index], (((0,), (0,)), ((), ())), preferred_element_type=jnp.float32))
    gradient = jnp.stack(layer_grads).reshape(MATS, KV, D) / jnp.sqrt(jnp.float32(TOKENS))
    square_sums = lax.optimization_barrier(jnp.sum(gradient * gradient, axis=(1, 2)))
    factors = clip_factors(square_sums, bucket_starts)
    momentum_out = momentum_rate * momentum + factors[:, None, None] * gradient
    nesterov = (factors[:, None, None] * gradient + momentum_rate * momentum_out).astype(jnp.bfloat16)
    orthogonalized = lax.map(orthogonal, nesterov)
    update_scale = math.sqrt(max(KV, D))
    update = update_scale * orthogonalized.astype(jnp.float32)
    slot_of = slot_numbers(owners)
    positions = owners * SLOTS + slot_of
    select = (jnp.arange(N_SHARD * SLOTS, dtype=jnp.int32)[:, None] == positions[None, :]).astype(jnp.float32)
    holdings = jnp.einsum('pm,mkd->pkd', select, update).astype(jnp.bfloat16)
    return (momentum_out, update, holdings)
```

```python
import functools
import math

import jax
import jax.numpy as jnp
from jax import lax
from jax.experimental import pallas as pl
from jax.experimental.pallas import tpu as pltpu
from jax.sharding import Mesh
from jax.sharding import PartitionSpec as P

D = 2048
KV = 256
ITERS = 5
MATS = 12
TOKENS = 32768
SHARD = ("shard_0", "shard_1")
REP_SHARD = ("rep_0", "rep_1", "rep_2", "shard_0", "shard_1")

coef_a = 3.4445
coef_b = -4.775
coef_c = 2.0315
momentum_rate = 0.95
clip_level = 0.5
epsilon = 1e-06

f32 = jnp.float32
bf16 = jnp.bfloat16
MESH = pl.DeviceIdType.MESH


def wrap(value, size):
    return lax.rem(value + 2 * size, size)


class Place:
    def __init__(self):
        self.x = lax.axis_index("rep_0")
        self.yh = lax.axis_index("rep_1")
        self.c = lax.axis_index("rep_2")
        self.z = lax.axis_index("shard_0")
        self.yl = lax.axis_index("shard_1")
        self.y = 2 * self.yh + self.yl
        self.block = 2 * self.x + self.yh
        self.column = 2 * self.z + self.yl

    def at(self, dx=0, dz=0):
        return (wrap(self.x + dx, 4), self.yh, self.c, wrap(self.z + dz, 8), self.yl)

    def at_y(self, dy):
        y = wrap(self.y + dy, 4)
        return (self.x, lax.div(y, 2), self.c, self.z, lax.rem(y, 2))

    def partner(self):
        return (self.x, self.yh, 1 - self.c, self.z, self.yl)

    def replicas(self):
        for dx in range(4):
            for dyh in range(2):
                if dx or dyh:
                    yield (wrap(self.x + dx, 4), lax.rem(self.yh + dyh, 2), self.c, self.z, self.yl)

    def columns(self):
        for dz in range(8):
            for dyl in range(2):
                if dz or dyl:
                    z, yl = wrap(self.z + dz, 8), lax.rem(self.yl + dyl, 2)
                    yield (self.x, self.yh, self.c, z, yl), 2 * z + yl


class Wire:
    def __init__(self, send_sems, recv_sems):
        self.send_sems, self.recv_sems = send_sems, recv_sems
        self.started = []

    def send(self, source, target, device):
        k = len(self.started)
        copy = pltpu.make_async_remote_copy(
            src_ref=source,
            dst_ref=target,
            send_sem=self.send_sems.at[k],
            recv_sem=self.recv_sems.at[k],
            device_id=device,
            device_id_type=MESH,
        )
        copy.start()
        self.started.append(copy)
        return copy

    def finish(self):
        for copy in self.started:
            copy.wait_send()


def greet(devices):
    barrier = pltpu.get_barrier_semaphore()
    devices = list(devices)
    for device in devices:
        pl.semaphore_signal(barrier, inc=1, device_id=device, device_id_type=MESH)
    pl.semaphore_wait(barrier, len(devices))


def rows_at(start, size):
    return pl.ds(pl.multiple_of(start, size), size)


Z_STEPS = {(0, 1): 4, (1, -1): 4, (1, 1): 3, (0, -1): 3}
Z_BASE = {(0, 1): 0, (1, -1): 4, (1, 1): 8, (0, -1): 11}
PAIR_BASE = {(0, 1): 0, (1, -1): 2, (1, 1): 4, (0, -1): 5}
PAIR_STEPS = {(0, 1): 2, (1, -1): 2, (1, 1): 1, (0, -1): 1}
REDUCE_SENDS = 6 + 14 + 6 + 6 + 9 + 17 + 7 + 7 + 15 + 2


def reduce_kernel(
    act, cot, g_out, sq_out,
    actv, cotv, cott, zs, zr, xs, xr, ys, yr,
    z2s, z2r, z3s, z3r, x2s, x2r, x3s, x3r, y2s, y2r, y3s, y3r,
    gb, sqs, sq2, sqb, local_sems, send_sems, recv_sems,
):
    me = Place()
    x, y, yh, yl, z, c = me.x, me.y, me.yh, me.yl, me.z, me.c
    wire = Wire(send_sems, recv_sems)
    mine = rows_at(c * 128, 128)

    loads = []
    for j in range(3):
        pair = (
            pltpu.make_async_copy(cot.at[3 * c + j], cotv.at[j, mine], local_sems.at[2 * j]),
            pltpu.make_async_copy(act.at[3 * c + j], actv.at[j, mine], local_sems.at[2 * j + 1]),
        )
        for copy in pair:
            copy.start()
        loads.append(pair)

    devices = [me.partner()]
    devices += [me.at(dx=d) for d in range(1, 4)]
    devices += [me.at_y(d) for d in range(1, 4)]
    devices += [(wrap(x + d, 4), 1 - yh, c, z, yl) for d in range(1, 4)]
    devices += [me.at(dz=d) for d in range(1, 8)]
    devices += [(x, yh, c, wrap(z + d, 8), 1 - yl) for d in range(1, 8)]
    greet(devices)

    swaps = []
    for j in range(3):
        swaps.append(
            (
                wire.send(cot.at[3 * (1 - c) + j], cotv.at[j, mine], me.partner()),
                wire.send(act.at[3 * (1 - c) + j], actv.at[j, mine], me.partner()),
            )
        )

    def prepare(j, inner_is_x):
        loads[j][0].wait()
        swaps[j][0].wait_recv()
        turned = cotv[j].T
        for bx in range(4):
            for by in range(2):
                for kv in range(2):
                    source = kv * 256 + (bx * 2 + by) * 32
                    target = (by * 256 + bx * 64 if inner_is_x else bx * 128 + by * 64) + kv * 32
                    cott[j, target : target + 32, :] = turned[source : source + 32, :]
        loads[j][1].wait()
        swaps[j][1].wait_recv()

    sent = {}

    def z_part(dest, half):
        columns = rows_at(dest * 256 + half * 128, 128)
        return jnp.dot(cott[0], actv[0, :, columns], preferred_element_type=f32)

    def z_send(half, d, n, k):
        part = z_part(wrap(z + d * (n + 1 - k), 8), half)
        slot = Z_BASE[half, d] + k - 1
        if k > 1:
            sent["z", half, d, k - 1].wait_recv()
            part += zr[slot - 1].astype(f32)
        zs[slot] = part.astype(bf16)
        sent["z", half, d, k] = wire.send(zs.at[slot], zr.at[slot], me.at(dz=d))

    def x_part(dest, half, i):
        columns = rows_at((4 * half + i) * 256, 256)
        return jnp.dot(cott[1, rows_at(dest * 128, 128), :], actv[1, :, columns], preferred_element_type=f32)

    def x_send(half, d, k):
        dest = wrap(x + d * (PAIR_STEPS[half, d] + 1 - k), 4)
        slot = PAIR_BASE[half, d] + k - 1
        if k > 1:
            sent["x", half, d, k - 1].wait_recv()

        def step(i, carry):
            part = x_part(dest, half, i)
            for t in range(2):
                value = part[:, t * 128 : (t + 1) * 128]
                if k > 1:
                    value += xr[slot - 1, 2 * i + t].astype(f32)
                xs[slot, 2 * i + t] = value.astype(bf16)
            return carry

        lax.fori_loop(0, 4, step, 0)
        sent["x", half, d, k] = wire.send(xs.at[slot], xr.at[slot], me.at(dx=d))

    def y_part(dest, half, i):
        columns = rows_at(((4 * half + i) * 2 + lax.rem(dest, 2)) * 128, 128)
        rows = rows_at(lax.div(dest, 2) * 256, 256)
        return jnp.dot(cott[2, rows, :], actv[2, :, columns], preferred_element_type=f32)

    def y_send(half, d, k):
        dest = wrap(y + d * (PAIR_STEPS[half, d] + 1 - k), 4)
        slot = PAIR_BASE[half, d] + k - 1
        if k > 1:
            sent["y", half, d, k - 1].wait_recv()

        def step(i, carry):
            value = y_part(dest, half, i)
            if k > 1:
                value += yr[slot - 1, i].astype(f32)
            ys[slot, i] = value.astype(bf16)
            return carry

        lax.fori_loop(0, 4, step, 0)
        sent["y", half, d, k] = wire.send(ys.at[slot], yr.at[slot], me.at_y(d))

    def z_round(k):
        for (half, d), n in Z_STEPS.items():
            if k <= n:
                z_send(half, d, n, k)

    prepare(0, False)
    z_round(1)
    prepare(1, False)
    x_send(0, 1, 1)
    x_send(1, -1, 1)
    prepare(2, True)
    y_send(0, 1, 1)
    y_send(1, -1, 1)
    x_send(1, 1, 1)
    x_send(0, -1, 1)
    y_send(1, 1, 1)
    y_send(0, -1, 1)
    z_round(2)
    x_send(0, 1, 2)
    x_send(1, -1, 2)
    y_send(0, 1, 2)
    y_send(1, -1, 2)
    z_round(3)
    z_round(4)

    for half in range(2):
        sent["x", half, 1, PAIR_STEPS[half, 1]].wait_recv()
        sent["x", half, -1, PAIR_STEPS[half, -1]].wait_recv()
        up = PAIR_BASE[half, 1] + PAIR_STEPS[half, 1] - 1
        down = PAIR_BASE[half, -1] + PAIR_STEPS[half, -1] - 1

        def x_last(i, carry, half=half, up=up, down=down):
            part = x_part(x, half, i)
            for t in range(2):
                value = part[:, t * 128 : (t + 1) * 128]
                value += xr[up, 2 * i + t].astype(f32) + xr[down, 2 * i + t].astype(f32)
                x2s[t, 4 * half + i] = value.astype(bf16)
            return carry

        lax.fori_loop(0, 4, x_last, 0)
    for d in (1, 3, 2):
        to = wrap(y + d, 4)
        sent["x2", d] = wire.send(
            x2s.at[lax.rem(to, 2), :, rows_at(lax.div(to, 2) * 64, 64), :], x2r.at[d - 1], me.at_y(d)
        )

    for half in range(2):
        sent["y", half, 1, PAIR_STEPS[half, 1]].wait_recv()
        sent["y", half, -1, PAIR_STEPS[half, -1]].wait_recv()
        up = PAIR_BASE[half, 1] + PAIR_STEPS[half, 1] - 1
        down = PAIR_BASE[half, -1] + PAIR_STEPS[half, -1] - 1

        def y_last(i, carry, half=half, up=up, down=down):
            value = y_part(y, half, i) + yr[up, i].astype(f32) + yr[down, i].astype(f32)
            y2s[4 * half + i] = value.astype(bf16)
            return carry

        lax.fori_loop(0, 4, y_last, 0)
    for d in (1, 3, 2):
        to = wrap(x + d, 4)
        sent["y2", d] = wire.send(y2s.at[:, rows_at(to * 64, 64), :], y2r.at[d - 1], me.at(dx=d))

    for half in range(2):
        last = []
        for d in (1, -1):
            n = Z_STEPS[half, d]
            sent["z", half, d, n].wait_recv()
            last.append(Z_BASE[half, d] + n - 1)
        value = z_part(z, half) + zr[last[0]].astype(f32) + zr[last[1]].astype(f32)
        z2s[half] = value.astype(bf16)
    for d in (1, 3, 2):
        to = wrap(x + d, 4)
        sent["z2", d] = wire.send(z2s.at[:, rows_at(to * 128, 128), :], z2r.at[d - 1], me.at(dx=d))

    for d in range(1, 4):
        sent["x2", d].wait_recv()

    def x_third(i, carry):
        value = x2s[yl, i, rows_at(yh * 64, 64), :].astype(f32)
        for d in range(3):
            value += x2r[d, i].astype(f32)
        x3s[i] = value.astype(bf16)
        return carry

    lax.fori_loop(0, 8, x_third, 0)
    for d in (4, 3, 5, 2, 6, 1, 7):
        sent["x3", d] = wire.send(x3s.at[wrap(z + d, 8)], x3r.at[d - 1], me.at(dz=d))

    for d in range(1, 4):
        sent["y2", d].wait_recv()

    def y_third(i, carry):
        value = y2s[i, rows_at(x * 64, 64), :].astype(f32)
        for d in range(3):
            value += y2r[d, i].astype(f32)
        y3s[i] = value.astype(bf16)
        return carry

    lax.fori_loop(0, 8, y_third, 0)
    for d in (4, 3, 5, 2, 6, 1, 7):
        sent["y3", d] = wire.send(y3s.at[wrap(z + d, 8)], y3r.at[d - 1], me.at(dz=d))

    for d in range(1, 4):
        sent["z2", d].wait_recv()
    for t in range(2):
        value = z2s[t, rows_at(x * 128, 128), :].astype(f32)
        for d in range(3):
            value += z2r[d, t].astype(f32)
        z3s[t] = value.astype(bf16)
    for d in (2, 1, 3):
        to = wrap(y + d, 4)
        sent["z3", d] = wire.send(
            z3s.at[lax.rem(to, 2), rows_at(lax.div(to, 2) * 64, 64), :], z3r.at[d - 1], me.at_y(d)
        )

    rows = rows_at(me.block * 32, 32)
    inverse = 1.0 / math.sqrt(TOKENS)
    sqs[me.block] = jnp.zeros((8, 128), f32)

    def piece(j, value):
        value = value * inverse
        for kv in range(2):
            block = value[kv * 32 : (kv + 1) * 32]
            gb[6 * c + 2 * j + kv, rows, :] = block.astype(bf16)
            total = jnp.sum(block * block, axis=(0, 1), keepdims=True)
            sqs[me.block, 2 * j + kv : 2 * j + kv + 1, :] = jnp.broadcast_to(total, (1, 128))

    for d in range(1, 8):
        sent["x3", d].wait_recv()
    value = x3s[z].astype(f32)
    for d in range(7):
        value += x3r[d].astype(f32)
    piece(1, value)
    for d in range(1, 8):
        sent["y3", d].wait_recv()
    value = y3s[z].astype(f32)
    for d in range(7):
        value += y3r[d].astype(f32)
    piece(2, value)
    for d in range(1, 4):
        sent["z3", d].wait_recv()
    value = z3s[yl, rows_at(yh * 64, 64), :].astype(f32)
    for d in range(3):
        value += z3r[d].astype(f32)
    piece(0, value)

    own = pl.ds(6 * c, 6)
    squares = [wire.send(sqs.at[me.block], sqs.at[me.block], device) for device in me.replicas()]
    pieces = [wire.send(gb.at[own, rows, :], gb.at[own, rows, :], device) for device in me.replicas()]
    for copy in squares:
        copy.wait_recv()
    sq2[me.column] = sum((sqs[i] for i in range(1, 8)), sqs[0])
    squares = [wire.send(sq2.at[me.column], sq2.at[me.column], device) for device, _ in me.columns()]
    for copy in pieces:
        copy.wait_recv()
    over = wire.send(gb.at[own], gb.at[own], me.partner())
    for copy in squares:
        copy.wait_recv()
    sqb[c] = sum((sq2[i] for i in range(1, 16)), sq2[0])
    other = wire.send(sqb.at[c], sqb.at[c], me.partner())
    over.wait_recv()
    store = pltpu.make_async_copy(gb, g_out, local_sems.at[6])
    store.start()
    other.wait_recv()
    sq_out[...] = sqb[...]
    store.wait()
    wire.finish()


def reduced(act, cot):
    vm = pltpu.VMEM
    return pl.pallas_call(
        reduce_kernel,
        out_shape=(
            jax.ShapeDtypeStruct((MATS, KV, 128), bf16),
            jax.ShapeDtypeStruct((2, 8, 128), f32),
        ),
        in_specs=[pl.BlockSpec(memory_space=pl.ANY)] * 2,
        out_specs=(pl.BlockSpec(memory_space=pl.ANY), pl.BlockSpec(memory_space=pltpu.VMEM)),
        scratch_shapes=[
            vm((3, 256, D), bf16), vm((3, 256, 512), bf16), vm((3, 512, 256), bf16),
            vm((14, 512, 128), bf16), vm((14, 512, 128), bf16),
            vm((6, 8, 128, 128), bf16), vm((6, 8, 128, 128), bf16),
            vm((6, 4, 256, 128), bf16), vm((6, 4, 256, 128), bf16),
            vm((2, 512, 128), bf16), vm((3, 2, 128, 128), bf16), vm((2, 128, 128), bf16), vm((3, 64, 128), bf16),
            vm((2, 8, 128, 128), bf16), vm((3, 8, 64, 128), bf16), vm((8, 64, 128), bf16), vm((7, 64, 128), bf16),
            vm((8, 256, 128), bf16), vm((3, 8, 64, 128), bf16), vm((8, 64, 128), bf16), vm((7, 64, 128), bf16),
            vm((MATS, KV, 128), bf16), vm((8, 8, 128), f32), vm((16, 8, 128), f32), vm((2, 8, 128), f32),
            pltpu.SemaphoreType.DMA((7,)),
            pltpu.SemaphoreType.DMA((REDUCE_SENDS,)),
            pltpu.SemaphoreType.DMA((REDUCE_SENDS,)),
        ],
        compiler_params=pltpu.CompilerParams(
            collective_id=0, has_side_effects=True, vmem_limit_bytes=60 * 1024 * 1024
        ),
        name="reduce",
    )(act, cot)


def orthogonalize(xin, xw):
    def squares(i, total):
        value = xin[rows_at(i * 16, 16), :].astype(f32)
        return total + value * value

    total = lax.fori_loop(0, 16, squares, jnp.zeros((16, D), f32))
    norm = jnp.sqrt(jnp.sum(total, axis=(0, 1), keepdims=True))
    scale = 1.0 / (norm + epsilon)

    def start(i, carry):
        xw[rows_at(i * 16, 16), :] = (xin[rows_at(i * 16, 16), :].astype(f32) * scale).astype(bf16)
        return carry

    lax.fori_loop(0, 16, start, 0)

    def iteration(i, carry):
        gram = lax.dot_general(xw[...], xw[...], (((1,), (1,)), ((), ())), preferred_element_type=f32).astype(bf16)
        square = jnp.dot(gram, gram, preferred_element_type=f32)
        mixing = (coef_b * gram.astype(f32) + coef_c * square).astype(bf16)
        for k in range(4):
            cols = slice(k * 512, (k + 1) * 512)
            old = xw[:, cols]
            product = jnp.dot(mixing, old, preferred_element_type=f32)
            xw[:, cols] = (coef_a * old.astype(f32) + product).astype(bf16)
        return carry

    lax.fori_loop(0, ITERS, iteration, 0)


OWNER_SENDS = 15 + 7 + 1 + 15 + 1 + 7 + 1


def owner_kernel(
    owners, u, upd_out, o_out, ub, xin, xw, rb, ob, us, local_sems, send_sems, recv_sems
):
    me = Place()
    c = me.c
    wire = Wire(send_sems, recv_sems)
    load = pltpu.make_async_copy(u, ub, local_sems.at[0])
    load.start()
    devices = [me.partner()] + list(me.replicas()) + [device for device, _ in me.columns()]
    greet(devices)
    load.wait()
    rows = rows_at(me.block * 32, 32)

    def choose(p, carry):
        found, seen = jnp.int32(0), jnp.int32(0)
        filled = jnp.int32(0)
        for m in range(MATS):
            held = (owners[m] == p).astype(jnp.int32)
            take = held * (seen == c).astype(jnp.int32)
            found = found + take * m
            filled = filled + take
            seen = seen + held
        block = ub[found, rows, :].astype(f32) * filled.astype(f32)
        us[p] = block.astype(bf16)
        return carry

    lax.fori_loop(0, 16, choose, 0)
    here = rows_at(me.column * 128, 128)
    copies = [wire.send(us.at[p], xin.at[rows, here], device) for device, p in me.columns()]
    xin[rows, here] = us[me.column]
    for copy in copies:
        copy.wait_recv()
    copies = [wire.send(xin.at[rows, :], xin.at[rows, :], device) for device in me.replicas()]
    for copy in copies:
        copy.wait_recv()

    orthogonalize(xin, xw)

    copies = [
        wire.send(xw.at[rows, rows_at(p * 128, 128)], rb.at[c, me.column], device)
        for device, p in me.columns()
    ]
    rb[c, me.column] = xw[rows, here]
    whole = wire.send(xw, o_out.at[c], me.partner())
    store = pltpu.make_async_copy(xw, o_out.at[c], local_sems.at[1])
    store.start()
    for copy in copies:
        copy.wait_recv()
    over = wire.send(rb.at[c], rb.at[c], me.partner())
    over.wait_recv()
    for k in range(6):
        m = 6 * c + k
        owner = owners[m]
        slot = jnp.int32(0)
        for j in range(MATS):
            slot = slot + (owners[j] == owner).astype(jnp.int32) * (j < m).astype(jnp.int32)
        ob[m, rows, :] = rb[jnp.minimum(slot, 1), owner]
    own = pl.ds(6 * c, 6)
    copies = [wire.send(ob.at[own, rows, :], ob.at[own, rows, :], device) for device in me.replicas()]
    for copy in copies:
        copy.wait_recv()
    over = wire.send(ob.at[own], ob.at[own], me.partner())
    over.wait_recv()
    out = pltpu.make_async_copy(ob, upd_out, local_sems.at[2])
    out.start()
    whole.wait_recv()
    store.wait()
    out.wait()
    wire.finish()


def orthogonal_pieces(u, owners):
    vm = pltpu.VMEM
    return pl.pallas_call(
        owner_kernel,
        out_shape=(
            jax.ShapeDtypeStruct((MATS, KV, 128), bf16),
            jax.ShapeDtypeStruct((2, KV, D), bf16),
        ),
        in_specs=[pl.BlockSpec(memory_space=pltpu.SMEM), pl.BlockSpec(memory_space=pl.ANY)],
        out_specs=(pl.BlockSpec(memory_space=pl.ANY), pl.BlockSpec(memory_space=pl.ANY)),
        scratch_shapes=[
            vm((MATS, KV, 128), bf16), vm((KV, D), bf16), vm((KV, D), bf16), vm((2, 16, 32, 128), bf16),
            vm((MATS, KV, 128), bf16), vm((16, 32, 128), bf16),
            pltpu.SemaphoreType.DMA((3,)),
            pltpu.SemaphoreType.DMA((OWNER_SENDS,)),
            pltpu.SemaphoreType.DMA((OWNER_SENDS,)),
        ],
        compiler_params=pltpu.CompilerParams(
            collective_id=1, has_side_effects=True, vmem_limit_bytes=60 * 1024 * 1024
        ),
        name="owner",
    )(owners, u)


def clip_factors(square_sums, bucket_starts):
    indices = jnp.arange(MATS, dtype=jnp.int32)
    buckets = jnp.sum((indices[:, None] >= bucket_starts[None, :]).astype(jnp.int32), axis=1)
    together = (buckets[:, None] == buckets[None, :]).astype(f32)
    totals = jnp.sum(together * square_sums[None, :], axis=1)
    members = jnp.sum(together, axis=1)
    root_mean = jnp.sqrt(totals / (members * KV * D) + epsilon)
    return jnp.minimum(1.0, clip_level / root_mean)


def per_device(activations, cotangents, momentum, owners, bucket_starts):
    update_scale = math.sqrt(max(KV, D))
    gradient, squares = reduced(activations, cotangents)
    gradient = gradient.astype(f32)
    factors = clip_factors(squares[:, :6, 0].reshape(MATS), bucket_starts)
    momentum_out = momentum_rate * momentum + factors[:, None, None] * gradient
    nesterov = (factors[:, None, None] * gradient + momentum_rate * momentum_out).astype(bf16)
    returned, whole = orthogonal_pieces(nesterov, owners)
    update = update_scale * returned.astype(f32)
    owned = (update_scale * whole.astype(f32)).astype(bf16)
    return (momentum_out, update, owned)


def solution(mesh):
    torus = Mesh(
        mesh.devices.reshape(4, 2, 2, 8, 2), ("rep_0", "rep_1", "rep_2", "shard_0", "shard_1")
    )
    return jax.shard_map(
        per_device,
        mesh=torus,
        in_specs=(
            P(None, REP_SHARD, None),
            P(None, REP_SHARD, None),
            P(None, None, SHARD),
            P(),
            P(),
        ),
        out_specs=(P(None, None, SHARD), P(None, None, SHARD), P(SHARD, None, None)),
        check_vma=False,
    )
```

```python
import functools
import math

import jax
import jax.numpy as jnp
from jax import lax
from jax.experimental import pallas as pl
from jax.experimental.pallas import tpu as pltpu
from jax.sharding import Mesh
from jax.sharding import PartitionSpec as P

D = 2048
KV = 256
ITERS = 5
MATS = 12
TOKENS = 32768
SHARD = ("shard_0", "shard_1")
REP_SHARD = ("rep_0", "rep_1", "rep_2", "shard_0", "shard_1")

coef_a = 3.4445
coef_b = -4.775
coef_c = 2.0315
momentum_rate = 0.95
clip_level = 0.5
epsilon = 1e-06

f32 = jnp.float32
bf16 = jnp.bfloat16
MESH = pl.DeviceIdType.MESH


def wrap(value, size):
    return lax.rem(value + 2 * size, size)


class Place:
    def __init__(self):
        self.x = lax.axis_index("rep_0")
        self.yh = lax.axis_index("rep_1")
        self.c = lax.axis_index("rep_2")
        self.z = lax.axis_index("shard_0")
        self.yl = lax.axis_index("shard_1")
        self.y = 2 * self.yh + self.yl
        self.block = 2 * self.x + self.yh
        self.column = 2 * self.z + self.yl

    def at(self, dx=0, dz=0):
        return (wrap(self.x + dx, 4), self.yh, self.c, wrap(self.z + dz, 8), self.yl)

    def at_y(self, dy):
        y = wrap(self.y + dy, 4)
        return (self.x, lax.div(y, 2), self.c, self.z, lax.rem(y, 2))

    def partner(self):
        return (self.x, self.yh, 1 - self.c, self.z, self.yl)

    def replicas(self):
        for dx in range(4):
            for dyh in range(2):
                if dx or dyh:
                    yield (wrap(self.x + dx, 4), lax.rem(self.yh + dyh, 2), self.c, self.z, self.yl)

    def columns_at(self, dz):
        for dyl in range(2):
            if dz or dyl:
                z, yl = wrap(self.z + dz, 8), lax.rem(self.yl + dyl, 2)
                yield (self.x, self.yh, self.c, z, yl), 2 * z + yl

    def columns(self):
        for dz in (4, 3, 5, 2, 6, 1, 7, 0):
            yield from self.columns_at(dz)


class Wire:
    def __init__(self, send_sems, recv_sems, device):
        self.send_sems, self.recv_sems, self.device = send_sems, recv_sems, device
        self.n_send = self.n_recv = 0
        self.leaving, self.kept, self.numbers = [], [], {}

    def copy(self, source, target, s, r, device):
        return pltpu.make_async_remote_copy(
            src_ref=source,
            dst_ref=target,
            send_sem=self.send_sems.at[s],
            recv_sem=self.recv_sems.at[r],
            device_id=device,
            device_id_type=MESH,
        )

    def outlet(self, whole):
        self.n_send += 1
        self.leaving.append((self.n_send - 1, whole))
        return self.n_send - 1

    def send(self, source, target, device, s=None):
        if s is None:
            s = self.outlet(source)
        r = self.n_recv
        self.n_recv += 1
        copy = self.copy(source, target, s, r, device)
        copy.start()
        return copy

    def opened(self, whole):
        s, r = self.outlet(whole), self.n_recv
        self.n_recv += 1
        copy = self.copy(whole, whole, s, r, self.device)
        self.kept.append(copy)
        self.numbers[id(copy)] = (s, r)
        return copy

    def join(self, group, copies):
        for source, target, device in copies:
            self.copy(source, target, *self.numbers[id(group)], device).start()

    def group(self, copies, whole):
        group = self.opened(whole)
        self.join(group, copies)
        return group

    def finish(self):
        assert (self.n_send, self.n_recv) == (OUTLETS, ARRIVALS), (self.n_send, self.n_recv)
        for s, whole in self.leaving:
            self.copy(whole, whole, s, 0, self.device).wait_send()


def signal_all(devices):
    barrier = pltpu.get_barrier_semaphore()
    for device in devices:
        pl.semaphore_signal(barrier, inc=1, device_id=device, device_id_type=MESH)


class Phases:
    def __init__(self):
        self.open = None

    def __call__(self, name):
        self.end()
        self.open = jax.named_scope(name)
        self.open.__enter__()

    def end(self):
        if self.open:
            self.open.__exit__(None, None, None)
        self.open = None


def rows_at(start, size):
    return pl.ds(pl.multiple_of(start, size), size)


Z_STEPS = {(0, 1): 4, (1, -1): 4, (1, 1): 3, (0, -1): 3}
Z_BASE = {(0, 1): 0, (1, -1): 4, (1, 1): 8, (0, -1): 11}
PAIR_BASE = {(0, 1): 0, (1, -1): 2, (1, 1): 4, (0, -1): 5}
PAIR_STEPS = {(0, 1): 2, (1, -1): 2, (1, 1): 1, (0, -1): 1}
OUTLETS, ARRIVALS = 24, 51


def step_kernel(
    owners_in, starts_in, act, cot, mom, g_out, f_out, upd_out, o_out,
    cin, cout, aout, actv, cott, zs, zr, xs, xr, ys, yr,
    z2s, z2r, z3s, z3r, x2s, x2r, x3s, x3r, y2s, y2r, y3s, y3r,
    gb, gp, sqs, sq2, mb, us, ms, fac, gq, mq, gin, xw, rb, ob, gram, owners, starts, table, local_sems, send_sems, recv_sems,
):
    me = Place()
    x, y, yh, yl, z, c = me.x, me.y, me.yh, me.yl, me.z, me.c
    wire = Wire(send_sems, recv_sems, me.partner())
    phase = Phases()
    mine = rows_at(c * 128, 128)

    load_cot = pltpu.make_async_copy(cot, cin, local_sems.at[0])
    load_cot.start()
    loads, loads_out = [], []
    for j in range(3):
        loads_out.append(pltpu.make_async_copy(act.at[3 * (1 - c) + j], aout.at[j], local_sems.at[1 + j]))
        loads.append(pltpu.make_async_copy(act.at[3 * c + j], actv.at[j, mine], local_sems.at[4 + j]))
        loads_out[j].start()
        loads[j].start()
    rows = rows_at(me.block * 32, 32)
    load_momentum = pltpu.make_async_copy(mom.at[:, rows, :], mb, local_sems.at[12])
    load_momentum.start()
    load_owners = pltpu.make_async_copy(owners_in, owners, local_sems.at[10])
    load_starts = pltpu.make_async_copy(starts_in, starts, local_sems.at[11])
    load_owners.start()
    load_starts.start()

    phase("r_greet")
    devices = [me.partner()]
    devices += [me.at(dx=d) for d in range(1, 4)]
    devices += [me.at_y(d) for d in range(1, 4)]
    devices += [(wrap(x + d, 4), 1 - yh, c, z, yl) for d in range(1, 4)]
    devices += [(dx, dy, 1 - c, dz, dl) for dx, dy, _, dz, dl in me.replicas()]
    devices += [me.at(dz=d) for d in range(1, 8)]
    devices += [(x, yh, c, wrap(z + d, 8), 1 - yl) for d in range(1, 8)]
    signal_all(devices)

    def turn(source, store, inner_is_x):
        turned = source.T
        for bx in range(4):
            for by in range(2):
                for kv in range(2):
                    at = kv * 256 + (bx * 2 + by) * 32
                    to = (by * 256 + bx * 64 if inner_is_x else bx * 128 + by * 64) + kv * 32
                    store(to, turned[at : at + 32, :])

    load_cot.wait()
    for j in range(3):

        def store_out(to, value, j=j):
            cout[j, to : to + 32, :] = value

        def store_own(to, value, j=j):
            cott[j, to : to + 32, mine] = value

        turn(cin[3 * (1 - c) + j], store_out, j == 2)
        turn(cin[3 * c + j], store_own, j == 2)

    phase("r_greetw")
    pl.semaphore_wait(pltpu.get_barrier_semaphore(), len(devices))
    phase("r_swap")
    out_cot, out_act = wire.outlet(cout), wire.outlet(aout)
    out_x, out_y, out_z = wire.outlet(xs), wire.outlet(ys), wire.outlet(zs)
    swaps = []
    for j in range(3):
        loads_out[j].wait()
        swaps.append(
            (
                wire.send(cout.at[j], cott.at[j, :, mine], me.partner(), out_cot),
                wire.send(aout.at[j], actv.at[j, mine], me.partner(), out_act),
            )
        )

    def prepare(j):
        loads[j].wait()
        swaps[j][0].wait_recv()
        swaps[j][1].wait_recv()

    sent = {}

    def z_part(dest, half):
        columns = rows_at(dest * 256 + half * 128, 128)
        return jnp.dot(cott[0], actv[0, :, columns], preferred_element_type=f32)

    def z_send(half, d, n, k):
        part = z_part(wrap(z + d * (n + 1 - k), 8), half)
        slot = Z_BASE[half, d] + k - 1
        if k > 1:
            sent["z", half, d, k - 1].wait_recv()
            part += zr[slot - 1].astype(f32)
        zs[slot] = part.astype(bf16)
        sent["z", half, d, k] = wire.send(zs.at[slot], zr.at[slot], me.at(dz=d), out_z)

    def x_part(dest, half, i):
        columns = rows_at((4 * half + i) * 256, 256)
        return jnp.dot(cott[1, rows_at(dest * 128, 128), :], actv[1, :, columns], preferred_element_type=f32)

    def x_send(half, d, k):
        dest = wrap(x + d * (PAIR_STEPS[half, d] + 1 - k), 4)
        slot = PAIR_BASE[half, d] + k - 1
        if k > 1:
            sent["x", half, d, k - 1].wait_recv()

        def step(i, carry):
            part = x_part(dest, half, i)
            for t in range(2):
                value = part[:, t * 128 : (t + 1) * 128]
                if k > 1:
                    value += xr[slot - 1, 2 * i + t].astype(f32)
                xs[slot, 2 * i + t] = value.astype(bf16)
            return carry

        lax.fori_loop(0, 4, step, 0, unroll=True)
        sent["x", half, d, k] = wire.send(xs.at[slot], xr.at[slot], me.at(dx=d), out_x)

    def y_part(dest, half, i):
        columns = rows_at(((4 * half + i) * 2 + lax.rem(dest, 2)) * 128, 128)
        rows = rows_at(lax.div(dest, 2) * 256, 256)
        return jnp.dot(cott[2, rows, :], actv[2, :, columns], preferred_element_type=f32)

    def y_send(half, d, k):
        dest = wrap(y + d * (PAIR_STEPS[half, d] + 1 - k), 4)
        slot = PAIR_BASE[half, d] + k - 1
        if k > 1:
            sent["y", half, d, k - 1].wait_recv()

        def step(i, carry):
            value = y_part(dest, half, i)
            if k > 1:
                value += yr[slot - 1, i].astype(f32)
            ys[slot, i] = value.astype(bf16)
            return carry

        lax.fori_loop(0, 4, step, 0, unroll=True)
        sent["y", half, d, k] = wire.send(ys.at[slot], yr.at[slot], me.at_y(d), out_y)

    def z_round(k):
        for (half, d), n in Z_STEPS.items():
            if k <= n:
                z_send(half, d, n, k)

    phase("r_prep0")
    prepare(0)
    phase("r_z1")
    z_round(1)
    phase("r_x1")
    prepare(1)
    x_send(0, 1, 1)
    x_send(1, -1, 1)
    phase("r_y1")
    prepare(2)
    y_send(0, 1, 1)
    y_send(1, -1, 1)
    phase("r_xy1b")
    x_send(1, 1, 1)
    x_send(0, -1, 1)
    y_send(1, 1, 1)
    y_send(0, -1, 1)
    phase("r_z2")
    z_round(2)
    phase("r_x2")
    x_send(0, 1, 2)
    x_send(1, -1, 2)
    phase("r_y2")
    y_send(0, 1, 2)
    y_send(1, -1, 2)
    phase("r_z3")
    z_round(3)
    phase("r_z4")
    z_round(4)

    here = rows_at(me.column * 128, 128)

    def slot_matrix(p):
        found, seen, filled = jnp.int32(0), jnp.int32(0), jnp.int32(0)
        for m in range(MATS):
            named = (owners[m] == p).astype(jnp.int32)
            take = named * (seen == c).astype(jnp.int32)
            found, filled, seen = found + take * m, filled + take, seen + named
        return found, filled

    def note(p, carry):
        table[0, p], table[1, p] = slot_matrix(p)
        return carry

    def gather_columns(pieces, target):
        def choose(p, carry):
            found, filled = table[0, p], table[1, p]
            target[p] = (pieces[found].astype(f32) * filled.astype(f32)).astype(bf16)
            return carry

        lax.fori_loop(0, 16, choose, 0, unroll=2)

    phase("r_msend")
    load_momentum.wait()
    load_owners.wait()
    load_starts.wait()
    lax.fori_loop(0, 16, note, 0)
    gather_columns(mb, ms)
    mq[:, here] = ms[me.column]

    phase("r_xlast")
    for half in range(2):
        sent["x", half, 1, PAIR_STEPS[half, 1]].wait_recv()
        sent["x", half, -1, PAIR_STEPS[half, -1]].wait_recv()
        up = PAIR_BASE[half, 1] + PAIR_STEPS[half, 1] - 1
        down = PAIR_BASE[half, -1] + PAIR_STEPS[half, -1] - 1

        def x_last(i, carry, half=half, up=up, down=down):
            part = x_part(x, half, i)
            for t in range(2):
                value = part[:, t * 128 : (t + 1) * 128]
                value += xr[up, 2 * i + t].astype(f32) + xr[down, 2 * i + t].astype(f32)
                x2s[t, 4 * half + i] = value.astype(bf16)
            return carry

        lax.fori_loop(0, 4, x_last, 0, unroll=True)
    copies = []
    for d in (1, 3, 2):
        to = wrap(y + d, 4)
        source = x2s.at[lax.rem(to, 2), :, rows_at(lax.div(to, 2) * 64, 64), :]
        copies.append((source, x2r.at[d - 1], me.at_y(d)))
    sent["x2"] = wire.group(copies, x2r)

    phase("r_ylast")
    for half in range(2):
        sent["y", half, 1, PAIR_STEPS[half, 1]].wait_recv()
        sent["y", half, -1, PAIR_STEPS[half, -1]].wait_recv()
        up = PAIR_BASE[half, 1] + PAIR_STEPS[half, 1] - 1
        down = PAIR_BASE[half, -1] + PAIR_STEPS[half, -1] - 1

        def y_last(i, carry, half=half, up=up, down=down):
            value = y_part(y, half, i) + yr[up, i].astype(f32) + yr[down, i].astype(f32)
            y2s[4 * half + i] = value.astype(bf16)
            return carry

        lax.fori_loop(0, 4, y_last, 0, unroll=True)
    copies = []
    for d in (1, 3, 2):
        to = wrap(x + d, 4)
        copies.append((y2s.at[:, rows_at(to * 64, 64), :], y2r.at[d - 1], me.at(dx=d)))
    sent["y2"] = wire.group(copies, y2r)

    phase("r_zlast")
    for half in range(2):
        last = []
        for d in (1, -1):
            n = Z_STEPS[half, d]
            sent["z", half, d, n].wait_recv()
            last.append(Z_BASE[half, d] + n - 1)
        value = z_part(z, half) + zr[last[0]].astype(f32) + zr[last[1]].astype(f32)
        z2s[half] = value.astype(bf16)
    copies = []
    for d in (1, 3, 2):
        to = wrap(x + d, 4)
        copies.append((z2s.at[:, rows_at(to * 128, 128), :], z2r.at[d - 1], me.at(dx=d)))
    sent["z2"] = wire.group(copies, z2r)
    copies = [(ms.at[p], mq.at[:, here], device) for device, p in me.columns()]
    momentum_to_owner = wire.group(copies, ms.at[:15])

    phase("r_x3")
    sent["x2"].wait_recv()

    def x_third(i, carry):
        value = x2s[yl, i, rows_at(yh * 64, 64), :].astype(f32)
        for d in range(3):
            value += x2r[d, i].astype(f32)
        x3s[i] = value.astype(bf16)
        return carry

    lax.fori_loop(0, 8, x_third, 0, unroll=True)
    copies = [(x3s.at[wrap(z + d, 8)], x3r.at[d - 1], me.at(dz=d)) for d in (4, 3, 5, 2, 6, 1, 7)]
    sent["x3"] = wire.group(copies, x3r)

    phase("r_y3")
    sent["y2"].wait_recv()

    def y_third(i, carry):
        value = y2s[i, rows_at(x * 64, 64), :].astype(f32)
        for d in range(3):
            value += y2r[d, i].astype(f32)
        y3s[i] = value.astype(bf16)
        return carry

    lax.fori_loop(0, 8, y_third, 0, unroll=True)
    copies = [(y3s.at[wrap(z + d, 8)], y3r.at[d - 1], me.at(dz=d)) for d in (4, 3, 5, 2, 6, 1, 7)]
    sent["y3"] = wire.group(copies, y3r)

    phase("r_z3b")
    sent["z2"].wait_recv()
    for t in range(2):
        value = z2s[t, rows_at(x * 128, 128), :].astype(f32)
        for d in range(3):
            value += z2r[d, t].astype(f32)
        z3s[t] = value.astype(bf16)
    copies = []
    for d in (2, 1, 3):
        to = wrap(y + d, 4)
        source = z3s.at[lax.rem(to, 2), rows_at(lax.div(to, 2) * 64, 64), :]
        copies.append((source, z3r.at[d - 1], me.at_y(d)))
    sent["z3"] = wire.group(copies, z3r)

    phase("r_xfin")
    inverse = 1.0 / math.sqrt(TOKENS)
    sqs[c, me.block] = jnp.zeros((8, 128), f32)

    def piece(j, value):
        value = value * inverse
        for kv in range(2):
            block = value[kv * 32 : (kv + 1) * 32]
            gb[6 * c + 2 * j + kv, rows, :] = block.astype(bf16)
            gp[6 * c + 2 * j + kv] = block.astype(bf16)
            total = jnp.sum(block * block, axis=(0, 1), keepdims=True)
            sqs[c, me.block, 2 * j + kv : 2 * j + kv + 1, :] = jnp.broadcast_to(total, (1, 128))

    sent["x3"].wait_recv()
    value = x3s[z].astype(f32)
    for d in range(7):
        value += x3r[d].astype(f32)
    piece(1, value)
    phase("r_yfin")
    sent["y3"].wait_recv()
    value = y3s[z].astype(f32)
    for d in range(7):
        value += y3r[d].astype(f32)
    piece(2, value)
    phase("r_zfin")
    sent["z3"].wait_recv()
    value = z3s[yl, rows_at(yh * 64, 64), :].astype(f32)
    for d in range(3):
        value += z3r[d].astype(f32)
    piece(0, value)

    phase("r_sqsend")
    own = pl.ds(6 * c, 6)
    swap = wire.send(gp.at[own], gp.at[own], me.partner())
    copies = [(sqs.at[c, me.block], sqs.at[c, me.block], me.partner())]
    for dx, dy, core, dz, dl in me.replicas():
        copies.append((sqs.at[c, me.block], sqs.at[c, me.block], (dx, dy, core, dz, dl)))
        copies.append((sqs.at[c, me.block], sqs.at[c, me.block], (dx, dy, 1 - core, dz, dl)))
    squares = wire.group(copies, sq2.at[:15, :8])
    swap.wait_recv()
    gather_columns(gp, us)
    gq[:, here] = us[me.column]
    to_owner = wire.group([(us.at[p], gq.at[:, here], device) for device, p in me.columns()], us.at[:15])
    phase("r_sqw1b")
    squares.wait_recv()
    for core in range(2):
        sq2[me.column, core * 8 : core * 8 + 8] = sum((sqs[core, i] for i in range(1, 8)), sqs[core, 0])
    squares = wire.group(
        [(sq2.at[me.column], sq2.at[me.column], device) for device, _ in me.columns()], sq2.at[:15]
    )
    phase("o_a2a")
    momentum_to_owner.wait_recv()
    to_owner.wait_recv()
    phase("r_sqw2")
    squares.wait_recv()
    totals = sum((sq2[i] for i in range(1, 16)), sq2[0])
    phase("o_choose")

    row = lax.broadcasted_iota(jnp.int32, (16, 128), 0)
    matrix = jnp.where(row >= 8, row - 2, row)
    held = (row < 6) | ((row >= 8) & (row < 14))
    bucket = (matrix >= starts[0]).astype(jnp.int32) + (matrix >= starts[1]).astype(jnp.int32)
    factors = jnp.ones((16, 128), f32)
    for b in range(3):
        inside = held & (bucket == b)
        total = jnp.sum(jnp.where(inside, totals, 0.0), axis=0, keepdims=True)
        members = jnp.sum(inside.astype(f32), axis=0, keepdims=True)
        root_mean = jnp.sqrt(total / (members * (KV * D)) + epsilon)
        factors = jnp.where(inside, jnp.minimum(1.0, clip_level / root_mean), factors)
    f_out[...] = factors
    fac[...] = factors
    mine_is = table[0, me.column]
    factor = fac[pl.ds(mine_is + 2 * (mine_is >= 6).astype(jnp.int32), 1), :]
    for k in range(4):
        cols = slice(k * 512, (k + 1) * 512)
        scaled = factor[:, :1] * gq[:, cols].astype(f32)
        value = scaled + momentum_rate * (momentum_rate * mq[:, cols].astype(f32) + scaled)
        gin[rows, cols] = value.astype(bf16)
    gathered_u = wire.group([(gin.at[rows, :], gin.at[rows, :], device) for device in me.replicas()], gin.at[:224])
    phase("o_ag")
    gathered_u.wait_recv()
    pieces = wire.group(
        [(gb.at[own, rows, :], gb.at[own, rows, :], device) for device in me.replicas()], gb.at[:6, :224, :]
    )

    phase("o_ns")
    orthogonalize(gin, xw, gram)

    phase("o_back")
    copies = [
        (xw.at[rows, rows_at(p * 128, 128)], rb.at[c, me.column], device) for device, p in me.columns()
    ]
    back = wire.group(copies, rb.at[0, :15])
    rb[c, me.column] = xw[rows, here]
    pieces.wait_recv()
    over_g = wire.send(gb.at[own], gb.at[own], me.partner())
    whole = wire.send(xw, o_out.at[c], me.partner())
    store = pltpu.make_async_copy(xw, o_out.at[c], local_sems.at[7])
    store.start()
    back.wait_recv()
    phase("o_over")
    over = wire.send(rb.at[c], rb.at[c], me.partner())
    over.wait_recv()
    for k in range(6):
        m = 6 * c + k
        owner = owners[m]
        slot = jnp.int32(0)
        for j in range(MATS):
            slot = slot + (owners[j] == owner).astype(jnp.int32) * (j < m).astype(jnp.int32)
        ob[m, rows, :] = rb[jnp.minimum(slot, 1), owner]
    phase("o_ag2")
    gathered = wire.group(
        [(ob.at[own, rows, :], ob.at[own, rows, :], device) for device in me.replicas()], ob.at[:6, :224, :]
    )
    over_g.wait_recv()
    store_g = pltpu.make_async_copy(gb, g_out, local_sems.at[8])
    store_g.start()
    gathered.wait_recv()
    phase("o_over2")
    over = wire.send(ob.at[own], ob.at[own], me.partner())
    over.wait_recv()
    out = pltpu.make_async_copy(ob, upd_out, local_sems.at[9])
    out.start()
    phase("o_finish")
    whole.wait_recv()
    store.wait()
    store_g.wait()
    out.wait()
    wire.finish()
    phase.end()


def orthogonalize(xin, xw, gram):
    def squares(i, total):
        value = xin[rows_at(i * 16, 16), :].astype(f32)
        return total + value * value

    total = lax.fori_loop(0, 16, squares, jnp.zeros((16, D), f32))
    norm = jnp.sqrt(jnp.sum(total, axis=(0, 1), keepdims=True))
    scale = 1.0 / (norm + epsilon)

    def start(i, carry):
        block = rows_at(i * 16, 16)
        xw[block, :] = (xin[block, :].astype(f32) * scale).astype(bf16)
        return carry

    lax.fori_loop(0, 16, start, 0)

    def outer(value):
        return lax.dot_general(value, value, (((1,), (1,)), ((), ())), preferred_element_type=f32)

    gram[...] = outer(xw[...])

    def iteration(i, carry):
        rounded = gram[...].astype(bf16)
        square = jnp.dot(rounded, rounded, preferred_element_type=f32)
        mixing = (coef_b * rounded.astype(f32) + coef_c * square).astype(bf16)
        total = None
        for k in range(4):
            cols = slice(k * 512, (k + 1) * 512)
            old = xw[:, cols]
            product = jnp.dot(mixing, old, preferred_element_type=f32)
            new = (coef_a * old.astype(f32) + product).astype(bf16)
            xw[:, cols] = new
            total = outer(new) if k == 0 else total + outer(new)
        gram[...] = total
        return carry

    lax.fori_loop(0, ITERS, iteration, 0)


def stepped(activations, cotangents, momentum, owners, bucket_starts):
    vm = pltpu.VMEM
    operands = (owners, bucket_starts, activations, cotangents, momentum)
    operands = [pltpu.with_memory_space_constraint(a, pltpu.HBM) for a in operands]
    return pl.pallas_call(
        step_kernel,
        out_shape=(
            jax.ShapeDtypeStruct((MATS, KV, 128), bf16),
            jax.ShapeDtypeStruct((16, 128), f32),
            jax.ShapeDtypeStruct((MATS, KV, 128), bf16),
            jax.ShapeDtypeStruct((2, KV, D), bf16),
        ),
        in_specs=[pl.BlockSpec(memory_space=pltpu.HBM)] * 5,
        out_specs=(
            pl.BlockSpec(memory_space=pl.ANY),
            pl.BlockSpec(memory_space=pltpu.VMEM),
            pl.BlockSpec(memory_space=pl.ANY),
            pl.BlockSpec(memory_space=pl.ANY),
        ),
        scratch_shapes=[
            vm((6, 128, 512), bf16), vm((3, 512, 128), bf16), vm((3, 128, D), bf16), vm((3, 256, D), bf16), vm((3, 512, 256), bf16),
            vm((14, 512, 128), bf16), vm((14, 512, 128), bf16),
            vm((6, 8, 128, 128), bf16), vm((6, 8, 128, 128), bf16),
            vm((6, 4, 256, 128), bf16), vm((6, 4, 256, 128), bf16),
            vm((2, 512, 128), bf16), vm((3, 2, 128, 128), bf16), vm((2, 128, 128), bf16), vm((3, 64, 128), bf16),
            vm((2, 8, 128, 128), bf16), vm((3, 8, 64, 128), bf16), vm((8, 64, 128), bf16), vm((7, 64, 128), bf16),
            vm((8, 256, 128), bf16), vm((3, 8, 64, 128), bf16), vm((8, 64, 128), bf16), vm((7, 64, 128), bf16),
            vm((MATS, KV, 128), bf16), vm((MATS, 32, 128), bf16), vm((2, 8, 8, 128), f32), vm((16, 16, 128), f32),
            vm((MATS, 32, 128), f32), vm((16, 32, 128), bf16), vm((16, 32, 128), bf16), vm((16, 128), f32),
            vm((32, D), bf16), vm((32, D), bf16), vm((KV, D), bf16), vm((KV, D), bf16), vm((2, 16, 32, 128), bf16), vm((MATS, KV, 128), bf16),
            vm((KV, KV), f32),
            pltpu.SMEM((MATS,), jnp.int32), pltpu.SMEM((2,), jnp.int32), pltpu.SMEM((2, 16), jnp.int32),
            pltpu.SemaphoreType.DMA((13,)),
            pltpu.SemaphoreType.DMA((OUTLETS,)),
            pltpu.SemaphoreType.DMA((ARRIVALS,)),
        ],
        compiler_params=pltpu.CompilerParams(
            collective_id=0, has_side_effects=True, vmem_limit_bytes=48 * 1024 * 1024
        ),
        name="step",
    )(*operands)


def finish_kernel(factors, g, mom, x, whole, mom_out, update, owned):
    i = pl.program_id(0)
    scale = math.sqrt(max(KV, D))
    for k in range(3):
        m = 3 * i + k
        factor = factors[pl.ds(m + 2 * (m >= 6).astype(jnp.int32), 1), :]
        mom_out[k] = momentum_rate * mom[k] + factor * g[k].astype(f32)
    update[...] = scale * x[...].astype(f32)
    owned[...] = (scale * whole[...].astype(f32)).astype(bf16)


def finished(factors, g, mom, x, whole):
    part = pl.BlockSpec((3, KV, 128), lambda i: (i, 0, 0))
    rows = pl.BlockSpec((2, KV // 4, D), lambda i: (0, i, 0))
    return pl.pallas_call(
        finish_kernel,
        grid=(4,),
        out_shape=(
            jax.ShapeDtypeStruct((MATS, KV, 128), f32),
            jax.ShapeDtypeStruct((MATS, KV, 128), f32),
            jax.ShapeDtypeStruct((2, KV, D), bf16),
        ),
        in_specs=[pl.BlockSpec((16, 128), lambda i: (0, 0)), part, part, part, rows],
        out_specs=(part, part, rows),
        compiler_params=pltpu.CompilerParams(vmem_limit_bytes=16 * 1024 * 1024),
        name="finish",
    )(factors, g, mom, x, whole)


def per_device(activations, cotangents, momentum, owners, bucket_starts):
    g, factors, x, whole = stepped(activations, cotangents, momentum, owners, bucket_starts)
    return finished(factors, g, momentum, x, whole)


def solution(mesh):
    torus = Mesh(
        mesh.devices.reshape(4, 2, 2, 8, 2), ("rep_0", "rep_1", "rep_2", "shard_0", "shard_1")
    )
    return jax.shard_map(
        per_device,
        mesh=torus,
        in_specs=(
            P(None, REP_SHARD, None),
            P(None, REP_SHARD, None),
            P(None, None, SHARD),
            P(),
            P(),
        ),
        out_specs=(P(None, None, SHARD), P(None, None, SHARD), P(SHARD, None, None)),
        check_vma=False,
    )
```

```python
import functools
import math

import jax
import jax.numpy as jnp
from jax import lax
from jax.experimental import pallas as pl
from jax.experimental.pallas import tpu as pltpu
from jax.sharding import Mesh
from jax.sharding import PartitionSpec as P

D = 2048
KV = 256
ITERS = 5
MATS = 12
TOKENS = 32768
SHARD = ("shard_0", "shard_1")
REP_SHARD = ("rep_0", "rep_1", "rep_2", "shard_0", "shard_1")

coef_a = 3.4445
coef_b = -4.775
coef_c = 2.0315
momentum_rate = 0.95
clip_level = 0.5
epsilon = 1e-06

f32 = jnp.float32
bf16 = jnp.bfloat16
MESH = pl.DeviceIdType.MESH


def wrap(value, size):
    return lax.rem(value + 2 * size, size)


class Place:
    def __init__(self):
        self.x = lax.axis_index("rep_0")
        self.yh = lax.axis_index("rep_1")
        self.c = lax.axis_index("rep_2")
        self.z = lax.axis_index("shard_0")
        self.yl = lax.axis_index("shard_1")
        self.y = 2 * self.yh + self.yl
        self.block = 2 * self.x + self.yh
        self.column = 2 * self.z + self.yl

    def at(self, dx=0, dz=0):
        return (wrap(self.x + dx, 4), self.yh, self.c, wrap(self.z + dz, 8), self.yl)

    def at_y(self, dy):
        y = wrap(self.y + dy, 4)
        return (self.x, lax.div(y, 2), self.c, self.z, lax.rem(y, 2))

    def partner(self):
        return (self.x, self.yh, 1 - self.c, self.z, self.yl)

    def near(self, dx, dy, dc, dz):
        y = wrap(self.y + dy, 4)
        core = 1 - self.c if dc else self.c
        return (wrap(self.x + dx, 4), lax.div(y, 2), core, wrap(self.z + dz, 8), lax.rem(y, 2))

    def replicas(self):
        for dx in range(4):
            for dyh in range(2):
                if dx or dyh:
                    yield (wrap(self.x + dx, 4), lax.rem(self.yh + dyh, 2), self.c, self.z, self.yl)

    def columns_at(self, dz):
        for dyl in range(2):
            if dz or dyl:
                z, yl = wrap(self.z + dz, 8), lax.rem(self.yl + dyl, 2)
                yield (self.x, self.yh, self.c, z, yl), 2 * z + yl

    def columns(self):
        for dz in (4, 3, 5, 2, 6, 1, 7, 0):
            yield from self.columns_at(dz)


class Wire:
    def __init__(self, send_sems, recv_sems, device):
        self.send_sems, self.recv_sems, self.device = send_sems, recv_sems, device
        self.n_send = self.n_recv = 0
        self.leaving, self.kept, self.numbers = [], [], {}

    def copy(self, source, target, s, r, device):
        return pltpu.make_async_remote_copy(
            src_ref=source,
            dst_ref=target,
            send_sem=self.send_sems.at[s],
            recv_sem=self.recv_sems.at[r],
            device_id=device,
            device_id_type=MESH,
        )

    def outlet(self, whole):
        self.n_send += 1
        self.leaving.append((self.n_send - 1, whole))
        return self.n_send - 1

    def send(self, source, target, device, s=None):
        if s is None:
            s = self.outlet(source)
        r = self.n_recv
        self.n_recv += 1
        copy = self.copy(source, target, s, r, device)
        copy.start()
        return copy

    def opened(self, whole):
        s, r = self.outlet(whole), self.n_recv
        self.n_recv += 1
        copy = self.copy(whole, whole, s, r, self.device)
        self.kept.append(copy)
        self.numbers[id(copy)] = (s, r)
        return copy

    def join(self, group, copies):
        for source, target, device in copies:
            self.copy(source, target, *self.numbers[id(group)], device).start()

    def group(self, copies, whole):
        group = self.opened(whole)
        self.join(group, copies)
        return group

    def finish(self):
        assert (self.n_send, self.n_recv) == (OUTLETS, ARRIVALS), (self.n_send, self.n_recv)
        for s, whole in self.leaving:
            self.copy(whole, whole, s, 0, self.device).wait_send()


def signal_all(devices):
    barrier = pltpu.get_barrier_semaphore()
    for device in devices:
        pl.semaphore_signal(barrier, inc=1, device_id=device, device_id_type=MESH)


class Phases:
    def __init__(self):
        self.open = None

    def __call__(self, name):
        self.end()
        self.open = jax.named_scope(name)
        self.open.__enter__()

    def end(self):
        if self.open:
            self.open.__exit__(None, None, None)
        self.open = None


def rows_at(start, size):
    return pl.ds(pl.multiple_of(start, size), size)


Z_STEPS = {(0, 1): 4, (1, -1): 4, (1, 1): 3, (0, -1): 3}
Z_BASE = {(0, 1): 0, (1, -1): 4, (1, 1): 8, (0, -1): 11}
PAIR_BASE = {(0, 1): 0, (1, -1): 2, (1, 1): 4, (0, -1): 5}
PAIR_STEPS = {(0, 1): 2, (1, -1): 2, (1, 1): 1, (0, -1): 1}
OUTLETS, ARRIVALS = 29, 56


def step_kernel(
    owners_in, starts_in, act, cot, mom, g_out, f_out, upd_out, o_out,
    cin, cout, aout, actv, cott, zs, zr, xs, xr, ys, yr,
    z2s, z2r, z3s, z3r, x2s, x2r, x3s, x3r, y2s, y2r, y3s, y3r,
    gb, gp, sqs, sq2, mb, us, ms, fac, gq, mq, gin, xw, rb, ob, gram, owners, starts, table, local_sems, send_sems, recv_sems,
):
    me = Place()
    x, y, yh, yl, z, c = me.x, me.y, me.yh, me.yl, me.z, me.c
    wire = Wire(send_sems, recv_sems, me.partner())
    phase = Phases()
    mine = rows_at(c * 128, 128)

    load_cot = pltpu.make_async_copy(cot, cin, local_sems.at[0])
    load_cot.start()
    loads, loads_out = [], []
    for j in range(3):
        loads_out.append(pltpu.make_async_copy(act.at[3 * (1 - c) + j], aout.at[j], local_sems.at[1 + j]))
        loads.append(pltpu.make_async_copy(act.at[3 * c + j], actv.at[j, mine], local_sems.at[4 + j]))
        loads_out[j].start()
        loads[j].start()
    rows = rows_at(me.block * 32, 32)
    load_momentum = pltpu.make_async_copy(mom.at[:, rows_at(x * 64, 64), :], mb, local_sems.at[12])
    load_momentum.start()
    load_owners = pltpu.make_async_copy(owners_in, owners, local_sems.at[10])
    load_starts = pltpu.make_async_copy(starts_in, starts, local_sems.at[11])
    load_owners.start()
    load_starts.start()

    phase("r_greet")
    plane = [(dx, dy, dc) for dx in range(4) for dy in range(4) for dc in range(2) if dx or dy or dc]
    devices = [me.near(dx, dy, dc, 0) for dx, dy, dc in plane]
    devices += [me.near(0, dy, 0, dz) for dy in range(4) for dz in range(1, 8)]
    signal_all(devices)

    def turn(source, store, inner_is_x):
        turned = source.T
        for bx in range(4):
            for by in range(2):
                for kv in range(2):
                    at = kv * 256 + (bx * 2 + by) * 32
                    to = (by * 256 + bx * 64 if inner_is_x else bx * 128 + by * 64) + kv * 32
                    store(to, turned[at : at + 32, :])

    load_cot.wait()
    for j in (1, 2, 0):

        def store_out(to, value, j=j):
            cout[j, to : to + 32, :] = value

        def store_own(to, value, j=j):
            cott[j, to : to + 32, mine] = value

        turn(cin[3 * (1 - c) + j], store_out, j == 2)
        turn(cin[3 * c + j], store_own, j == 2)

    phase("r_greetw")
    pl.semaphore_wait(pltpu.get_barrier_semaphore(), len(devices))
    phase("r_swap")
    out_cot, out_act = wire.outlet(cout), wire.outlet(aout)
    out_x, out_y, out_z = wire.outlet(xs), wire.outlet(ys), wire.outlet(zs)
    swaps = {}
    for j in (1, 2, 0):
        loads_out[j].wait()
        swaps[j] = (
            wire.send(cout.at[j], cott.at[j, :, mine], me.partner(), out_cot),
            wire.send(aout.at[j], actv.at[j, mine], me.partner(), out_act),
        )

    def prepare(j):
        loads[j].wait()
        swaps[j][0].wait_recv()
        swaps[j][1].wait_recv()

    sent = {}

    def z_part(dest, half):
        columns = rows_at(dest * 256 + half * 128, 128)
        return jnp.dot(cott[0], actv[0, :, columns], preferred_element_type=f32)

    def z_send(half, d, n, k):
        part = z_part(wrap(z + d * (n + 1 - k), 8), half)
        slot = Z_BASE[half, d] + k - 1
        if k > 1:
            sent["z", half, d, k - 1].wait_recv()
            part += zr[slot - 1].astype(f32)
        zs[slot] = part.astype(bf16)
        sent["z", half, d, k] = wire.send(zs.at[slot], zr.at[slot], me.at(dz=d), out_z)

    def x_part(dest, half, i):
        columns = rows_at((4 * half + i) * 256, 256)
        return jnp.dot(cott[1, rows_at(dest * 128, 128), :], actv[1, :, columns], preferred_element_type=f32)

    def x_send(half, d, k):
        dest = wrap(x + d * (PAIR_STEPS[half, d] + 1 - k), 4)
        slot = PAIR_BASE[half, d] + k - 1
        if k > 1:
            sent["x", half, d, k - 1].wait_recv()

        def step(i, carry):
            part = x_part(dest, half, i)
            for t in range(2):
                value = part[:, t * 128 : (t + 1) * 128]
                if k > 1:
                    value += xr[slot - 1, 2 * i + t].astype(f32)
                xs[slot, 2 * i + t] = value.astype(bf16)
            return carry

        lax.fori_loop(0, 4, step, 0, unroll=True)
        sent["x", half, d, k] = wire.send(xs.at[slot], xr.at[slot], me.at(dx=d), out_x)

    def y_part(dest, half, i):
        columns = rows_at(((4 * half + i) * 2 + lax.rem(dest, 2)) * 128, 128)
        rows = rows_at(lax.div(dest, 2) * 256, 256)
        return jnp.dot(cott[2, rows, :], actv[2, :, columns], preferred_element_type=f32)

    def y_send(half, d, k):
        dest = wrap(y + d * (PAIR_STEPS[half, d] + 1 - k), 4)
        slot = PAIR_BASE[half, d] + k - 1
        if k > 1:
            sent["y", half, d, k - 1].wait_recv()

        def step(i, carry):
            value = y_part(dest, half, i)
            if k > 1:
                value += yr[slot - 1, i].astype(f32)
            ys[slot, i] = value.astype(bf16)
            return carry

        lax.fori_loop(0, 4, step, 0, unroll=True)
        sent["y", half, d, k] = wire.send(ys.at[slot], yr.at[slot], me.at_y(d), out_y)

    def z_round(k):
        for (half, d), n in Z_STEPS.items():
            if k <= n:
                z_send(half, d, n, k)

    phase("r_prep0")
    prepare(1)
    phase("r_x1")
    x_send(0, 1, 1)
    x_send(1, -1, 1)
    phase("r_y1")
    prepare(2)
    y_send(0, 1, 1)
    y_send(1, -1, 1)
    phase("r_z1")
    prepare(0)
    z_round(1)
    phase("r_xy1b")
    x_send(1, 1, 1)
    x_send(0, -1, 1)
    y_send(1, 1, 1)
    y_send(0, -1, 1)
    phase("r_z2")
    z_round(2)
    phase("r_x2")
    x_send(0, 1, 2)
    x_send(1, -1, 2)
    phase("r_y2")
    y_send(0, 1, 2)
    y_send(1, -1, 2)
    phase("r_z3")
    z_round(3)
    phase("r_z4")
    z_round(4)

    here = rows_at(me.column * 128, 128)

    def slot_matrix(p):
        found, seen, filled = jnp.int32(0), jnp.int32(0), jnp.int32(0)
        for m in range(MATS):
            named = (owners[m] == p).astype(jnp.int32)
            take = named * (seen == c).astype(jnp.int32)
            found, filled, seen = found + take * m, filled + take, seen + named
        return found, filled

    def note(p, carry):
        table[0, p], table[1, p] = slot_matrix(p)
        return carry

    def gather_columns(pieces, target):
        def choose(p, carry):
            found, filled = table[0, p], table[1, p]
            target[p] = (pieces[found].astype(f32) * filled.astype(f32)).astype(bf16)
            return carry

        lax.fori_loop(0, 16, choose, 0, unroll=2)

    phase("r_msend")
    load_momentum.wait()
    load_owners.wait()
    load_starts.wait()
    lax.fori_loop(0, 16, note, 0)
    gather_columns(mb, ms)
    mq[:, here] = ms[me.column]

    phase("r_xlast")
    for half in range(2):
        sent["x", half, 1, PAIR_STEPS[half, 1]].wait_recv()
        sent["x", half, -1, PAIR_STEPS[half, -1]].wait_recv()
        up = PAIR_BASE[half, 1] + PAIR_STEPS[half, 1] - 1
        down = PAIR_BASE[half, -1] + PAIR_STEPS[half, -1] - 1

        def x_last(i, carry, half=half, up=up, down=down):
            part = x_part(x, half, i)
            for t in range(2):
                value = part[:, t * 128 : (t + 1) * 128]
                value += xr[up, 2 * i + t].astype(f32) + xr[down, 2 * i + t].astype(f32)
                x2s[t, 4 * half + i] = value.astype(bf16)
            return carry

        lax.fori_loop(0, 4, x_last, 0, unroll=True)
    copies = []
    for d in (1, 3, 2):
        to = wrap(y + d, 4)
        source = x2s.at[lax.rem(to, 2), :, rows_at(lax.div(to, 2) * 64, 64), :]
        copies.append((source, x2r.at[d - 1], me.at_y(d)))
    sent["x2"] = wire.group(copies, x2r)

    phase("r_ylast")
    for half in range(2):
        sent["y", half, 1, PAIR_STEPS[half, 1]].wait_recv()
        sent["y", half, -1, PAIR_STEPS[half, -1]].wait_recv()
        up = PAIR_BASE[half, 1] + PAIR_STEPS[half, 1] - 1
        down = PAIR_BASE[half, -1] + PAIR_STEPS[half, -1] - 1

        def y_last(i, carry, half=half, up=up, down=down):
            value = y_part(y, half, i) + yr[up, i].astype(f32) + yr[down, i].astype(f32)
            y2s[4 * half + i] = value.astype(bf16)
            return carry

        lax.fori_loop(0, 4, y_last, 0, unroll=True)
    copies = []
    for d in (1, 3, 2):
        to = wrap(x + d, 4)
        copies.append((y2s.at[:, rows_at(to * 64, 64), :], y2r.at[d - 1], me.at(dx=d)))
    sent["y2"] = wire.group(copies, y2r)

    phase("r_zlast")
    for half in range(2):
        last = []
        for d in (1, -1):
            n = Z_STEPS[half, d]
            sent["z", half, d, n].wait_recv()
            last.append(Z_BASE[half, d] + n - 1)
        value = z_part(z, half) + zr[last[0]].astype(f32) + zr[last[1]].astype(f32)
        z2s[half] = value.astype(bf16)
    copies = []
    for d in (1, 3, 2):
        to = wrap(x + d, 4)
        copies.append((z2s.at[:, rows_at(to * 128, 128), :], z2r.at[d - 1], me.at(dx=d)))
    sent["z2"] = wire.group(copies, z2r)
    copies = [(ms.at[p], mq.at[:, here], device) for device, p in me.columns()]
    momentum_to_owner = wire.group(copies, ms.at[:15])

    phase("r_x3")
    sent["x2"].wait_recv()

    def x_third(i, carry):
        value = x2s[yl, i, rows_at(yh * 64, 64), :].astype(f32)
        for d in range(3):
            value += x2r[d, i].astype(f32)
        x3s[i] = value.astype(bf16)
        return carry

    lax.fori_loop(0, 8, x_third, 0, unroll=True)
    copies = [(x3s.at[wrap(z + d, 8)], x3r.at[d - 1], me.at(dz=d)) for d in (4, 3, 5, 2, 6, 1, 7)]
    sent["x3"] = wire.group(copies, x3r)

    phase("r_y3")
    sent["y2"].wait_recv()

    def y_third(i, carry):
        value = y2s[i, rows_at(x * 64, 64), :].astype(f32)
        for d in range(3):
            value += y2r[d, i].astype(f32)
        y3s[i] = value.astype(bf16)
        return carry

    lax.fori_loop(0, 8, y_third, 0, unroll=True)
    copies = [(y3s.at[wrap(z + d, 8)], y3r.at[d - 1], me.at(dz=d)) for d in (4, 3, 5, 2, 6, 1, 7)]
    sent["y3"] = wire.group(copies, y3r)

    phase("r_z3b")
    sent["z2"].wait_recv()
    for t in range(2):
        value = z2s[t, rows_at(x * 128, 128), :].astype(f32)
        for d in range(3):
            value += z2r[d, t].astype(f32)
        z3s[t] = value.astype(bf16)
    copies = []
    for d in (2, 1, 3):
        to = wrap(y + d, 4)
        source = z3s.at[lax.rem(to, 2), rows_at(lax.div(to, 2) * 64, 64), :]
        copies.append((source, z3r.at[d - 1], me.at_y(d)))
    sent["z3"] = wire.group(copies, z3r)

    phase("r_xfin")
    inverse = 1.0 / math.sqrt(TOKENS)
    sqs[z] = jnp.zeros((8, 128), f32)

    def piece(j, value):
        value = value * inverse
        for kv in range(2):
            block = value[kv * 32 : (kv + 1) * 32]
            gb[6 * c + 2 * j + kv, rows, :] = block.astype(bf16)
            gp[6 * c + 2 * j + kv] = block.astype(bf16)
            total = jnp.sum(block * block, axis=(0, 1), keepdims=True)
            sqs[z, 2 * j + kv : 2 * j + kv + 1, :] = jnp.broadcast_to(total, (1, 128))

    sent["x3"].wait_recv()
    value = x3s[z].astype(f32)
    for d in range(7):
        value += x3r[d].astype(f32)
    piece(1, value)
    phase("r_yfin")
    sent["y3"].wait_recv()
    value = y3s[z].astype(f32)
    for d in range(7):
        value += y3r[d].astype(f32)
    piece(2, value)
    phase("r_zfin")
    sent["z3"].wait_recv()
    value = z3s[yl, rows_at(yh * 64, 64), :].astype(f32)
    for d in range(3):
        value += z3r[d].astype(f32)
    piece(0, value)

    phase("r_sqsend")
    own = pl.ds(6 * c, 6)
    squares = wire.group([(sqs.at[z], sqs.at[z], me.at(dz=d)) for d in (4, 3, 5, 2, 6, 1, 7)], sqs.at[:7])
    swap = wire.send(gp.at[own], gp.at[own], me.partner())
    swap.wait_recv()
    gather_columns(gp, us)
    half = rows_at(yh * 32, 32)
    gq[half, here] = us[me.column]
    copies = []
    for dz in (4, 3, 5, 2, 6, 1, 7, 0):
        for dy in (2, 1, 3, 0):
            if dz or dy:
                device = me.near(0, dy, 0, dz)
                copies.append((us.at[2 * device[3] + device[4]], gq.at[half, here], device))
    to_owner = wire.group(copies, rb.at[:31])
    phase("r_sqw1b")
    squares.wait_recv()
    spot = c * 16 + 4 * x + y
    sq2[spot] = sum((sqs[i] for i in range(1, 8)), sqs[0])
    squares = wire.group(
        [(sq2.at[spot], sq2.at[spot], me.near(dx, dy, dc, 0)) for dx, dy, dc in plane], sq2.at[:31]
    )
    phase("r_sqw2")
    squares.wait_recv()
    totals = [sum((sq2[k * 16 + i] for i in range(1, 16)), sq2[k * 16]) for k in range(2)]
    totals = jnp.concatenate(totals, axis=0)
    phase("o_a2a")
    momentum_to_owner.wait_recv()
    to_owner.wait_recv()
    phase("o_choose")

    row = lax.broadcasted_iota(jnp.int32, (16, 128), 0)
    matrix = jnp.where(row >= 8, row - 2, row)
    held = (row < 6) | ((row >= 8) & (row < 14))
    bucket = (matrix >= starts[0]).astype(jnp.int32) + (matrix >= starts[1]).astype(jnp.int32)
    factors = jnp.ones((16, 128), f32)
    for b in range(3):
        inside = held & (bucket == b)
        total = jnp.sum(jnp.where(inside, totals, 0.0), axis=0, keepdims=True)
        members = jnp.sum(inside.astype(f32), axis=0, keepdims=True)
        root_mean = jnp.sqrt(total / (members * (KV * D)) + epsilon)
        factors = jnp.where(inside, jnp.minimum(1.0, clip_level / root_mean), factors)
    f_out[...] = factors
    fac[...] = factors
    mine_is = table[0, me.column]
    factor = fac[pl.ds(mine_is + 2 * (mine_is >= 6).astype(jnp.int32), 1), :]
    for k in range(4):
        cols = slice(k * 512, (k + 1) * 512)
        scaled = factor[:, :1] * gq[:, cols].astype(f32)
        value = scaled + momentum_rate * (momentum_rate * mq[:, cols].astype(f32) + scaled)
        gin[rows_at(x * 64, 64), cols] = value.astype(bf16)

    phase("o_ag")

    def part(dx, h):
        return gin.at[rows_at(wrap(x + dx, 4) * 64 + 32 * h, 32), :]

    ahead, behind = me.at(dx=1), me.at(dx=-1)
    first_up = wire.send(part(0, 0), part(0, 0), ahead)
    first_down = wire.send(part(0, 1), part(0, 1), behind)
    second_up = wire.send(part(0, 1), part(0, 1), ahead)
    second_down = wire.send(part(0, 0), part(0, 0), behind)
    first_up.wait_recv()
    third_up = wire.send(part(-1, 0), part(-1, 0), ahead)
    first_down.wait_recv()
    third_down = wire.send(part(1, 1), part(1, 1), behind)
    for copy in (second_up, second_down, third_up, third_down):
        copy.wait_recv()
    pieces = wire.group(
        [(gb.at[own, rows, :], gb.at[own, rows, :], device) for device in me.replicas()], gb.at[:6, :224, :]
    )

    phase("o_ns")
    orthogonalize(gin, xw, gram)

    phase("o_back")
    copies = [
        (xw.at[rows, rows_at(p * 128, 128)], rb.at[c * 16 + me.column], device) for device, p in me.columns()
    ]
    back = wire.group(copies, rb.at[:15])
    rb[c * 16 + me.column] = xw[rows, here]
    pieces.wait_recv()
    over_g = wire.send(gb.at[own], gb.at[own], me.partner())
    whole = wire.send(xw, o_out.at[c], me.partner())
    store = pltpu.make_async_copy(xw, o_out.at[c], local_sems.at[7])
    store.start()
    back.wait_recv()
    phase("o_over")
    slots = pl.ds(c * 16, 16)
    over = wire.send(rb.at[slots], rb.at[slots], me.partner())
    over.wait_recv()
    for k in range(6):
        m = 6 * c + k
        owner = owners[m]
        slot = jnp.int32(0)
        for j in range(MATS):
            slot = slot + (owners[j] == owner).astype(jnp.int32) * (j < m).astype(jnp.int32)
        ob[m, rows, :] = rb[jnp.minimum(slot, 1) * 16 + owner]
    phase("o_ag2")
    gathered = wire.group(
        [(ob.at[own, rows, :], ob.at[own, rows, :], device) for device in me.replicas()], ob.at[:6, :224, :]
    )
    over_g.wait_recv()
    store_g = pltpu.make_async_copy(gb, g_out, local_sems.at[8])
    store_g.start()
    gathered.wait_recv()
    phase("o_over2")
    over = wire.send(ob.at[own], ob.at[own], me.partner())
    over.wait_recv()
    out = pltpu.make_async_copy(ob, upd_out, local_sems.at[9])
    out.start()
    phase("o_finish")
    whole.wait_recv()
    store.wait()
    store_g.wait()
    out.wait()
    wire.finish()
    phase.end()


def orthogonalize(xin, xw, gram):
    def outer(value):
        return lax.dot_general(value, value, (((1,), (1,)), ((), ())), preferred_element_type=f32)

    def iteration(x_of, last):
        rounded = gram[...].astype(bf16)
        square = jnp.dot(rounded, rounded, preferred_element_type=f32)
        mixing = (coef_b * rounded.astype(f32) + coef_c * square).astype(bf16)
        total = None
        for k in range(4):
            cols = slice(k * 512, (k + 1) * 512)
            old = x_of(cols)
            product = jnp.dot(mixing, old, preferred_element_type=f32)
            new = (coef_a * old.astype(f32) + product).astype(bf16)
            xw[:, cols] = new
            if not last:
                total = outer(new) if k == 0 else total + outer(new)
        if not last:
            gram[...] = total

    first = outer(xin[...])
    diagonal = lax.broadcasted_iota(jnp.int32, (KV, KV), 0) == lax.broadcasted_iota(jnp.int32, (KV, KV), 1)
    norm = jnp.sqrt(jnp.sum(jnp.where(diagonal, first, 0.0), axis=(0, 1), keepdims=True))
    scale = 1.0 / (norm + epsilon)
    gram[...] = first * scale * scale
    iteration(lambda cols: (xin[:, cols].astype(f32) * scale).astype(bf16), False)

    def middle(i, carry):
        iteration(lambda cols: xw[:, cols], False)
        return carry

    lax.fori_loop(0, ITERS - 2, middle, 0)
    iteration(lambda cols: xw[:, cols], True)


def stepped(activations, cotangents, momentum, owners, bucket_starts):
    vm = pltpu.VMEM
    operands = (owners, bucket_starts, activations, cotangents, momentum)
    operands = [pltpu.with_memory_space_constraint(a, pltpu.HBM) for a in operands]
    return pl.pallas_call(
        step_kernel,
        out_shape=(
            jax.ShapeDtypeStruct((MATS, KV, 128), bf16),
            jax.ShapeDtypeStruct((16, 128), f32),
            jax.ShapeDtypeStruct((MATS, KV, 128), bf16),
            jax.ShapeDtypeStruct((2, KV, D), bf16),
        ),
        in_specs=[pl.BlockSpec(memory_space=pltpu.HBM)] * 5,
        out_specs=(
            pl.BlockSpec(memory_space=pl.ANY),
            pl.BlockSpec(memory_space=pltpu.VMEM),
            pl.BlockSpec(memory_space=pl.ANY),
            pl.BlockSpec(memory_space=pl.ANY),
        ),
        scratch_shapes=[
            vm((6, 128, 512), bf16), vm((3, 512, 128), bf16), vm((3, 128, D), bf16), vm((3, 256, D), bf16), vm((3, 512, 256), bf16),
            vm((14, 512, 128), bf16), vm((14, 512, 128), bf16),
            vm((6, 8, 128, 128), bf16), vm((6, 8, 128, 128), bf16),
            vm((6, 4, 256, 128), bf16), vm((6, 4, 256, 128), bf16),
            vm((2, 512, 128), bf16), vm((3, 2, 128, 128), bf16), vm((2, 128, 128), bf16), vm((3, 64, 128), bf16),
            vm((2, 8, 128, 128), bf16), vm((3, 8, 64, 128), bf16), vm((8, 64, 128), bf16), vm((7, 64, 128), bf16),
            vm((8, 256, 128), bf16), vm((3, 8, 64, 128), bf16), vm((8, 64, 128), bf16), vm((7, 64, 128), bf16),
            vm((MATS, KV, 128), bf16), vm((MATS, 32, 128), bf16), vm((8, 8, 128), f32), vm((32, 8, 128), f32),
            vm((MATS, 64, 128), f32), vm((16, 32, 128), bf16), vm((16, 64, 128), bf16), vm((16, 128), f32),
            vm((64, D), bf16), vm((64, D), bf16), vm((KV, D), bf16), vm((KV, D), bf16), vm((32, 32, 128), bf16), vm((MATS, KV, 128), bf16),
            vm((KV, KV), f32),
            pltpu.SMEM((MATS,), jnp.int32), pltpu.SMEM((2,), jnp.int32), pltpu.SMEM((2, 16), jnp.int32),
            pltpu.SemaphoreType.DMA((13,)),
            pltpu.SemaphoreType.DMA((OUTLETS,)),
            pltpu.SemaphoreType.DMA((ARRIVALS,)),
        ],
        compiler_params=pltpu.CompilerParams(
            collective_id=0, has_side_effects=True, vmem_limit_bytes=48 * 1024 * 1024
        ),
        name="step",
    )(*operands)


def finish_kernel(factors, g, mom, x, whole, mom_out, update, owned):
    i = pl.program_id(0)
    scale = math.sqrt(max(KV, D))
    for k in range(3):
        m = 3 * i + k
        factor = factors[pl.ds(m + 2 * (m >= 6).astype(jnp.int32), 1), :]
        mom_out[k] = momentum_rate * mom[k] + factor * g[k].astype(f32)
    update[...] = scale * x[...].astype(f32)
    owned[...] = (scale * whole[...].astype(f32)).astype(bf16)


def finished(factors, g, mom, x, whole):
    part = pl.BlockSpec((3, KV, 128), lambda i: (i, 0, 0))
    rows = pl.BlockSpec((2, KV // 4, D), lambda i: (0, i, 0))
    return pl.pallas_call(
        finish_kernel,
        grid=(4,),
        out_shape=(
            jax.ShapeDtypeStruct((MATS, KV, 128), f32),
            jax.ShapeDtypeStruct((MATS, KV, 128), f32),
            jax.ShapeDtypeStruct((2, KV, D), bf16),
        ),
        in_specs=[pl.BlockSpec((16, 128), lambda i: (0, 0)), part, part, part, rows],
        out_specs=(part, part, rows),
        compiler_params=pltpu.CompilerParams(vmem_limit_bytes=16 * 1024 * 1024),
        name="finish",
    )(factors, g, mom, x, whole)


def per_device(activations, cotangents, momentum, owners, bucket_starts):
    g, factors, x, whole = stepped(activations, cotangents, momentum, owners, bucket_starts)
    return finished(factors, g, momentum, x, whole)


def solution(mesh):
    torus = Mesh(
        mesh.devices.reshape(4, 2, 2, 8, 2), ("rep_0", "rep_1", "rep_2", "shard_0", "shard_1")
    )
    return jax.shard_map(
        per_device,
        mesh=torus,
        in_specs=(
            P(None, REP_SHARD, None),
            P(None, REP_SHARD, None),
            P(None, None, SHARD),
            P(),
            P(),
        ),
        out_specs=(P(None, None, SHARD), P(None, None, SHARD), P(SHARD, None, None)),
        check_vma=False,
    )
```

```python
import functools
import math

import jax
import jax.numpy as jnp
from jax import lax
from jax.experimental import pallas as pl
from jax.experimental.pallas import tpu as pltpu
from jax.sharding import Mesh
from jax.sharding import PartitionSpec as P

D = 2048
KV = 256
ITERS = 5
MATS = 12
TOKENS = 32768
SHARD = ("shard_0", "shard_1")
REP_SHARD = ("rep_0", "rep_1", "rep_2", "shard_0", "shard_1")

coef_a = 3.4445
coef_b = -4.775
coef_c = 2.0315
momentum_rate = 0.95
clip_level = 0.5
epsilon = 1e-06

f32 = jnp.float32
bf16 = jnp.bfloat16
MESH = pl.DeviceIdType.MESH


def wrap(value, size):
    return lax.rem(value + 2 * size, size)


class Place:
    def __init__(self):
        self.x = lax.axis_index("rep_0")
        self.yh = lax.axis_index("rep_1")
        self.c = lax.axis_index("rep_2")
        self.z = lax.axis_index("shard_0")
        self.yl = lax.axis_index("shard_1")
        self.y = 2 * self.yh + self.yl
        self.block = 2 * self.x + self.yh
        self.column = 2 * self.z + self.yl

    def at(self, dx=0, dz=0):
        return (wrap(self.x + dx, 4), self.yh, self.c, wrap(self.z + dz, 8), self.yl)

    def at_y(self, dy):
        y = wrap(self.y + dy, 4)
        return (self.x, lax.div(y, 2), self.c, self.z, lax.rem(y, 2))

    def partner(self):
        return (self.x, self.yh, 1 - self.c, self.z, self.yl)

    def near(self, dx, dy, dc, dz):
        y = wrap(self.y + dy, 4)
        core = 1 - self.c if dc else self.c
        return (wrap(self.x + dx, 4), lax.div(y, 2), core, wrap(self.z + dz, 8), lax.rem(y, 2))

    def replicas(self):
        for dx, dyh in self.offsets():
            yield (wrap(self.x + dx, 4), lax.rem(self.yh + dyh, 2), self.c, self.z, self.yl)

    def offsets(self):
        return ((1, 0), (3, 0), (0, 1), (2, 0), (1, 1), (3, 1), (2, 1))

    def columns_at(self, dz):
        for dyl in range(2):
            if dz or dyl:
                z, yl = wrap(self.z + dz, 8), lax.rem(self.yl + dyl, 2)
                yield (self.x, self.yh, self.c, z, yl), 2 * z + yl

    def columns(self):
        for dz in (4, 3, 5, 2, 6, 1, 7, 0):
            yield from self.columns_at(dz)


class Wire:
    def __init__(self, send_sems, recv_sems, device):
        self.send_sems, self.recv_sems, self.device = send_sems, recv_sems, device
        self.n_send = self.n_recv = 0
        self.leaving, self.kept, self.numbers = [], [], {}

    def copy(self, source, target, s, r, device):
        return pltpu.make_async_remote_copy(
            src_ref=source,
            dst_ref=target,
            send_sem=self.send_sems.at[s],
            recv_sem=self.recv_sems.at[r],
            device_id=device,
            device_id_type=MESH,
        )

    def outlet(self, whole):
        self.n_send += 1
        self.leaving.append((self.n_send - 1, whole))
        return self.n_send - 1

    def send(self, source, target, device, s=None):
        if s is None:
            s = self.outlet(source)
        r = self.n_recv
        self.n_recv += 1
        copy = self.copy(source, target, s, r, device)
        copy.start()
        return copy

    def opened(self, whole):
        s, r = self.outlet(whole), self.n_recv
        self.n_recv += 1
        copy = self.copy(whole, whole, s, r, self.device)
        self.kept.append(copy)
        self.numbers[id(copy)] = (s, r)
        return copy

    def join(self, group, copies):
        for source, target, device in copies:
            self.copy(source, target, *self.numbers[id(group)], device).start()

    def group(self, copies, whole):
        group = self.opened(whole)
        self.join(group, copies)
        return group

    def finish(self):
        assert (self.n_send, self.n_recv) == (OUTLETS, ARRIVALS), (self.n_send, self.n_recv)
        for s, whole in self.leaving:
            self.copy(whole, whole, s, 0, self.device).wait_send()


def signal_all(devices):
    barrier = pltpu.get_barrier_semaphore()
    for device in devices:
        pl.semaphore_signal(barrier, inc=1, device_id=device, device_id_type=MESH)


class Phases:
    def __init__(self):
        self.open = None

    def __call__(self, name):
        self.end()
        self.open = jax.named_scope(name)
        self.open.__enter__()

    def end(self):
        if self.open:
            self.open.__exit__(None, None, None)
        self.open = None


def rows_at(start, size):
    return pl.ds(pl.multiple_of(start, size), size)


Z_STEPS = {(0, 1): 4, (1, -1): 4, (1, 1): 3, (0, -1): 3}
Z_BASE = {(0, 1): 0, (1, -1): 4, (1, 1): 8, (0, -1): 11}
PAIR_BASE = {(0, 1): 0, (1, -1): 2, (1, 1): 4, (0, -1): 5}
PAIR_STEPS = {(0, 1): 2, (1, -1): 2, (1, 1): 1, (0, -1): 1}
OUTLETS, ARRIVALS = 39, 67


def step_kernel(
    owners_in, starts_in, act, cot, mom, g_out, f_out, upd_out, o_out,
    cin, cout, aout, actv, cott, zs, zr, xs, xr, ys, yr,
    z2s, z2r, z3s, z3r, x2s, x2r, x3s, x3r, y2s, y2r, y3s, y3r,
    gb, gp, sqs, sq2, mb, us, ms, fac, gq, mq, gin, xw, rb, ob, gram, owners, starts, table, local_sems, send_sems, recv_sems,
):
    me = Place()
    x, y, yh, yl, z, c = me.x, me.y, me.yh, me.yl, me.z, me.c
    wire = Wire(send_sems, recv_sems, me.partner())
    phase = Phases()
    mine = rows_at(c * 128, 128)

    load_cot = pltpu.make_async_copy(cot, cin, local_sems.at[0])
    load_cot.start()
    loads, loads_out = [], []
    for j in range(3):
        loads_out.append(pltpu.make_async_copy(act.at[3 * (1 - c) + j], aout.at[j], local_sems.at[1 + j]))
        loads.append(pltpu.make_async_copy(act.at[3 * c + j], actv.at[j, mine], local_sems.at[4 + j]))
        loads_out[j].start()
        loads[j].start()
    rows = rows_at(me.block * 32, 32)
    load_momentum = pltpu.make_async_copy(mom.at[:, rows_at(x * 64, 64), :], mb, local_sems.at[12])
    load_momentum.start()
    load_owners = pltpu.make_async_copy(owners_in, owners, local_sems.at[10])
    load_starts = pltpu.make_async_copy(starts_in, starts, local_sems.at[11])
    load_owners.start()
    load_starts.start()

    phase("r_greet")
    plane = [(dx, dy, dc) for dx in range(4) for dy in range(4) for dc in range(2) if dx or dy or dc]
    devices = [me.near(dx, dy, dc, 0) for dx, dy, dc in plane]
    devices += [me.near(0, dy, 0, dz) for dy in range(4) for dz in range(1, 8)]
    signal_all(devices)

    def turn(source, store, inner_is_x):
        turned = source.T
        for bx in range(4):
            for by in range(2):
                for kv in range(2):
                    at = kv * 256 + (bx * 2 + by) * 32
                    to = (by * 256 + bx * 64 if inner_is_x else bx * 128 + by * 64) + kv * 32
                    store(to, turned[at : at + 32, :])

    load_cot.wait()
    for j in (1, 2, 0):

        def store_out(to, value, j=j):
            cout[j, to : to + 32, :] = value

        def store_own(to, value, j=j):
            cott[j, to : to + 32, mine] = value

        turn(cin[3 * (1 - c) + j], store_out, j == 2)
        turn(cin[3 * c + j], store_own, j == 2)

    phase("r_greetw")
    pl.semaphore_wait(pltpu.get_barrier_semaphore(), len(devices))
    phase("r_swap")
    out_cot, out_act = wire.outlet(cout), wire.outlet(aout)
    out_x, out_y, out_z = wire.outlet(xs), wire.outlet(ys), wire.outlet(zs)
    swaps = {}
    for j in (1, 2, 0):
        loads_out[j].wait()
        swaps[j] = [wire.send(cout.at[j], cott.at[j, :, mine], me.partner(), out_cot)]
        parts = 2 if j == 1 else 1
        for k in range(parts):
            cols = pl.ds(k * (D // parts), D // parts)
            swaps[j].append(
                wire.send(aout.at[j, :, cols], actv.at[j, mine, cols], me.partner(), out_act)
            )

    def prepare(j):
        loads[j].wait()
        swaps[j][0].wait_recv()
        swaps[j][1].wait_recv()

    sent = {}

    def z_part(dest, half):
        columns = rows_at(dest * 256 + half * 128, 128)
        return jnp.dot(cott[0], actv[0, :, columns], preferred_element_type=f32)

    def z_send(half, d, n, k):
        part = z_part(wrap(z + d * (n + 1 - k), 8), half)
        slot = Z_BASE[half, d] + k - 1
        if k > 1:
            sent["z", half, d, k - 1].wait_recv()
            part += zr[slot - 1].astype(f32)
        zs[slot] = part.astype(bf16)
        sent["z", half, d, k] = wire.send(zs.at[slot], zr.at[slot], me.at(dz=d), out_z)

    def x_part(dest, half, i):
        columns = rows_at((4 * half + i) * 256, 256)
        return jnp.dot(cott[1, rows_at(dest * 128, 128), :], actv[1, :, columns], preferred_element_type=f32)

    def x_send(half, d, k):
        dest = wrap(x + d * (PAIR_STEPS[half, d] + 1 - k), 4)
        slot = PAIR_BASE[half, d] + k - 1
        if k > 1:
            sent["x", half, d, k - 1].wait_recv()

        def step(i, carry):
            part = x_part(dest, half, i)
            for t in range(2):
                value = part[:, t * 128 : (t + 1) * 128]
                if k > 1:
                    value += xr[slot - 1, 2 * i + t].astype(f32)
                xs[slot, 2 * i + t] = value.astype(bf16)
            return carry

        lax.fori_loop(0, 4, step, 0, unroll=True)
        sent["x", half, d, k] = wire.send(xs.at[slot], xr.at[slot], me.at(dx=d), out_x)

    def y_part(dest, half, i):
        columns = rows_at(((4 * half + i) * 2 + lax.rem(dest, 2)) * 128, 128)
        rows = rows_at(lax.div(dest, 2) * 256, 256)
        return jnp.dot(cott[2, rows, :], actv[2, :, columns], preferred_element_type=f32)

    def y_send(half, d, k):
        dest = wrap(y + d * (PAIR_STEPS[half, d] + 1 - k), 4)
        slot = PAIR_BASE[half, d] + k - 1
        if k > 1:
            sent["y", half, d, k - 1].wait_recv()

        def step(i, carry):
            value = y_part(dest, half, i)
            if k > 1:
                value += yr[slot - 1, i].astype(f32)
            ys[slot, i] = value.astype(bf16)
            return carry

        lax.fori_loop(0, 4, step, 0, unroll=True)
        sent["y", half, d, k] = wire.send(ys.at[slot], yr.at[slot], me.at_y(d), out_y)

    def z_round(k, long=None):
        for (half, d), n in Z_STEPS.items():
            if k <= n and long in (None, n == 4):
                z_send(half, d, n, k)

    phase("r_prep0")
    prepare(1)
    phase("r_x1")
    x_send(0, 1, 1)
    swaps[1][2].wait_recv()
    x_send(1, -1, 1)
    phase("r_y1")
    prepare(2)
    y_send(0, 1, 1)
    y_send(1, -1, 1)
    phase("r_z1")
    prepare(0)
    z_round(1)
    phase("r_xy1b")
    x_send(1, 1, 1)
    x_send(0, -1, 1)
    y_send(1, 1, 1)
    y_send(0, -1, 1)
    here = rows_at(me.column * 128, 128)

    def slot_matrix(p):
        found, seen, filled = jnp.int32(0), jnp.int32(0), jnp.int32(0)
        for m in range(MATS):
            named = (owners[m] == p).astype(jnp.int32)
            take = named * (seen == c).astype(jnp.int32)
            found, filled, seen = found + take * m, filled + take, seen + named
        return found, filled

    def note(p, carry):
        table[0, p], table[1, p] = slot_matrix(p)
        return carry

    def gather_columns(pieces, target):
        def choose(p, carry):
            found, filled = table[0, p], table[1, p]
            target[p] = (pieces[found].astype(f32) * filled.astype(f32)).astype(bf16)
            return carry

        lax.fori_loop(0, 16, choose, 0, unroll=2)

    phase("r_msend")
    load_momentum.wait()
    load_owners.wait()
    load_starts.wait()
    lax.fori_loop(0, 16, note, 0)
    gather_columns(mb, ms)
    mq[:, here] = ms[me.column]

    phase("r_z2")
    z_round(2, True)
    phase("r_x2")
    x_send(0, 1, 2)
    x_send(1, -1, 2)
    phase("r_y2")
    y_send(0, 1, 2)
    y_send(1, -1, 2)
    phase("r_z2b")
    z_round(2, False)
    phase("r_z3")
    z_round(3, True)
    z_round(3, False)
    phase("r_z4")
    z_round(4)
    copies = [(ms.at[p], mq.at[:, here], device) for device, p in me.columns()]
    momentum_to_owner = wire.group(copies, ms.at[:15])

    phase("r_xlast")
    def turned_z(to):
        return wrap(to - z - 2, 8)

    def third(second, buffer, arrived, here, store):
        for e in range(4 * second, 4 * second + 4):
            value = here(e).astype(f32)
            for d in range(3):
                value += arrived[second, d, e % 4].astype(f32)
            buffer[e] = value.astype(bf16)
        places = (2, 1, 3, 0) if second == 0 else (4, 7, 5)
        copies = [(buffer.at[e], store.at[e], me.at(dz=e + 2)) for e in places]
        return wire.group(copies, store.at[: len(places)])

    for half in range(2):
        sent["x", half, 1, PAIR_STEPS[half, 1]].wait_recv()
        sent["x", half, -1, PAIR_STEPS[half, -1]].wait_recv()
        up = PAIR_BASE[half, 1] + PAIR_STEPS[half, 1] - 1
        down = PAIR_BASE[half, -1] + PAIR_STEPS[half, -1] - 1

        def x_last(i, carry, half=half, up=up, down=down):
            part = x_part(x, half, i)
            for t in range(2):
                value = part[:, t * 128 : (t + 1) * 128]
                value += xr[up, 2 * i + t].astype(f32) + xr[down, 2 * i + t].astype(f32)
                x2s[t, turned_z(4 * half + i)] = value.astype(bf16)
            return carry

        lax.fori_loop(0, 4, x_last, 0, unroll=True)
    for second in range(2):
        copies = []
        for d in (1, 3, 2):
            to = wrap(y + d, 4)
            source = x2s.at[lax.rem(to, 2), pl.ds(4 * second, 4), rows_at(lax.div(to, 2) * 64, 64), :]
            copies.append((source, x2r.at[second, d - 1], me.at_y(d)))
        sent["x2", second] = wire.group(copies, x2r.at[second])

    phase("r_ylast")
    for half in range(2):
        sent["y", half, 1, PAIR_STEPS[half, 1]].wait_recv()
        sent["y", half, -1, PAIR_STEPS[half, -1]].wait_recv()
        up = PAIR_BASE[half, 1] + PAIR_STEPS[half, 1] - 1
        down = PAIR_BASE[half, -1] + PAIR_STEPS[half, -1] - 1

        def y_last(i, carry, half=half, up=up, down=down):
            value = y_part(y, half, i) + yr[up, i].astype(f32) + yr[down, i].astype(f32)
            y2s[turned_z(4 * half + i)] = value.astype(bf16)
            return carry

        lax.fori_loop(0, 4, y_last, 0, unroll=True)
    for second in range(2):
        copies = []
        for d in (1, 3, 2):
            source = y2s.at[pl.ds(4 * second, 4), rows_at(wrap(x + d, 4) * 64, 64), :]
            copies.append((source, y2r.at[second, d - 1], me.at(dx=d)))
        sent["y2", second] = wire.group(copies, y2r.at[second])

    phase("r_zlast")
    for half in range(2):
        last = []
        for d in (1, -1):
            n = Z_STEPS[half, d]
            sent["z", half, d, n].wait_recv()
            last.append(Z_BASE[half, d] + n - 1)
        value = z_part(z, half) + zr[last[0]].astype(f32) + zr[last[1]].astype(f32)
        z2s[half] = value.astype(bf16)
    copies = []
    for d in (1, 3, 2):
        to = wrap(x + d, 4)
        copies.append((z2s.at[:, rows_at(to * 128, 128), :], z2r.at[d - 1], me.at(dx=d)))
    sent["z2"] = wire.group(copies, z2r)
    def z_second():
        phase("r_z3b")
        sent["z2"].wait_recv()
        for t in range(2):
            value = z2s[t, rows_at(x * 128, 128), :].astype(f32)
            for d in range(3):
                value += z2r[d, t].astype(f32)
            z3s[t] = value.astype(bf16)
        copies = []
        for d in (2, 1, 3):
            to = wrap(y + d, 4)
            source = z3s.at[lax.rem(to, 2), rows_at(lax.div(to, 2) * 64, 64), :]
            copies.append((source, z3r.at[d - 1], me.at_y(d)))
        sent["z3"] = wire.group(copies, z3r)

    def x_here(e):
        return x2s[yl, e, rows_at(yh * 64, 64), :]

    def y_here(e):
        return y2s[e, rows_at(x * 64, 64), :]

    for second in range(2):
        phase("r_x3" + "ab"[second])
        sent["x2", second].wait_recv()
        sent["x3", second] = third(second, x3s, x2r, x_here, x3r)
        phase("r_y3" + "ab"[second])
        sent["y2", second].wait_recv()
        sent["y3", second] = third(second, y3s, y2r, y_here, y3r)
        if second == 0:
            z_second()

    phase("r_xfin")
    inverse = 1.0 / math.sqrt(TOKENS)
    sqs[z] = jnp.zeros((8, 128), f32)

    def piece(j, value):
        value = value * inverse
        for kv in range(2):
            block = value[kv * 32 : (kv + 1) * 32]
            gb[6 * c + 2 * j + kv, rows, :] = block.astype(bf16)
            gp[6 * c + 2 * j + kv] = block.astype(bf16)
            total = jnp.sum(block * block, axis=(0, 1), keepdims=True)
            sqs[z, 2 * j + kv : 2 * j + kv + 1, :] = jnp.broadcast_to(total, (1, 128))

    sent["x3", 0].wait_recv()
    sent["x3", 1].wait_recv()
    value = x3s[6].astype(f32)
    for e in (0, 1, 2, 3, 4, 5, 7):
        value += x3r[e].astype(f32)
    piece(1, value)
    phase("r_yfin")
    sent["y3", 0].wait_recv()
    sent["y3", 1].wait_recv()
    value = y3s[6].astype(f32)
    for e in (0, 1, 2, 3, 4, 5, 7):
        value += y3r[e].astype(f32)
    piece(2, value)
    phase("r_zfin")
    sent["z3"].wait_recv()
    value = z3s[yl, rows_at(yh * 64, 64), :].astype(f32)
    for d in range(3):
        value += z3r[d].astype(f32)
    piece(0, value)

    phase("r_sqsend")
    own = pl.ds(6 * c, 6)
    squares = wire.group([(sqs.at[z], sqs.at[z], me.at(dz=d)) for d in (4, 3, 5, 2, 6, 1, 7)], sqs.at[:7])
    swap = wire.send(gp.at[own], gp.at[own], me.partner())
    swap.wait_recv()
    gather_columns(gp, us)
    half = rows_at(yh * 32, 32)
    gq[half, here] = us[me.column]
    copies = []
    for dz in (4, 3, 5, 2, 6, 1, 7, 0):
        for dy in (2, 1, 3, 0):
            if dz or dy:
                device = me.near(0, dy, 0, dz)
                copies.append((us.at[2 * device[3] + device[4]], gq.at[half, here], device))
    to_owner = wire.group(copies, rb.at[:31])
    phase("r_sqw1b")
    squares.wait_recv()
    spot = c * 16 + 4 * x + y
    sq2[spot] = sum((sqs[i] for i in range(1, 8)), sqs[0])
    squares = wire.group(
        [(sq2.at[spot], sq2.at[spot], me.near(dx, dy, dc, 0)) for dx, dy, dc in plane], sq2.at[:31]
    )
    phase("r_sqw2")
    squares.wait_recv()
    totals = [sum((sq2[k * 16 + i] for i in range(1, 16)), sq2[k * 16]) for k in range(2)]
    totals = jnp.concatenate(totals, axis=0)
    phase("o_a2a")
    momentum_to_owner.wait_recv()
    to_owner.wait_recv()
    phase("o_choose")

    row = lax.broadcasted_iota(jnp.int32, (16, 128), 0)
    matrix = jnp.where(row >= 8, row - 2, row)
    held = (row < 6) | ((row >= 8) & (row < 14))
    bucket = (matrix >= starts[0]).astype(jnp.int32) + (matrix >= starts[1]).astype(jnp.int32)
    factors = jnp.ones((16, 128), f32)
    for b in range(3):
        inside = held & (bucket == b)
        total = jnp.sum(jnp.where(inside, totals, 0.0), axis=0, keepdims=True)
        members = jnp.sum(inside.astype(f32), axis=0, keepdims=True)
        root_mean = jnp.sqrt(total / (members * (KV * D)) + epsilon)
        factors = jnp.where(inside, jnp.minimum(1.0, clip_level / root_mean), factors)
    f_out[...] = factors
    fac[...] = factors
    mine_is = table[0, me.column]
    factor = fac[pl.ds(mine_is + 2 * (mine_is >= 6).astype(jnp.int32), 1), :]
    for k in range(4):
        cols = slice(k * 512, (k + 1) * 512)
        scaled = factor[:, :1] * gq[:, cols].astype(f32)
        value = scaled + momentum_rate * (momentum_rate * mq[:, cols].astype(f32) + scaled)
        gin[rows_at(x * 64, 64), cols] = value.astype(bf16)

    phase("o_ag")

    def part(dx, h):
        return gin.at[rows_at(wrap(x + dx, 4) * 64 + 32 * h, 32), :]

    ahead, behind = me.at(dx=1), me.at(dx=-1)
    first_up = wire.send(part(0, 0), part(0, 0), ahead)
    first_down = wire.send(part(0, 1), part(0, 1), behind)
    second_up = wire.send(part(0, 1), part(0, 1), ahead)
    second_down = wire.send(part(0, 0), part(0, 0), behind)
    first_up.wait_recv()
    third_up = wire.send(part(-1, 0), part(-1, 0), ahead)
    first_down.wait_recv()
    third_down = wire.send(part(1, 1), part(1, 1), behind)
    for copy in (second_up, second_down, third_up, third_down):
        copy.wait_recv()
    pieces = wire.group(
        [(gb.at[own, rows, :], gb.at[own, rows, :], device) for device in me.replicas()], gb.at[:6, :224, :]
    )

    phase("o_ns")
    orthogonalize(gin, xw, gram)

    phase("o_back")
    copies = [
        (xw.at[rows, rows_at(p * 128, 128)], rb.at[c * 16 + me.column], device) for device, p in me.columns()
    ]
    back = wire.group(copies, rb.at[:15])
    rb[c * 16 + me.column] = xw[rows, here]
    pieces.wait_recv()
    over_g = wire.send(gb.at[own], gb.at[own], me.partner())
    whole = wire.send(xw, o_out.at[c], me.partner())
    store = pltpu.make_async_copy(xw, o_out.at[c], local_sems.at[7])
    store.start()
    back.wait_recv()
    phase("o_over")
    slots = pl.ds(c * 16, 16)
    over = wire.send(rb.at[slots], rb.at[slots], me.partner())
    over.wait_recv()
    for k in range(6):
        m = 6 * c + k
        owner = owners[m]
        slot = jnp.int32(0)
        for j in range(MATS):
            slot = slot + (owners[j] == owner).astype(jnp.int32) * (j < m).astype(jnp.int32)
        ob[m, rows, :] = rb[jnp.minimum(slot, 1) * 16 + owner]
    phase("o_ag2")
    gathered = [wire.send(ob.at[own, rows, :], ob.at[own, rows, :], device) for device in me.replicas()]
    onward = wire.opened(ob.at[:6])
    wire.join(onward, [(ob.at[own, rows, :], ob.at[own, rows, :], me.partner())])
    over_g.wait_recv()
    store_g = pltpu.make_async_copy(gb, g_out, local_sems.at[8])
    store_g.start()
    for copy, (dx, dyh) in zip(gathered, me.offsets(), strict=True):
        copy.wait_recv()
        block = 2 * wrap(x - dx, 4) + lax.rem(yh + dyh, 2)
        arrived = ob.at[own, rows_at(block * 32, 32), :]
        wire.join(onward, [(arrived, arrived, me.partner())])
    phase("o_over2")
    onward.wait_recv()
    out = pltpu.make_async_copy(ob, upd_out, local_sems.at[9])
    out.start()
    phase("o_finish")
    whole.wait_recv()
    store.wait()
    store_g.wait()
    out.wait()
    wire.finish()
    phase.end()


def orthogonalize(xin, xw, gram):
    def outer(value):
        return lax.dot_general(value, value, (((1,), (1,)), ((), ())), preferred_element_type=f32)

    def iteration(x_of, last):
        rounded = gram[...].astype(bf16)
        square = jnp.dot(rounded, rounded, preferred_element_type=f32)
        mixing = (coef_b * rounded.astype(f32) + coef_c * square).astype(bf16)
        total = None
        for k in range(4):
            cols = slice(k * 512, (k + 1) * 512)
            old = x_of(cols)
            product = jnp.dot(mixing, old, preferred_element_type=f32)
            new = (coef_a * old.astype(f32) + product).astype(bf16)
            xw[:, cols] = new
            if not last:
                total = outer(new) if k == 0 else total + outer(new)
        if not last:
            gram[...] = total

    first = outer(xin[...])
    diagonal = lax.broadcasted_iota(jnp.int32, (KV, KV), 0) == lax.broadcasted_iota(jnp.int32, (KV, KV), 1)
    norm = jnp.sqrt(jnp.sum(jnp.where(diagonal, first, 0.0), axis=(0, 1), keepdims=True))
    scale = 1.0 / (norm + epsilon)
    gram[...] = first * scale * scale
    iteration(lambda cols: (xin[:, cols].astype(f32) * scale).astype(bf16), False)

    def middle(i, carry):
        iteration(lambda cols: xw[:, cols], False)
        return carry

    lax.fori_loop(0, ITERS - 2, middle, 0)
    iteration(lambda cols: xw[:, cols], True)


def stepped(activations, cotangents, momentum, owners, bucket_starts):
    vm = pltpu.VMEM
    operands = (owners, bucket_starts, activations, cotangents, momentum)
    operands = [pltpu.with_memory_space_constraint(a, pltpu.HBM) for a in operands]
    return pl.pallas_call(
        step_kernel,
        out_shape=(
            jax.ShapeDtypeStruct((MATS, KV, 128), bf16),
            jax.ShapeDtypeStruct((16, 128), f32),
            jax.ShapeDtypeStruct((MATS, KV, 128), bf16),
            jax.ShapeDtypeStruct((2, KV, D), bf16),
        ),
        in_specs=[pl.BlockSpec(memory_space=pltpu.HBM)] * 5,
        out_specs=(
            pl.BlockSpec(memory_space=pl.ANY),
            pl.BlockSpec(memory_space=pltpu.VMEM),
            pl.BlockSpec(memory_space=pl.ANY),
            pl.BlockSpec(memory_space=pl.ANY),
        ),
        scratch_shapes=[
            vm((6, 128, 512), bf16), vm((3, 512, 128), bf16), vm((3, 128, D), bf16), vm((3, 256, D), bf16), vm((3, 512, 256), bf16),
            vm((14, 512, 128), bf16), vm((14, 512, 128), bf16),
            vm((6, 8, 128, 128), bf16), vm((6, 8, 128, 128), bf16),
            vm((6, 4, 256, 128), bf16), vm((6, 4, 256, 128), bf16),
            vm((2, 512, 128), bf16), vm((3, 2, 128, 128), bf16), vm((2, 128, 128), bf16), vm((3, 64, 128), bf16),
            vm((2, 8, 128, 128), bf16), vm((2, 3, 4, 64, 128), bf16), vm((8, 64, 128), bf16), vm((8, 64, 128), bf16),
            vm((8, 256, 128), bf16), vm((2, 3, 4, 64, 128), bf16), vm((8, 64, 128), bf16), vm((8, 64, 128), bf16),
            vm((MATS, KV, 128), bf16), vm((MATS, 32, 128), bf16), vm((8, 8, 128), f32), vm((32, 8, 128), f32),
            vm((MATS, 64, 128), f32), vm((16, 32, 128), bf16), vm((16, 64, 128), bf16), vm((16, 128), f32),
            vm((64, D), bf16), vm((64, D), bf16), vm((KV, D), bf16), vm((KV, D), bf16), vm((32, 32, 128), bf16), vm((MATS, KV, 128), bf16),
            vm((KV, KV), f32),
            pltpu.SMEM((MATS,), jnp.int32), pltpu.SMEM((2,), jnp.int32), pltpu.SMEM((2, 16), jnp.int32),
            pltpu.SemaphoreType.DMA((13,)),
            pltpu.SemaphoreType.DMA((OUTLETS,)),
            pltpu.SemaphoreType.DMA((ARRIVALS,)),
        ],
        compiler_params=pltpu.CompilerParams(
            collective_id=0, has_side_effects=True, vmem_limit_bytes=48 * 1024 * 1024
        ),
        name="step",
    )(*operands)


def finish_kernel(factors, g, mom, x, whole, mom_out, update, owned):
    i = pl.program_id(0)
    scale = math.sqrt(max(KV, D))
    for k in range(3):
        m = 3 * i + k
        factor = factors[pl.ds(m + 2 * (m >= 6).astype(jnp.int32), 1), :]
        mom_out[k] = momentum_rate * mom[k] + factor * g[k].astype(f32)
    update[...] = scale * x[...].astype(f32)
    owned[...] = (scale * whole[...].astype(f32)).astype(bf16)


def finished(factors, g, mom, x, whole):
    part = pl.BlockSpec((3, KV, 128), lambda i: (i, 0, 0))
    rows = pl.BlockSpec((2, KV // 4, D), lambda i: (0, i, 0))
    return pl.pallas_call(
        finish_kernel,
        grid=(4,),
        out_shape=(
            jax.ShapeDtypeStruct((MATS, KV, 128), f32),
            jax.ShapeDtypeStruct((MATS, KV, 128), f32),
            jax.ShapeDtypeStruct((2, KV, D), bf16),
        ),
        in_specs=[pl.BlockSpec((16, 128), lambda i: (0, 0)), part, part, part, rows],
        out_specs=(part, part, rows),
        compiler_params=pltpu.CompilerParams(vmem_limit_bytes=16 * 1024 * 1024),
        name="finish",
    )(factors, g, mom, x, whole)


def per_device(activations, cotangents, momentum, owners, bucket_starts):
    g, factors, x, whole = stepped(activations, cotangents, momentum, owners, bucket_starts)
    return finished(factors, g, momentum, x, whole)


def solution(mesh):
    torus = Mesh(
        mesh.devices.reshape(4, 2, 2, 8, 2), ("rep_0", "rep_1", "rep_2", "shard_0", "shard_1")
    )
    return jax.shard_map(
        per_device,
        mesh=torus,
        in_specs=(
            P(None, REP_SHARD, None),
            P(None, REP_SHARD, None),
            P(None, None, SHARD),
            P(),
            P(),
        ),
        out_specs=(P(None, None, SHARD), P(None, None, SHARD), P(SHARD, None, None)),
        check_vma=False,
    )
```

```python
import functools
import math

import jax
import jax.numpy as jnp
from jax import lax
from jax.experimental import pallas as pl
from jax.experimental.pallas import tpu as pltpu
from jax.sharding import Mesh
from jax.sharding import PartitionSpec as P

D = 2048
KV = 256
ITERS = 5
MATS = 12
TOKENS = 32768
SHARD = ("shard_0", "shard_1")
REP_SHARD = ("rep_0", "rep_1", "rep_2", "shard_0", "shard_1")

coef_a = 3.4445
coef_b = -4.775
coef_c = 2.0315
momentum_rate = 0.95
clip_level = 0.5
epsilon = 1e-06

f32 = jnp.float32
bf16 = jnp.bfloat16
MESH = pl.DeviceIdType.MESH


def wrap(value, size):
    return lax.rem(value + 2 * size, size)


class Place:
    def __init__(self):
        self.x = lax.axis_index("rep_0")
        self.yh = lax.axis_index("rep_1")
        self.c = lax.axis_index("rep_2")
        self.z = lax.axis_index("shard_0")
        self.yl = lax.axis_index("shard_1")
        self.y = 2 * self.yh + self.yl
        self.block = 2 * self.x + self.yh
        self.column = 2 * self.z + self.yl

    def at(self, dx=0, dz=0):
        return (wrap(self.x + dx, 4), self.yh, self.c, wrap(self.z + dz, 8), self.yl)

    def at_y(self, dy):
        y = wrap(self.y + dy, 4)
        return (self.x, lax.div(y, 2), self.c, self.z, lax.rem(y, 2))

    def partner(self):
        return (self.x, self.yh, 1 - self.c, self.z, self.yl)

    def near(self, dx, dy, dc, dz):
        y = wrap(self.y + dy, 4)
        core = 1 - self.c if dc else self.c
        return (wrap(self.x + dx, 4), lax.div(y, 2), core, wrap(self.z + dz, 8), lax.rem(y, 2))

    def replicas(self):
        for dx, dyh in self.offsets():
            yield (wrap(self.x + dx, 4), lax.rem(self.yh + dyh, 2), self.c, self.z, self.yl)

    def offsets(self):
        return ((1, 0), (3, 0), (0, 1), (2, 0), (1, 1), (3, 1), (2, 1))

    def columns_at(self, dz):
        for dyl in range(2):
            if dz or dyl:
                z, yl = wrap(self.z + dz, 8), lax.rem(self.yl + dyl, 2)
                yield (self.x, self.yh, self.c, z, yl), 2 * z + yl

    def columns(self):
        for dz in (4, 3, 5, 2, 6, 1, 7, 0):
            yield from self.columns_at(dz)


class Wire:
    def __init__(self, send_sems, recv_sems, device):
        self.send_sems, self.recv_sems, self.device = send_sems, recv_sems, device
        self.n_send = self.n_recv = 0
        self.leaving, self.kept, self.numbers = [], [], {}

    def copy(self, source, target, s, r, device):
        return pltpu.make_async_remote_copy(
            src_ref=source,
            dst_ref=target,
            send_sem=self.send_sems.at[s],
            recv_sem=self.recv_sems.at[r],
            device_id=device,
            device_id_type=MESH,
        )

    def outlet(self, whole):
        self.n_send += 1
        self.leaving.append((self.n_send - 1, whole))
        return self.n_send - 1

    def send(self, source, target, device, s=None):
        if s is None:
            s = self.outlet(source)
        r = self.n_recv
        self.n_recv += 1
        copy = self.copy(source, target, s, r, device)
        copy.start()
        return copy

    def opened(self, whole):
        s, r = self.outlet(whole), self.n_recv
        self.n_recv += 1
        copy = self.copy(whole, whole, s, r, self.device)
        self.kept.append(copy)
        self.numbers[id(copy)] = (s, r)
        return copy

    def join(self, group, copies):
        for source, target, device in copies:
            self.copy(source, target, *self.numbers[id(group)], device).start()

    def group(self, copies, whole):
        group = self.opened(whole)
        self.join(group, copies)
        return group

    def finish(self):
        assert (self.n_send, self.n_recv) == (OUTLETS, ARRIVALS), (self.n_send, self.n_recv)
        for s, whole in self.leaving:
            self.copy(whole, whole, s, 0, self.device).wait_send()


def signal_all(devices):
    barrier = pltpu.get_barrier_semaphore()
    for device in devices:
        pl.semaphore_signal(barrier, inc=1, device_id=device, device_id_type=MESH)


class Phases:
    def __init__(self):
        self.open = None

    def __call__(self, name):
        self.end()
        self.open = jax.named_scope(name)
        self.open.__enter__()

    def end(self):
        if self.open:
            self.open.__exit__(None, None, None)
        self.open = None


def rows_at(start, size):
    return pl.ds(pl.multiple_of(start, size), size)


Z_STEPS = {(0, 1): 4, (1, -1): 4, (1, 1): 3, (0, -1): 3}
Z_BASE = {(0, 1): 0, (1, -1): 4, (1, 1): 8, (0, -1): 11}
PAIR_BASE = {(0, 1): 0, (1, -1): 2, (1, 1): 4, (0, -1): 5}
PAIR_STEPS = {(0, 1): 2, (1, -1): 2, (1, 1): 1, (0, -1): 1}
OUTLETS, ARRIVALS = 29, 68


def step_kernel(
    owners_in, starts_in, act, cot, mom, g_out, f_out, upd_out, o_out,
    cin, cout, aout, actv, cott, zs, zr, xs, xr, ys, yr,
    z2s, z2r, z3s, z3r, x2s, x2r, x3s, x3r, y2s, y2r, y3s, y3r,
    gb, gp, sqs, sq2, mb, us, ms, fac, gq, mq, gin, xw, rb, ob, gram, owners, starts, table, local_sems, send_sems, recv_sems,
):
    me = Place()
    x, y, yh, yl, z, c = me.x, me.y, me.yh, me.yl, me.z, me.c
    wire = Wire(send_sems, recv_sems, me.partner())
    phase = Phases()
    mine = rows_at(c * 128, 128)

    load_cot = pltpu.make_async_copy(cot, cin, local_sems.at[0])
    load_cot.start()
    loads, loads_out = [], []
    for j in range(3):
        loads_out.append(pltpu.make_async_copy(act.at[3 * (1 - c) + j], aout.at[j], local_sems.at[1 + j]))
        loads.append(pltpu.make_async_copy(act.at[3 * c + j], actv.at[j, mine], local_sems.at[4 + j]))
        loads_out[j].start()
        loads[j].start()
    rows = rows_at(me.block * 32, 32)
    load_momentum = pltpu.make_async_copy(mom.at[:, rows, :], mb, local_sems.at[12])
    load_momentum.start()
    load_owners = pltpu.make_async_copy(owners_in, owners, local_sems.at[10])
    load_starts = pltpu.make_async_copy(starts_in, starts, local_sems.at[11])
    load_owners.start()
    load_starts.start()

    phase("r_greet")
    plane = [(dx, dy, dc) for dx in range(4) for dy in range(4) for dc in range(2) if dx or dy or dc]
    devices = [me.partner()]
    devices += [me.near(d, 0, 0, 0) for d in range(1, 4)]
    devices += [me.near(0, d, 0, 0) for d in range(1, 4)]
    devices += [me.near(0, 0, 0, d) for d in range(1, 8)]
    devices += [(x, yh, c, wrap(z + d, 8), 1 - yl) for d in range(1, 8)]
    signal_all(devices)

    def turn(source, store, inner_is_x):
        turned = source.T
        for bx in range(4):
            for by in range(2):
                for kv in range(2):
                    at = kv * 256 + (bx * 2 + by) * 32
                    to = (by * 256 + bx * 64 if inner_is_x else bx * 128 + by * 64) + kv * 32
                    store(to, turned[at : at + 32, :])

    load_cot.wait()
    for j in (1, 2, 0):

        def store_out(to, value, j=j):
            cout[j, to : to + 32, :] = value

        def store_own(to, value, j=j):
            cott[j, to : to + 32, mine] = value

        turn(cin[3 * (1 - c) + j], store_out, j == 2)
        turn(cin[3 * c + j], store_own, j == 2)

    phase("r_greetw")
    pl.semaphore_wait(pltpu.get_barrier_semaphore(), len(devices))
    phase("r_swap")
    out_cot, out_act = wire.outlet(cout), wire.outlet(aout)
    out_x, out_y, out_z = wire.outlet(xs), wire.outlet(ys), wire.outlet(zs)
    swaps = {}
    for j in (1, 2, 0):
        loads_out[j].wait()
        swaps[j] = [wire.send(cout.at[j], cott.at[j, :, mine], me.partner(), out_cot)]
        parts = 2 if j == 1 else 1
        for k in range(parts):
            cols = pl.ds(k * (D // parts), D // parts)
            swaps[j].append(
                wire.send(aout.at[j, :, cols], actv.at[j, mine, cols], me.partner(), out_act)
            )

    def prepare(j):
        loads[j].wait()
        swaps[j][0].wait_recv()
        swaps[j][1].wait_recv()

    sent = {}

    def z_part(dest, half):
        columns = rows_at(dest * 256 + half * 128, 128)
        return jnp.dot(cott[0], actv[0, :, columns], preferred_element_type=f32)

    def z_send(half, d, n, k):
        part = z_part(wrap(z + d * (n + 1 - k), 8), half)
        slot = Z_BASE[half, d] + k - 1
        if k > 1:
            sent["z", half, d, k - 1].wait_recv()
            part += zr[slot - 1].astype(f32)
        zs[slot] = part.astype(bf16)
        sent["z", half, d, k] = wire.send(zs.at[slot], zr.at[slot], me.at(dz=d), out_z)

    def x_part(dest, half, i):
        columns = rows_at((4 * half + i) * 256, 256)
        return jnp.dot(cott[1, rows_at(dest * 128, 128), :], actv[1, :, columns], preferred_element_type=f32)

    def x_send(half, d, k):
        dest = wrap(x + d * (PAIR_STEPS[half, d] + 1 - k), 4)
        slot = PAIR_BASE[half, d] + k - 1
        if k > 1:
            sent["x", half, d, k - 1].wait_recv()

        def step(i, carry):
            part = x_part(dest, half, i)
            for t in range(2):
                value = part[:, t * 128 : (t + 1) * 128]
                if k > 1:
                    value += xr[slot - 1, 2 * i + t].astype(f32)
                xs[slot, 2 * i + t] = value.astype(bf16)
            return carry

        lax.fori_loop(0, 4, step, 0, unroll=True)
        sent["x", half, d, k] = wire.send(xs.at[slot], xr.at[slot], me.at(dx=d), out_x)

    def y_part(dest, half, i):
        columns = rows_at(((4 * half + i) * 2 + lax.rem(dest, 2)) * 128, 128)
        rows = rows_at(lax.div(dest, 2) * 256, 256)
        return jnp.dot(cott[2, rows, :], actv[2, :, columns], preferred_element_type=f32)

    def y_send(half, d, k):
        dest = wrap(y + d * (PAIR_STEPS[half, d] + 1 - k), 4)
        slot = PAIR_BASE[half, d] + k - 1
        if k > 1:
            sent["y", half, d, k - 1].wait_recv()

        def step(i, carry):
            value = y_part(dest, half, i)
            if k > 1:
                value += yr[slot - 1, i].astype(f32)
            ys[slot, i] = value.astype(bf16)
            return carry

        lax.fori_loop(0, 4, step, 0, unroll=True)
        sent["y", half, d, k] = wire.send(ys.at[slot], yr.at[slot], me.at_y(d), out_y)

    def z_round(k, long=None):
        for (half, d), n in Z_STEPS.items():
            if k <= n and long in (None, n == 4):
                z_send(half, d, n, k)

    phase("r_prep0")
    prepare(1)
    phase("r_x1")
    x_send(0, 1, 1)
    swaps[1][2].wait_recv()
    x_send(1, -1, 1)
    phase("r_y1")
    prepare(2)
    y_send(0, 1, 1)
    y_send(1, -1, 1)
    phase("r_z1")
    prepare(0)
    z_round(1)
    phase("r_xy1b")
    x_send(1, 1, 1)
    x_send(0, -1, 1)
    y_send(1, 1, 1)
    y_send(0, -1, 1)
    here = rows_at(me.column * 128, 128)

    def slot_matrix(p):
        found, seen, filled = jnp.int32(0), jnp.int32(0), jnp.int32(0)
        for m in range(MATS):
            named = (owners[m] == p).astype(jnp.int32)
            take = named * (seen == c).astype(jnp.int32)
            found, filled, seen = found + take * m, filled + take, seen + named
        return found, filled

    def note(p, carry):
        table[0, p], table[1, p] = slot_matrix(p)
        return carry

    def gather_columns(pieces, target):
        def choose(p, carry):
            found, filled = table[0, p], table[1, p]
            target[p] = (pieces[found].astype(f32) * filled.astype(f32)).astype(bf16)
            return carry

        lax.fori_loop(0, 16, choose, 0, unroll=2)

    phase("r_msend")
    load_momentum.wait()
    load_owners.wait()
    load_starts.wait()
    lax.fori_loop(0, 16, note, 0)
    gather_columns(mb, ms)
    own_half = rows_at(yh * 32, 32)
    mq[own_half, here] = ms[me.column]

    phase("r_z2")
    z_round(2, True)
    phase("r_x2")
    x_send(0, 1, 2)
    x_send(1, -1, 2)
    phase("r_y2")
    y_send(0, 1, 2)
    y_send(1, -1, 2)
    phase("r_z2b")
    z_round(2, False)
    phase("r_z3")
    z_round(3, True)
    z_round(3, False)
    phase("r_z4")
    z_round(4)
    copies = [(ms.at[p], mq.at[own_half, here], device) for device, p in me.columns()]
    momentum_to_owner = wire.group(copies, ms.at[:15])

    phase("r_xlast")
    def turned_z(to):
        return wrap(to - z - 2, 8)

    def third(second, buffer, arrived, here, store):
        for e in range(4 * second, 4 * second + 4):
            value = here(e).astype(f32)
            for d in range(3):
                value += arrived[second, d, e % 4].astype(f32)
            buffer[e] = value.astype(bf16)
        places = (2, 1, 3, 0) if second == 0 else (4, 7, 5)
        copies = [(buffer.at[e], store.at[e], me.at(dz=e + 2)) for e in places]
        return wire.group(copies, store.at[: len(places)])

    for half in range(2):
        sent["x", half, 1, PAIR_STEPS[half, 1]].wait_recv()
        sent["x", half, -1, PAIR_STEPS[half, -1]].wait_recv()
        up = PAIR_BASE[half, 1] + PAIR_STEPS[half, 1] - 1
        down = PAIR_BASE[half, -1] + PAIR_STEPS[half, -1] - 1

        def x_last(i, carry, half=half, up=up, down=down):
            part = x_part(x, half, i)
            for t in range(2):
                value = part[:, t * 128 : (t + 1) * 128]
                value += xr[up, 2 * i + t].astype(f32) + xr[down, 2 * i + t].astype(f32)
                x2s[t, turned_z(4 * half + i)] = value.astype(bf16)
            return carry

        lax.fori_loop(0, 4, x_last, 0, unroll=True)
    for second in range(2):
        copies = []
        for d in (1, 3, 2):
            to = wrap(y + d, 4)
            source = x2s.at[lax.rem(to, 2), pl.ds(4 * second, 4), rows_at(lax.div(to, 2) * 64, 64), :]
            copies.append((source, x2r.at[second, d - 1], me.at_y(d)))
        sent["x2", second] = wire.group(copies, x2r.at[second])

    phase("r_ylast")
    for half in range(2):
        sent["y", half, 1, PAIR_STEPS[half, 1]].wait_recv()
        sent["y", half, -1, PAIR_STEPS[half, -1]].wait_recv()
        up = PAIR_BASE[half, 1] + PAIR_STEPS[half, 1] - 1
        down = PAIR_BASE[half, -1] + PAIR_STEPS[half, -1] - 1

        def y_last(i, carry, half=half, up=up, down=down):
            value = y_part(y, half, i) + yr[up, i].astype(f32) + yr[down, i].astype(f32)
            y2s[turned_z(4 * half + i)] = value.astype(bf16)
            return carry

        lax.fori_loop(0, 4, y_last, 0, unroll=True)
    for second in range(2):
        copies = []
        for d in (1, 3, 2):
            source = y2s.at[pl.ds(4 * second, 4), rows_at(wrap(x + d, 4) * 64, 64), :]
            copies.append((source, y2r.at[second, d - 1], me.at(dx=d)))
        sent["y2", second] = wire.group(copies, y2r.at[second])

    phase("r_zlast")
    for half in range(2):
        last = []
        for d in (1, -1):
            n = Z_STEPS[half, d]
            sent["z", half, d, n].wait_recv()
            last.append(Z_BASE[half, d] + n - 1)
        value = z_part(z, half) + zr[last[0]].astype(f32) + zr[last[1]].astype(f32)
        z2s[half] = value.astype(bf16).reshape(4, 2, 64, 128)
    copies = []
    for d in (1, 3, 2):
        to = wrap(y + d, 4)
        copies.append((z2s.at[lax.rem(to, 2), :, lax.div(to, 2)], z2r.at[d - 1], me.at_y(d)))
    sent["z2"] = wire.group(copies, z2r)
    def z_second():
        phase("r_z3b")
        sent["z2"].wait_recv()
        for to in range(4):
            value = z2s[yl, to, yh].astype(f32)
            for d in range(3):
                value += z2r[d, to].astype(f32)
            z3s[to] = value.astype(bf16)
        copies = [(z3s.at[wrap(x + d, 4)], z3r.at[d - 1], me.at(dx=d)) for d in (2, 1, 3)]
        sent["z3"] = wire.group(copies, z3r)

    def x_here(e):
        return x2s[yl, e, rows_at(yh * 64, 64), :]

    def y_here(e):
        return y2s[e, rows_at(x * 64, 64), :]

    for second in range(2):
        phase("r_x3" + "ab"[second])
        sent["x2", second].wait_recv()
        sent["x3", second] = third(second, x3s, x2r, x_here, x3r)
        phase("r_y3" + "ab"[second])
        sent["y2", second].wait_recv()
        sent["y3", second] = third(second, y3s, y2r, y_here, y3r)
    z_second()
    momentum_to_owner.wait_recv()
    momentum_over = wire.send(mq.at[own_half], mq.at[own_half], me.near(0, 2, 0, 0))

    phase("r_xfin")
    inverse = 1.0 / math.sqrt(TOKENS)
    sqs[z] = jnp.zeros((8, 128), f32)

    def piece(j, value):
        value = value * inverse
        for kv in range(2):
            block = value[kv * 32 : (kv + 1) * 32]
            gb[6 * c + 2 * j + kv, rows, :] = block.astype(bf16)
            gp[6 * c + 2 * j + kv] = block.astype(bf16)
            total = jnp.sum(block * block, axis=(0, 1), keepdims=True)
            sqs[z, 2 * j + kv : 2 * j + kv + 1, :] = jnp.broadcast_to(total, (1, 128))

    sent["x3", 0].wait_recv()
    sent["x3", 1].wait_recv()
    value = x3s[6].astype(f32)
    for e in (0, 1, 2, 3, 4, 5, 7):
        value += x3r[e].astype(f32)
    piece(1, value)
    phase("r_yfin")
    sent["y3", 0].wait_recv()
    sent["y3", 1].wait_recv()
    value = y3s[6].astype(f32)
    for e in (0, 1, 2, 3, 4, 5, 7):
        value += y3r[e].astype(f32)
    piece(2, value)
    phase("r_zfin")
    sent["z3"].wait_recv()
    value = z3s[x].astype(f32)
    for d in range(3):
        value += z3r[d].astype(f32)
    piece(0, value)

    phase("r_sqsend")
    own = pl.ds(6 * c, 6)
    squares = wire.group([(sqs.at[z], sqs.at[z], me.at(dz=d)) for d in (4, 3, 5, 2, 6, 1, 7)], sqs.at[:7])
    swap = wire.send(gp.at[own], gp.at[own], me.partner())
    swap.wait_recv()
    gather_columns(gp, us)
    gq[own_half, here] = us[me.column]
    copies = []
    for dz in (4, 3, 5, 2, 6, 1, 7, 0):
        for dy in (2, 1, 3, 0):
            if dz or dy:
                device = me.near(0, dy, 0, dz)
                copies.append((us.at[2 * device[3] + device[4]], gq.at[own_half, here], device))
    to_owner = wire.group(copies, rb.at[:31])
    phase("r_sqw1b")
    squares.wait_recv()
    spot = c * 16 + 4 * x + y
    sq2[spot] = sum((sqs[i] for i in range(1, 8)), sqs[0])
    squares = wire.group(
        [(sq2.at[spot], sq2.at[spot], me.near(dx, dy, dc, 0)) for dx, dy, dc in plane], sq2.at[:31]
    )
    phase("r_sqw2")
    squares.wait_recv()
    totals = [sum((sq2[k * 16 + i] for i in range(1, 16)), sq2[k * 16]) for k in range(2)]
    totals = jnp.concatenate(totals, axis=0)
    phase("o_a2a")
    momentum_over.wait_recv()
    to_owner.wait_recv()
    phase("o_choose")

    row = lax.broadcasted_iota(jnp.int32, (16, 128), 0)
    matrix = jnp.where(row >= 8, row - 2, row)
    held = (row < 6) | ((row >= 8) & (row < 14))
    bucket = (matrix >= starts[0]).astype(jnp.int32) + (matrix >= starts[1]).astype(jnp.int32)
    factors = jnp.ones((16, 128), f32)
    for b in range(3):
        inside = held & (bucket == b)
        total = jnp.sum(jnp.where(inside, totals, 0.0), axis=0, keepdims=True)
        members = jnp.sum(inside.astype(f32), axis=0, keepdims=True)
        root_mean = jnp.sqrt(total / (members * (KV * D)) + epsilon)
        factors = jnp.where(inside, jnp.minimum(1.0, clip_level / root_mean), factors)
    f_out[...] = factors
    fac[...] = factors
    mine_is = table[0, me.column]
    factor = fac[pl.ds(mine_is + 2 * (mine_is >= 6).astype(jnp.int32), 1), :]
    for k in range(4):
        cols = slice(k * 512, (k + 1) * 512)
        scaled = factor[:, :1] * gq[:, cols].astype(f32)
        value = scaled + momentum_rate * (momentum_rate * mq[:, cols].astype(f32) + scaled)
        gin[rows_at(x * 64, 64), cols] = value.astype(bf16)

    phase("o_ag")

    def part(dx, h):
        return gin.at[rows_at(wrap(x + dx, 4) * 64 + 32 * h, 32), :]

    ahead, behind = me.at(dx=1), me.at(dx=-1)
    out_u = wire.outlet(gin.at[:192])
    first_up = wire.send(part(0, 0), part(0, 0), ahead, out_u)
    first_down = wire.send(part(0, 1), part(0, 1), behind, out_u)
    second_up = wire.send(part(0, 1), part(0, 1), ahead, out_u)
    second_down = wire.send(part(0, 0), part(0, 0), behind, out_u)
    first_up.wait_recv()
    third_up = wire.send(part(-1, 0), part(-1, 0), ahead, out_u)
    first_down.wait_recv()
    third_down = wire.send(part(1, 1), part(1, 1), behind, out_u)
    for copy in (second_up, second_down, third_up, third_down):
        copy.wait_recv()
    pieces = wire.group(
        [(gb.at[own, rows, :], gb.at[own, rows, :], device) for device in me.replicas()], gb.at[:6, :224, :]
    )

    phase("o_ns")
    orthogonalize(gin, xw, gram)

    phase("o_back")
    copies = [
        (xw.at[rows, rows_at(p * 128, 128)], rb.at[c * 16 + me.column], device) for device, p in me.columns()
    ]
    back = wire.group(copies, rb.at[:15])
    rb[c * 16 + me.column] = xw[rows, here]
    pieces.wait_recv()
    over_g = wire.send(gb.at[own], gb.at[own], me.partner())
    whole = wire.send(xw, o_out.at[c], me.partner())
    store = pltpu.make_async_copy(xw, o_out.at[c], local_sems.at[7])
    store.start()
    back.wait_recv()
    phase("o_over")
    slots = pl.ds(c * 16, 16)
    over = wire.send(rb.at[slots], rb.at[slots], me.partner())
    over.wait_recv()
    for k in range(6):
        m = 6 * c + k
        owner = owners[m]
        slot = jnp.int32(0)
        for j in range(MATS):
            slot = slot + (owners[j] == owner).astype(jnp.int32) * (j < m).astype(jnp.int32)
        ob[m, rows, :] = rb[jnp.minimum(slot, 1) * 16 + owner]
    phase("o_ag2")
    out_pieces = wire.outlet(ob.at[:6, :224])
    gathered = [wire.send(ob.at[own, rows, :], ob.at[own, rows, :], device, out_pieces) for device in me.replicas()]
    onward = wire.opened(ob.at[:6])
    wire.join(onward, [(ob.at[own, rows, :], ob.at[own, rows, :], me.partner())])
    over_g.wait_recv()
    store_g = pltpu.make_async_copy(gb, g_out, local_sems.at[8])
    store_g.start()
    for copy, (dx, dyh) in zip(gathered, me.offsets(), strict=True):
        copy.wait_recv()
        block = 2 * wrap(x - dx, 4) + lax.rem(yh + dyh, 2)
        arrived = ob.at[own, rows_at(block * 32, 32), :]
        wire.join(onward, [(arrived, arrived, me.partner())])
    phase("o_over2")
    onward.wait_recv()
    out = pltpu.make_async_copy(ob, upd_out, local_sems.at[9])
    out.start()
    phase("o_finish")
    whole.wait_recv()
    store.wait()
    store_g.wait()
    out.wait()
    wire.finish()
    phase.end()


def orthogonalize(xin, xw, gram):
    def outer(value):
        return lax.dot_general(value, value, (((1,), (1,)), ((), ())), preferred_element_type=f32)

    def iteration(x_of, last):
        rounded = gram[...].astype(bf16)
        square = jnp.dot(rounded, rounded, preferred_element_type=f32)
        mixing = (coef_b * rounded.astype(f32) + coef_c * square).astype(bf16)
        total = None
        for k in range(4):
            cols = slice(k * 512, (k + 1) * 512)
            old = x_of(cols)
            product = jnp.dot(mixing, old, preferred_element_type=f32)
            new = (coef_a * old.astype(f32) + product).astype(bf16)
            xw[:, cols] = new
            if not last:
                total = outer(new) if k == 0 else total + outer(new)
        if not last:
            gram[...] = total

    first = outer(xin[...])
    diagonal = lax.broadcasted_iota(jnp.int32, (KV, KV), 0) == lax.broadcasted_iota(jnp.int32, (KV, KV), 1)
    norm = jnp.sqrt(jnp.sum(jnp.where(diagonal, first, 0.0), axis=(0, 1), keepdims=True))
    scale = 1.0 / (norm + epsilon)
    gram[...] = first * scale * scale
    iteration(lambda cols: (xin[:, cols].astype(f32) * scale).astype(bf16), False)

    def middle(i, carry):
        iteration(lambda cols: xw[:, cols], False)
        return carry

    lax.fori_loop(0, ITERS - 2, middle, 0)
    iteration(lambda cols: xw[:, cols], True)


def stepped(activations, cotangents, momentum, owners, bucket_starts):
    vm = pltpu.VMEM
    operands = (owners, bucket_starts, activations, cotangents, momentum)
    operands = [pltpu.with_memory_space_constraint(a, pltpu.HBM) for a in operands]
    return pl.pallas_call(
        step_kernel,
        out_shape=(
            jax.ShapeDtypeStruct((MATS, KV, 128), bf16),
            jax.ShapeDtypeStruct((16, 128), f32),
            jax.ShapeDtypeStruct((MATS, KV, 128), bf16),
            jax.ShapeDtypeStruct((2, KV, D), bf16),
        ),
        in_specs=[pl.BlockSpec(memory_space=pltpu.HBM)] * 5,
        out_specs=(
            pl.BlockSpec(memory_space=pl.ANY),
            pl.BlockSpec(memory_space=pltpu.VMEM),
            pl.BlockSpec(memory_space=pl.ANY),
            pl.BlockSpec(memory_space=pl.ANY),
        ),
        scratch_shapes=[
            vm((6, 128, 512), bf16), vm((3, 512, 128), bf16), vm((3, 128, D), bf16), vm((3, 256, D), bf16), vm((3, 512, 256), bf16),
            vm((14, 512, 128), bf16), vm((14, 512, 128), bf16),
            vm((6, 8, 128, 128), bf16), vm((6, 8, 128, 128), bf16),
            vm((6, 4, 256, 128), bf16), vm((6, 4, 256, 128), bf16),
            vm((2, 4, 2, 64, 128), bf16), vm((3, 4, 64, 128), bf16), vm((4, 64, 128), bf16), vm((3, 64, 128), bf16),
            vm((2, 8, 128, 128), bf16), vm((2, 3, 4, 64, 128), bf16), vm((8, 64, 128), bf16), vm((8, 64, 128), bf16),
            vm((8, 256, 128), bf16), vm((2, 3, 4, 64, 128), bf16), vm((8, 64, 128), bf16), vm((8, 64, 128), bf16),
            vm((MATS, KV, 128), bf16), vm((MATS, 32, 128), bf16), vm((8, 8, 128), f32), vm((32, 8, 128), f32),
            vm((MATS, 32, 128), f32), vm((16, 32, 128), bf16), vm((16, 32, 128), bf16), vm((16, 128), f32),
            vm((64, D), bf16), vm((64, D), bf16), vm((KV, D), bf16), vm((KV, D), bf16), vm((32, 32, 128), bf16), vm((MATS, KV, 128), bf16),
            vm((KV, KV), f32),
            pltpu.SMEM((MATS,), jnp.int32), pltpu.SMEM((2,), jnp.int32), pltpu.SMEM((2, 16), jnp.int32),
            pltpu.SemaphoreType.DMA((13,)),
            pltpu.SemaphoreType.DMA((OUTLETS,)),
            pltpu.SemaphoreType.DMA((ARRIVALS,)),
        ],
        compiler_params=pltpu.CompilerParams(
            collective_id=0, has_side_effects=True, vmem_limit_bytes=48 * 1024 * 1024
        ),
        name="step",
    )(*operands)


def finish_kernel(factors, g, mom, x, whole, mom_out, update, owned, mv, uv, ov, sems):
    scale = math.sqrt(max(KV, D))
    copies = []

    def store(source, target):
        copy = pltpu.make_async_copy(source, target, sems.at[len(copies)])
        copy.start()
        copies.append(copy)

    for i in range(4):
        rows, mats = pl.ds(64 * i, 64), pl.ds(3 * i, 3)
        ov[:, rows] = (scale * whole[:, rows].astype(f32)).astype(bf16)
        store(ov.at[:, rows], owned.at[:, rows])
        for m in range(3 * i, 3 * i + 3):
            r = m if m < 6 else m + 2
            mv[m] = momentum_rate * mom[m] + factors[r : r + 1, :] * g[m].astype(f32)
        store(mv.at[mats], mom_out.at[mats])
        uv[mats] = scale * x[mats].astype(f32)
        store(uv.at[mats], update.at[mats])
    for copy in copies:
        copy.wait()


def finished(factors, g, mom, x, whole):
    return pl.pallas_call(
        finish_kernel,
        out_shape=(
            jax.ShapeDtypeStruct((MATS, KV, 128), f32),
            jax.ShapeDtypeStruct((MATS, KV, 128), f32),
            jax.ShapeDtypeStruct((2, KV, D), bf16),
        ),
        in_specs=[pl.BlockSpec(memory_space=pltpu.VMEM)] * 5,
        out_specs=[pl.BlockSpec(memory_space=pltpu.HBM)] * 3,
        scratch_shapes=[
            pltpu.VMEM((MATS, KV, 128), f32),
            pltpu.VMEM((MATS, KV, 128), f32),
            pltpu.VMEM((2, KV, D), bf16),
            pltpu.SemaphoreType.DMA((12,)),
        ],
        compiler_params=pltpu.CompilerParams(vmem_limit_bytes=16 * 1024 * 1024),
        name="finish",
    )(factors, g, mom, x, whole)


def per_device(activations, cotangents, momentum, owners, bucket_starts):
    g, factors, x, whole = stepped(activations, cotangents, momentum, owners, bucket_starts)
    return finished(factors, g, momentum, x, whole)


def solution(mesh):
    torus = Mesh(
        mesh.devices.reshape(4, 2, 2, 8, 2), ("rep_0", "rep_1", "rep_2", "shard_0", "shard_1")
    )
    return jax.shard_map(
        per_device,
        mesh=torus,
        in_specs=(
            P(None, REP_SHARD, None),
            P(None, REP_SHARD, None),
            P(None, None, SHARD),
            P(),
            P(),
        ),
        out_specs=(P(None, None, SHARD), P(None, None, SHARD), P(SHARD, None, None)),
        check_vma=False,
    )
```

```python
import functools
import math

import jax
import jax.numpy as jnp
from jax import lax
from jax.experimental import pallas as pl
from jax.experimental.pallas import tpu as pltpu
from jax.sharding import Mesh
from jax.sharding import PartitionSpec as P

D = 2048
KV = 256
ITERS = 5
MATS = 12
TOKENS = 32768
SHARD = ("shard_0", "shard_1")
REP_SHARD = ("rep_0", "rep_1", "rep_2", "shard_0", "shard_1")

coef_a = 3.4445
coef_b = -4.775
coef_c = 2.0315
momentum_rate = 0.95
clip_level = 0.5
epsilon = 1e-06

f32 = jnp.float32
bf16 = jnp.bfloat16
MESH = pl.DeviceIdType.MESH


def wrap(value, size):
    return lax.rem(value + 2 * size, size)


class Place:
    def __init__(self):
        self.x = lax.axis_index("rep_0")
        self.yh = lax.axis_index("rep_1")
        self.c = lax.axis_index("rep_2")
        self.z = lax.axis_index("shard_0")
        self.yl = lax.axis_index("shard_1")
        self.y = 2 * self.yh + self.yl
        self.block = 2 * self.x + self.yh
        self.column = 2 * self.z + self.yl

    def at(self, dx=0, dz=0):
        return (wrap(self.x + dx, 4), self.yh, self.c, wrap(self.z + dz, 8), self.yl)

    def at_y(self, dy):
        y = wrap(self.y + dy, 4)
        return (self.x, lax.div(y, 2), self.c, self.z, lax.rem(y, 2))

    def partner(self):
        return (self.x, self.yh, 1 - self.c, self.z, self.yl)

    def near(self, dx, dy, dc, dz):
        y = wrap(self.y + dy, 4)
        core = 1 - self.c if dc else self.c
        return (wrap(self.x + dx, 4), lax.div(y, 2), core, wrap(self.z + dz, 8), lax.rem(y, 2))

    def replicas(self):
        for dx, dyh in self.offsets():
            yield (wrap(self.x + dx, 4), lax.rem(self.yh + dyh, 2), self.c, self.z, self.yl)

    def offsets(self):
        return ((2, 1), (1, 1), (3, 1), (2, 0), (0, 1), (1, 0), (3, 0))

    def columns_at(self, dz):
        for dyl in range(2):
            if dz or dyl:
                z, yl = wrap(self.z + dz, 8), lax.rem(self.yl + dyl, 2)
                yield (self.x, self.yh, self.c, z, yl), 2 * z + yl

    def columns(self):
        for dz in (4, 3, 5, 2, 6, 1, 7, 0):
            yield from self.columns_at(dz)


class Wire:
    def __init__(self, send_sems, recv_sems, device):
        self.send_sems, self.recv_sems, self.device = send_sems, recv_sems, device
        self.n_send = self.n_recv = 0
        self.leaving, self.kept, self.numbers = [], [], {}

    def copy(self, source, target, s, r, device):
        return pltpu.make_async_remote_copy(
            src_ref=source,
            dst_ref=target,
            send_sem=self.send_sems.at[s],
            recv_sem=self.recv_sems.at[r],
            device_id=device,
            device_id_type=MESH,
        )

    def outlet(self, whole):
        self.n_send += 1
        self.leaving.append((self.n_send - 1, whole))
        return self.n_send - 1

    def send(self, source, target, device, s=None):
        if s is None:
            s = self.outlet(source)
        r = self.n_recv
        self.n_recv += 1
        copy = self.copy(source, target, s, r, device)
        copy.start()
        return copy

    def opened(self, whole):
        s, r = self.outlet(whole), self.n_recv
        self.n_recv += 1
        copy = self.copy(whole, whole, s, r, self.device)
        self.kept.append(copy)
        self.numbers[id(copy)] = (s, r)
        return copy

    def join(self, group, copies):
        for source, target, device in copies:
            self.copy(source, target, *self.numbers[id(group)], device).start()

    def group(self, copies, whole):
        group = self.opened(whole)
        self.join(group, copies)
        return group

    def finish(self):
        assert (self.n_send, self.n_recv) == (OUTLETS, ARRIVALS), (self.n_send, self.n_recv)
        for s, whole in self.leaving:
            self.copy(whole, whole, s, 0, self.device).wait_send()


def signal_all(devices):
    barrier = pltpu.get_barrier_semaphore()
    for device in devices:
        pl.semaphore_signal(barrier, inc=1, device_id=device, device_id_type=MESH)


class Phases:
    def __init__(self):
        self.open = None

    def __call__(self, name):
        self.end()
        self.open = jax.named_scope(name)
        self.open.__enter__()

    def end(self):
        if self.open:
            self.open.__exit__(None, None, None)
        self.open = None


def rows_at(start, size):
    return pl.ds(pl.multiple_of(start, size), size)


Z_STEPS = {(0, 1): 4, (1, -1): 4, (1, 1): 3, (0, -1): 3}
Z_BASE = {(0, 1): 0, (1, -1): 4, (1, 1): 8, (0, -1): 11}
PAIR_BASE = {(0, 1): 0, (1, -1): 2, (1, 1): 4, (0, -1): 5}
PAIR_STEPS = {(0, 1): 2, (1, -1): 2, (1, 1): 1, (0, -1): 1}
OUTLETS, ARRIVALS = 29, 68


def step_kernel(
    owners_in, starts_in, act, cot, mom, g_out, f_out, upd_out, o_out,
    cin, cout, aout, actv, cott, zs, zr, xs, xr, ys, yr,
    z2s, z2r, z3s, z3r, x2s, x2r, x3s, x3r, y2s, y2r, y3s, y3r,
    gb, gp, sqs, sq2, mb, us, ms, fac, gq, mq, gin, xw, rb, ob, gram, owners, starts, table, local_sems, send_sems, recv_sems,
):
    me = Place()
    x, y, yh, yl, z, c = me.x, me.y, me.yh, me.yl, me.z, me.c
    wire = Wire(send_sems, recv_sems, me.partner())
    phase = Phases()
    mine = rows_at(c * 128, 128)

    load_cot = pltpu.make_async_copy(cot, cin, local_sems.at[0])
    load_cot.start()
    loads, loads_out = [], []
    for j in range(3):
        loads_out.append(pltpu.make_async_copy(act.at[3 * (1 - c) + j], aout.at[j], local_sems.at[1 + j]))
        loads.append(pltpu.make_async_copy(act.at[3 * c + j], actv.at[j, mine], local_sems.at[4 + j]))
        loads_out[j].start()
        loads[j].start()
    rows = rows_at(me.block * 32, 32)
    load_momentum = pltpu.make_async_copy(mom.at[:, rows, :], mb, local_sems.at[12])
    load_momentum.start()
    load_owners = pltpu.make_async_copy(owners_in, owners, local_sems.at[10])
    load_starts = pltpu.make_async_copy(starts_in, starts, local_sems.at[11])
    load_owners.start()
    load_starts.start()

    phase("r_greet")
    plane = [(dx, dy, dc) for dx in range(4) for dy in range(4) for dc in range(2) if dx or dy or dc]
    devices = [me.partner()]
    devices += [me.near(d, 0, 0, 0) for d in range(1, 4)]
    devices += [me.near(0, d, 0, 0) for d in range(1, 4)]
    devices += [me.near(0, 0, 0, d) for d in range(1, 8)]
    devices += [(x, yh, c, wrap(z + d, 8), 1 - yl) for d in range(1, 8)]
    signal_all(devices)

    def turn(source, store, inner_is_x):
        turned = source.T
        for bx in range(4):
            for by in range(2):
                for kv in range(2):
                    at = kv * 256 + (bx * 2 + by) * 32
                    to = (by * 256 + bx * 64 if inner_is_x else bx * 128 + by * 64) + kv * 32
                    store(to, turned[at : at + 32, :])

    def turn_layer(j):
        def store_out(to, value, j=j):
            cout[j, to : to + 32, :] = value

        def store_own(to, value, j=j):
            cott[j, to : to + 32, mine] = value

        turn(cin[3 * (1 - c) + j], store_out, j == 2)
        turn(cin[3 * c + j], store_own, j == 2)

    load_cot.wait()
    turn_layer(1)
    phase("r_greetw")
    pl.semaphore_wait(pltpu.get_barrier_semaphore(), len(devices))
    phase("r_swap")
    out_cot, out_act = wire.outlet(cout), wire.outlet(aout)
    out_x, out_y, out_z = wire.outlet(xs), wire.outlet(ys), wire.outlet(zs)
    swaps = {}
    for j in (1, 2, 0):
        if j != 1:
            turn_layer(j)
        loads_out[j].wait()
        swaps[j] = [wire.send(cout.at[j], cott.at[j, :, mine], me.partner(), out_cot)]
        parts = 2 if j == 1 else 1
        for k in range(parts):
            cols = pl.ds(k * (D // parts), D // parts)
            swaps[j].append(
                wire.send(aout.at[j, :, cols], actv.at[j, mine, cols], me.partner(), out_act)
            )

    def prepare(j):
        loads[j].wait()
        swaps[j][0].wait_recv()
        swaps[j][1].wait_recv()

    sent = {}

    def z_part(dest, half):
        columns = rows_at(dest * 256 + half * 128, 128)
        return jnp.dot(cott[0], actv[0, :, columns], preferred_element_type=f32)

    def z_send(half, d, n, k):
        part = z_part(wrap(z + d * (n + 1 - k), 8), half)
        slot = Z_BASE[half, d] + k - 1
        if k > 1:
            sent["z", half, d, k - 1].wait_recv()
            part += zr[slot - 1].astype(f32)
        zs[slot] = part.astype(bf16)
        sent["z", half, d, k] = wire.send(zs.at[slot], zr.at[slot], me.at(dz=d), out_z)

    def x_part(dest, half, i):
        columns = rows_at((4 * half + i) * 256, 256)
        return jnp.dot(cott[1, rows_at(dest * 128, 128), :], actv[1, :, columns], preferred_element_type=f32)

    def x_send(half, d, k):
        dest = wrap(x + d * (PAIR_STEPS[half, d] + 1 - k), 4)
        slot = PAIR_BASE[half, d] + k - 1
        if k > 1:
            sent["x", half, d, k - 1].wait_recv()

        def step(i, carry):
            part = x_part(dest, half, i)
            for t in range(2):
                value = part[:, t * 128 : (t + 1) * 128]
                if k > 1:
                    value += xr[slot - 1, 2 * i + t].astype(f32)
                xs[slot, 2 * i + t] = value.astype(bf16)
            return carry

        lax.fori_loop(0, 4, step, 0, unroll=True)
        sent["x", half, d, k] = wire.send(xs.at[slot], xr.at[slot], me.at(dx=d), out_x)

    def y_part(dest, half, i):
        columns = rows_at(((4 * half + i) * 2 + lax.rem(dest, 2)) * 128, 128)
        rows = rows_at(lax.div(dest, 2) * 256, 256)
        return jnp.dot(cott[2, rows, :], actv[2, :, columns], preferred_element_type=f32)

    def y_send(half, d, k):
        dest = wrap(y + d * (PAIR_STEPS[half, d] + 1 - k), 4)
        slot = PAIR_BASE[half, d] + k - 1
        if k > 1:
            sent["y", half, d, k - 1].wait_recv()

        def step(i, carry):
            value = y_part(dest, half, i)
            if k > 1:
                value += yr[slot - 1, i].astype(f32)
            ys[slot, i] = value.astype(bf16)
            return carry

        lax.fori_loop(0, 4, step, 0, unroll=True)
        sent["y", half, d, k] = wire.send(ys.at[slot], yr.at[slot], me.at_y(d), out_y)

    def z_round(k, long=None):
        for (half, d), n in Z_STEPS.items():
            if k <= n and long in (None, n == 4):
                z_send(half, d, n, k)

    phase("r_prep0")
    prepare(1)
    phase("r_x1")
    x_send(0, 1, 1)
    swaps[1][2].wait_recv()
    x_send(1, -1, 1)
    phase("r_y1")
    prepare(2)
    y_send(0, 1, 1)
    y_send(1, -1, 1)
    phase("r_z1")
    prepare(0)
    z_round(1)
    phase("r_xy1b")
    x_send(1, 1, 1)
    x_send(0, -1, 1)
    y_send(1, 1, 1)
    y_send(0, -1, 1)
    here = rows_at(me.column * 128, 128)

    def slot_matrix(p):
        found, seen, filled = jnp.int32(0), jnp.int32(0), jnp.int32(0)
        for m in range(MATS):
            named = (owners[m] == p).astype(jnp.int32)
            take = named * (seen == c).astype(jnp.int32)
            found, filled, seen = found + take * m, filled + take, seen + named
        return found, filled

    def note(p, carry):
        table[0, p], table[1, p] = slot_matrix(p)
        return carry

    def gather_columns(pieces, target):
        def choose(p, carry):
            found, filled = table[0, p], table[1, p]
            target[p] = (pieces[found].astype(f32) * filled.astype(f32)).astype(bf16)
            return carry

        lax.fori_loop(0, 16, choose, 0, unroll=2)

    phase("r_msend")
    load_momentum.wait()
    load_owners.wait()
    load_starts.wait()
    lax.fori_loop(0, 16, note, 0)
    gather_columns(mb, ms)
    own_half = rows_at(yh * 32, 32)
    mq[own_half, here] = ms[me.column]

    phase("r_z2")
    z_round(2, True)
    phase("r_x2")
    x_send(0, 1, 2)
    x_send(1, -1, 2)
    phase("r_y2")
    y_send(0, 1, 2)
    y_send(1, -1, 2)
    phase("r_z2b")
    z_round(2, False)
    phase("r_z3")
    z_round(3, True)
    z_round(3, False)
    phase("r_z4")
    z_round(4)
    copies = [(ms.at[p], mq.at[own_half, here], device) for device, p in me.columns()]
    momentum_to_owner = wire.group(copies, ms.at[:15])

    phase("r_xlast")
    def turned_z(to):
        return wrap(to - z - 2, 8)

    def third(second, buffer, arrived, here, store):
        for e in range(4 * second, 4 * second + 4):
            value = here(e).astype(f32)
            for d in range(3):
                value += arrived[second, d, e % 4].astype(f32)
            buffer[e] = value.astype(bf16)
        places = (2, 1, 3, 0) if second == 0 else (4, 7, 5)
        copies = [(buffer.at[e], store.at[e], me.at(dz=e + 2)) for e in places]
        return wire.group(copies, store.at[: len(places)])

    for half in range(2):
        sent["x", half, 1, PAIR_STEPS[half, 1]].wait_recv()
        sent["x", half, -1, PAIR_STEPS[half, -1]].wait_recv()
        up = PAIR_BASE[half, 1] + PAIR_STEPS[half, 1] - 1
        down = PAIR_BASE[half, -1] + PAIR_STEPS[half, -1] - 1

        def x_last(i, carry, half=half, up=up, down=down):
            part = x_part(x, half, i)
            for t in range(2):
                value = part[:, t * 128 : (t + 1) * 128]
                value += xr[up, 2 * i + t].astype(f32) + xr[down, 2 * i + t].astype(f32)
                x2s[t, turned_z(4 * half + i)] = value.astype(bf16)
            return carry

        lax.fori_loop(0, 4, x_last, 0, unroll=True)
    for second in range(2):
        copies = []
        for d in (2, 1, 3):
            to = wrap(y + d, 4)
            source = x2s.at[lax.rem(to, 2), pl.ds(4 * second, 4), rows_at(lax.div(to, 2) * 64, 64), :]
            copies.append((source, x2r.at[second, d - 1], me.at_y(d)))
        sent["x2", second] = wire.group(copies, x2r.at[second])

    phase("r_ylast")
    for half in range(2):
        sent["y", half, 1, PAIR_STEPS[half, 1]].wait_recv()
        sent["y", half, -1, PAIR_STEPS[half, -1]].wait_recv()
        up = PAIR_BASE[half, 1] + PAIR_STEPS[half, 1] - 1
        down = PAIR_BASE[half, -1] + PAIR_STEPS[half, -1] - 1

        def y_last(i, carry, half=half, up=up, down=down):
            value = y_part(y, half, i) + yr[up, i].astype(f32) + yr[down, i].astype(f32)
            y2s[turned_z(4 * half + i)] = value.astype(bf16)
            return carry

        lax.fori_loop(0, 4, y_last, 0, unroll=True)
    for second in range(2):
        copies = []
        for d in (2, 1, 3):
            source = y2s.at[pl.ds(4 * second, 4), rows_at(wrap(x + d, 4) * 64, 64), :]
            copies.append((source, y2r.at[second, d - 1], me.at(dx=d)))
        sent["y2", second] = wire.group(copies, y2r.at[second])

    phase("r_zlast")
    for half in range(2):
        last = []
        for d in (1, -1):
            n = Z_STEPS[half, d]
            sent["z", half, d, n].wait_recv()
            last.append(Z_BASE[half, d] + n - 1)
        value = z_part(z, half) + zr[last[0]].astype(f32) + zr[last[1]].astype(f32)
        z2s[half] = value.astype(bf16).reshape(4, 2, 64, 128)
    copies = []
    for d in (1, 3, 2):
        to = wrap(y + d, 4)
        copies.append((z2s.at[lax.rem(to, 2), :, lax.div(to, 2)], z2r.at[d - 1], me.at_y(d)))
    sent["z2"] = wire.group(copies, z2r)
    def z_second():
        phase("r_z3b")
        sent["z2"].wait_recv()
        for to in range(4):
            value = z2s[yl, to, yh].astype(f32)
            for d in range(3):
                value += z2r[d, to].astype(f32)
            z3s[to] = value.astype(bf16)
        copies = [(z3s.at[wrap(x + d, 4)], z3r.at[d - 1], me.at(dx=d)) for d in (2, 1, 3)]
        sent["z3"] = wire.group(copies, z3r)

    def x_here(e):
        return x2s[yl, e, rows_at(yh * 64, 64), :]

    def y_here(e):
        return y2s[e, rows_at(x * 64, 64), :]

    for second in range(2):
        phase("r_x3" + "ab"[second])
        sent["x2", second].wait_recv()
        sent["x3", second] = third(second, x3s, x2r, x_here, x3r)
        phase("r_y3" + "ab"[second])
        sent["y2", second].wait_recv()
        sent["y3", second] = third(second, y3s, y2r, y_here, y3r)
    z_second()
    momentum_to_owner.wait_recv()
    momentum_over = wire.send(mq.at[own_half], mq.at[own_half], me.near(0, 2, 0, 0))

    phase("r_xfin")
    inverse = 1.0 / math.sqrt(TOKENS)
    sqs[z] = jnp.zeros((8, 128), f32)

    def piece(j, value):
        value = value * inverse
        for kv in range(2):
            block = value[kv * 32 : (kv + 1) * 32]
            gb[6 * c + 2 * j + kv, rows, :] = block.astype(bf16)
            gp[6 * c + 2 * j + kv] = block.astype(bf16)
            total = jnp.sum(block * block, axis=(0, 1), keepdims=True)
            sqs[z, 2 * j + kv : 2 * j + kv + 1, :] = jnp.broadcast_to(total, (1, 128))

    sent["x3", 0].wait_recv()
    sent["x3", 1].wait_recv()
    value = x3s[6].astype(f32)
    for e in (0, 1, 2, 3, 4, 5, 7):
        value += x3r[e].astype(f32)
    piece(1, value)
    phase("r_yfin")
    sent["y3", 0].wait_recv()
    sent["y3", 1].wait_recv()
    value = y3s[6].astype(f32)
    for e in (0, 1, 2, 3, 4, 5, 7):
        value += y3r[e].astype(f32)
    piece(2, value)
    phase("r_zfin")
    sent["z3"].wait_recv()
    value = z3s[x].astype(f32)
    for d in range(3):
        value += z3r[d].astype(f32)
    piece(0, value)

    phase("r_sqsend")
    own = pl.ds(6 * c, 6)
    squares = wire.group([(sqs.at[z], sqs.at[z], me.at(dz=d)) for d in (4, 3, 5, 2, 6, 1, 7)], sqs.at[:7])
    swap = wire.send(gp.at[own], gp.at[own], me.partner())
    swap.wait_recv()
    gather_columns(gp, us)
    gq[own_half, here] = us[me.column]
    copies = []
    for dz in (4, 3, 5, 2, 6, 1, 7, 0):
        for dy in (2, 1, 3, 0):
            if dz or dy:
                device = me.near(0, dy, 0, dz)
                copies.append((us.at[2 * device[3] + device[4]], gq.at[own_half, here], device))
    to_owner = wire.group(copies, rb.at[:31])
    phase("r_sqw1b")
    squares.wait_recv()
    spot = c * 16 + 4 * x + y
    farthest = sorted(plane, key=lambda d: -min(d[0], 4 - d[0]) - min(d[1], 4 - d[1]))
    sq2[spot] = sum((sqs[i] for i in range(1, 8)), sqs[0])
    squares = wire.group(
        [(sq2.at[spot], sq2.at[spot], me.near(dx, dy, dc, 0)) for dx, dy, dc in farthest], sq2.at[:31]
    )
    phase("r_sqw2")
    squares.wait_recv()
    totals = [sum((sq2[k * 16 + i] for i in range(1, 16)), sq2[k * 16]) for k in range(2)]
    totals = jnp.concatenate(totals, axis=0)
    phase("o_a2a")
    momentum_over.wait_recv()
    to_owner.wait_recv()
    phase("o_choose")

    row = lax.broadcasted_iota(jnp.int32, (16, 128), 0)
    matrix = jnp.where(row >= 8, row - 2, row)
    held = (row < 6) | ((row >= 8) & (row < 14))
    bucket = (matrix >= starts[0]).astype(jnp.int32) + (matrix >= starts[1]).astype(jnp.int32)
    factors = jnp.ones((16, 128), f32)
    for b in range(3):
        inside = held & (bucket == b)
        total = jnp.sum(jnp.where(inside, totals, 0.0), axis=0, keepdims=True)
        members = jnp.sum(inside.astype(f32), axis=0, keepdims=True)
        root_mean = jnp.sqrt(total / (members * (KV * D)) + epsilon)
        factors = jnp.where(inside, jnp.minimum(1.0, clip_level / root_mean), factors)
    f_out[...] = factors
    fac[...] = factors
    mine_is = table[0, me.column]
    factor = fac[pl.ds(mine_is + 2 * (mine_is >= 6).astype(jnp.int32), 1), :]
    for k in range(4):
        cols = slice(k * 512, (k + 1) * 512)
        scaled = factor[:, :1] * gq[:, cols].astype(f32)
        value = scaled + momentum_rate * (momentum_rate * mq[:, cols].astype(f32) + scaled)
        gin[rows_at(x * 64, 64), cols] = value.astype(bf16)

    phase("o_ag")

    def part(dx, h):
        return gin.at[rows_at(wrap(x + dx, 4) * 64 + 32 * h, 32), :]

    ahead, behind = me.at(dx=1), me.at(dx=-1)
    out_u = wire.outlet(gin.at[:192])
    first_up = wire.send(part(0, 0), part(0, 0), ahead, out_u)
    first_down = wire.send(part(0, 1), part(0, 1), behind, out_u)
    second_up = wire.send(part(0, 1), part(0, 1), ahead, out_u)
    second_down = wire.send(part(0, 0), part(0, 0), behind, out_u)
    first_up.wait_recv()
    third_up = wire.send(part(-1, 0), part(-1, 0), ahead, out_u)
    first_down.wait_recv()
    third_down = wire.send(part(1, 1), part(1, 1), behind, out_u)
    for copy in (second_up, second_down, third_up, third_down):
        copy.wait_recv()
    pieces = wire.group(
        [(gb.at[own, rows, :], gb.at[own, rows, :], device) for device in me.replicas()], gb.at[:6, :224, :]
    )

    phase("o_ns")
    orthogonalize(gin, xw, gram)

    phase("o_back")
    copies = [
        (xw.at[rows, rows_at(p * 128, 128)], rb.at[c * 16 + me.column], device) for device, p in me.columns()
    ]
    back = wire.group(copies, rb.at[:15])
    rb[c * 16 + me.column] = xw[rows, here]
    pieces.wait_recv()
    over_g = wire.send(gb.at[own], gb.at[own], me.partner())
    whole = wire.send(xw, o_out.at[c], me.partner())
    store = pltpu.make_async_copy(xw, o_out.at[c], local_sems.at[7])
    store.start()
    back.wait_recv()
    phase("o_over")
    slots = pl.ds(c * 16, 16)
    over = wire.send(rb.at[slots], rb.at[slots], me.partner())
    over.wait_recv()
    for k in range(6):
        m = 6 * c + k
        owner = owners[m]
        slot = jnp.int32(0)
        for j in range(MATS):
            slot = slot + (owners[j] == owner).astype(jnp.int32) * (j < m).astype(jnp.int32)
        ob[m, rows, :] = rb[jnp.minimum(slot, 1) * 16 + owner]
    phase("o_ag2")
    out_pieces = wire.outlet(ob.at[:6, :224])
    gathered = [wire.send(ob.at[own, rows, :], ob.at[own, rows, :], device, out_pieces) for device in me.replicas()]
    onward = wire.opened(ob.at[:6])
    wire.join(onward, [(ob.at[own, rows, :], ob.at[own, rows, :], me.partner())])
    over_g.wait_recv()
    store_g = pltpu.make_async_copy(gb, g_out, local_sems.at[8])
    store_g.start()
    for copy, (dx, dyh) in zip(gathered, me.offsets(), strict=True):
        copy.wait_recv()
        block = 2 * wrap(x - dx, 4) + lax.rem(yh + dyh, 2)
        arrived = ob.at[own, rows_at(block * 32, 32), :]
        wire.join(onward, [(arrived, arrived, me.partner())])
    phase("o_over2")
    onward.wait_recv()
    out = pltpu.make_async_copy(ob, upd_out, local_sems.at[9])
    out.start()
    phase("o_finish")
    whole.wait_recv()
    store.wait()
    store_g.wait()
    out.wait()
    wire.finish()
    phase.end()


def orthogonalize(xin, xw, gram):
    def outer(value):
        return lax.dot_general(value, value, (((1,), (1,)), ((), ())), preferred_element_type=f32)

    def iteration(x_of, last):
        rounded = gram[...].astype(bf16)
        square = jnp.dot(rounded, rounded, preferred_element_type=f32)
        mixing = (coef_b * rounded.astype(f32) + coef_c * square).astype(bf16)
        total = None
        for k in range(4):
            cols = slice(k * 512, (k + 1) * 512)
            old = x_of(cols)
            product = jnp.dot(mixing, old, preferred_element_type=f32)
            new = (coef_a * old.astype(f32) + product).astype(bf16)
            xw[:, cols] = new
            if not last:
                total = outer(new) if k == 0 else total + outer(new)
        if not last:
            gram[...] = total

    first = outer(xin[...])
    diagonal = lax.broadcasted_iota(jnp.int32, (KV, KV), 0) == lax.broadcasted_iota(jnp.int32, (KV, KV), 1)
    norm = jnp.sqrt(jnp.sum(jnp.where(diagonal, first, 0.0), axis=(0, 1), keepdims=True))
    scale = 1.0 / (norm + epsilon)
    gram[...] = first * scale * scale
    iteration(lambda cols: (xin[:, cols].astype(f32) * scale).astype(bf16), False)

    def middle(i, carry):
        iteration(lambda cols: xw[:, cols], False)
        return carry

    lax.fori_loop(0, ITERS - 2, middle, 0)
    iteration(lambda cols: xw[:, cols], True)


def stepped(activations, cotangents, momentum, owners, bucket_starts):
    vm = pltpu.VMEM
    operands = (owners, bucket_starts, activations, cotangents, momentum)
    operands = [pltpu.with_memory_space_constraint(a, pltpu.HBM) for a in operands]
    return pl.pallas_call(
        step_kernel,
        out_shape=(
            jax.ShapeDtypeStruct((MATS, KV, 128), bf16),
            jax.ShapeDtypeStruct((16, 128), f32),
            jax.ShapeDtypeStruct((MATS, KV, 128), bf16),
            jax.ShapeDtypeStruct((2, KV, D), bf16),
        ),
        in_specs=[pl.BlockSpec(memory_space=pltpu.HBM)] * 5,
        out_specs=(
            pl.BlockSpec(memory_space=pl.ANY),
            pl.BlockSpec(memory_space=pltpu.VMEM),
            pl.BlockSpec(memory_space=pl.ANY),
            pl.BlockSpec(memory_space=pl.ANY),
        ),
        scratch_shapes=[
            vm((6, 128, 512), bf16), vm((3, 512, 128), bf16), vm((3, 128, D), bf16), vm((3, 256, D), bf16), vm((3, 512, 256), bf16),
            vm((14, 512, 128), bf16), vm((14, 512, 128), bf16),
            vm((6, 8, 128, 128), bf16), vm((6, 8, 128, 128), bf16),
            vm((6, 4, 256, 128), bf16), vm((6, 4, 256, 128), bf16),
            vm((2, 4, 2, 64, 128), bf16), vm((3, 4, 64, 128), bf16), vm((4, 64, 128), bf16), vm((3, 64, 128), bf16),
            vm((2, 8, 128, 128), bf16), vm((2, 3, 4, 64, 128), bf16), vm((8, 64, 128), bf16), vm((8, 64, 128), bf16),
            vm((8, 256, 128), bf16), vm((2, 3, 4, 64, 128), bf16), vm((8, 64, 128), bf16), vm((8, 64, 128), bf16),
            vm((MATS, KV, 128), bf16), vm((MATS, 32, 128), bf16), vm((8, 8, 128), f32), vm((32, 8, 128), f32),
            vm((MATS, 32, 128), f32), vm((16, 32, 128), bf16), vm((16, 32, 128), bf16), vm((16, 128), f32),
            vm((64, D), bf16), vm((64, D), bf16), vm((KV, D), bf16), vm((KV, D), bf16), vm((32, 32, 128), bf16), vm((MATS, KV, 128), bf16),
            vm((KV, KV), f32),
            pltpu.SMEM((MATS,), jnp.int32), pltpu.SMEM((2,), jnp.int32), pltpu.SMEM((2, 16), jnp.int32),
            pltpu.SemaphoreType.DMA((13,)),
            pltpu.SemaphoreType.DMA((OUTLETS,)),
            pltpu.SemaphoreType.DMA((ARRIVALS,)),
        ],
        compiler_params=pltpu.CompilerParams(
            collective_id=0, has_side_effects=True, vmem_limit_bytes=48 * 1024 * 1024
        ),
        name="step",
    )(*operands)


def finish_kernel(factors, g, mom, x, whole, mom_out, update, owned, mv, uv, ov, sems):
    scale = math.sqrt(max(KV, D))
    copies = []

    def store(source, target):
        copy = pltpu.make_async_copy(source, target, sems.at[len(copies)])
        copy.start()
        copies.append(copy)

    for i in range(4):
        rows, mats = pl.ds(64 * i, 64), pl.ds(3 * i, 3)
        ov[:, rows] = (scale * whole[:, rows].astype(f32)).astype(bf16)
        store(ov.at[:, rows], owned.at[:, rows])
        for m in range(3 * i, 3 * i + 3):
            r = m if m < 6 else m + 2
            mv[m] = momentum_rate * mom[m] + factors[r : r + 1, :] * g[m].astype(f32)
        store(mv.at[mats], mom_out.at[mats])
        uv[mats] = scale * x[mats].astype(f32)
        store(uv.at[mats], update.at[mats])
    for copy in copies:
        copy.wait()


def finished(factors, g, mom, x, whole):
    return pl.pallas_call(
        finish_kernel,
        out_shape=(
            jax.ShapeDtypeStruct((MATS, KV, 128), f32),
            jax.ShapeDtypeStruct((MATS, KV, 128), f32),
            jax.ShapeDtypeStruct((2, KV, D), bf16),
        ),
        in_specs=[pl.BlockSpec(memory_space=pltpu.VMEM)] * 5,
        out_specs=[pl.BlockSpec(memory_space=pltpu.HBM)] * 3,
        scratch_shapes=[
            pltpu.VMEM((MATS, KV, 128), f32),
            pltpu.VMEM((MATS, KV, 128), f32),
            pltpu.VMEM((2, KV, D), bf16),
            pltpu.SemaphoreType.DMA((12,)),
        ],
        compiler_params=pltpu.CompilerParams(vmem_limit_bytes=16 * 1024 * 1024),
        name="finish",
    )(factors, g, mom, x, whole)


def per_device(activations, cotangents, momentum, owners, bucket_starts):
    g, factors, x, whole = stepped(activations, cotangents, momentum, owners, bucket_starts)
    return finished(factors, g, momentum, x, whole)


def solution(mesh):
    torus = Mesh(
        mesh.devices.reshape(4, 2, 2, 8, 2), ("rep_0", "rep_1", "rep_2", "shard_0", "shard_1")
    )
    return jax.shard_map(
        per_device,
        mesh=torus,
        in_specs=(
            P(None, REP_SHARD, None),
            P(None, REP_SHARD, None),
            P(None, None, SHARD),
            P(),
            P(),
        ),
        out_specs=(P(None, None, SHARD), P(None, None, SHARD), P(SHARD, None, None)),
        check_vma=False,
    )
```

```python
import functools
import math

import jax
import jax.numpy as jnp
from jax import lax
from jax.experimental import pallas as pl
from jax.experimental.pallas import tpu as pltpu
from jax.sharding import Mesh
from jax.sharding import PartitionSpec as P

D = 2048
KV = 256
ITERS = 5
MATS = 12
TOKENS = 32768
SHARD = ("shard_0", "shard_1")
REP_SHARD = ("rep_0", "rep_1", "rep_2", "shard_0", "shard_1")

coef_a = 3.4445
coef_b = -4.775
coef_c = 2.0315
momentum_rate = 0.95
clip_level = 0.5
epsilon = 1e-06

f32 = jnp.float32
bf16 = jnp.bfloat16
MESH = pl.DeviceIdType.MESH


def wrap(value, size):
    return lax.rem(value + 2 * size, size)


class Place:
    def __init__(self):
        self.x = lax.axis_index("rep_0")
        self.yh = lax.axis_index("rep_1")
        self.c = lax.axis_index("rep_2")
        self.z = lax.axis_index("shard_0")
        self.yl = lax.axis_index("shard_1")
        self.y = 2 * self.yh + self.yl
        self.block = 2 * self.x + self.yh
        self.column = 2 * self.z + self.yl

    def at(self, dx=0, dz=0):
        return (wrap(self.x + dx, 4), self.yh, self.c, wrap(self.z + dz, 8), self.yl)

    def at_y(self, dy):
        y = wrap(self.y + dy, 4)
        return (self.x, lax.div(y, 2), self.c, self.z, lax.rem(y, 2))

    def partner(self):
        return (self.x, self.yh, 1 - self.c, self.z, self.yl)

    def near(self, dx, dy, dc, dz):
        y = wrap(self.y + dy, 4)
        core = 1 - self.c if dc else self.c
        return (wrap(self.x + dx, 4), lax.div(y, 2), core, wrap(self.z + dz, 8), lax.rem(y, 2))

    def replicas(self):
        for dx, dyh in self.offsets():
            yield (wrap(self.x + dx, 4), lax.rem(self.yh + dyh, 2), self.c, self.z, self.yl)

    def offsets(self):
        return ((2, 1), (1, 1), (3, 1), (2, 0), (0, 1), (1, 0), (3, 0))

    def columns_at(self, dz):
        for dyl in range(2):
            if dz or dyl:
                z, yl = wrap(self.z + dz, 8), lax.rem(self.yl + dyl, 2)
                yield (self.x, self.yh, self.c, z, yl), 2 * z + yl

    def columns(self):
        for dz in (4, 3, 5, 2, 6, 1, 7, 0):
            yield from self.columns_at(dz)


class Wire:
    def __init__(self, send_sems, recv_sems, device):
        self.send_sems, self.recv_sems, self.device = send_sems, recv_sems, device
        self.n_send = self.n_recv = 0
        self.leaving, self.kept, self.numbers = [], [], {}

    def copy(self, source, target, s, r, device):
        return pltpu.make_async_remote_copy(
            src_ref=source,
            dst_ref=target,
            send_sem=self.send_sems.at[s],
            recv_sem=self.recv_sems.at[r],
            device_id=device,
            device_id_type=MESH,
        )

    def outlet(self, whole):
        self.n_send += 1
        self.leaving.append((self.n_send - 1, whole))
        return self.n_send - 1

    def send(self, source, target, device, s=None):
        if s is None:
            s = self.outlet(source)
        r = self.n_recv
        self.n_recv += 1
        copy = self.copy(source, target, s, r, device)
        copy.start()
        return copy

    def opened(self, whole):
        s, r = self.outlet(whole), self.n_recv
        self.n_recv += 1
        copy = self.copy(whole, whole, s, r, self.device)
        self.kept.append(copy)
        self.numbers[id(copy)] = (s, r)
        return copy

    def join(self, group, copies):
        for source, target, device in copies:
            self.copy(source, target, *self.numbers[id(group)], device).start()

    def group(self, copies, whole):
        group = self.opened(whole)
        self.join(group, copies)
        return group

    def finish(self):
        assert (self.n_send, self.n_recv) == (OUTLETS, ARRIVALS), (self.n_send, self.n_recv)
        for s, whole in self.leaving:
            self.copy(whole, whole, s, 0, self.device).wait_send()


def signal_all(devices):
    barrier = pltpu.get_barrier_semaphore()
    for device in devices:
        pl.semaphore_signal(barrier, inc=1, device_id=device, device_id_type=MESH)


class Phases:
    def __init__(self):
        self.open = None

    def __call__(self, name):
        self.end()
        self.open = jax.named_scope(name)
        self.open.__enter__()

    def end(self):
        if self.open:
            self.open.__exit__(None, None, None)
        self.open = None


def rows_at(start, size):
    return pl.ds(pl.multiple_of(start, size), size)


Z_STEPS = {(0, 1): 4, (1, -1): 4, (1, 1): 3, (0, -1): 3}
Z_BASE = {(0, 1): 0, (1, -1): 4, (1, 1): 8, (0, -1): 11}
PAIR_BASE = {(0, 1): 0, (1, -1): 2, (1, 1): 4, (0, -1): 5}
PAIR_STEPS = {(0, 1): 2, (1, -1): 2, (1, 1): 1, (0, -1): 1}
OUTLETS, ARRIVALS = 29, 69


def step_kernel(
    owners_in, starts_in, act, cot, mom, g_out, f_out, upd_out, o_out,
    cin, cout, aout, actv, cott, zs, zr, xs, xr, ys, yr,
    z2s, z2r, z3s, z3r, x2s, x2r, x3s, x3r, y2s, y2r, y3s, y3r,
    gb, gp, sqs, sq2, mb, us, ms, fac, gq, mq, gin, xw, rb, ob, gram, owners, starts, table, local_sems, send_sems, recv_sems,
):
    me = Place()
    x, y, yh, yl, z, c = me.x, me.y, me.yh, me.yl, me.z, me.c
    wire = Wire(send_sems, recv_sems, me.partner())
    phase = Phases()
    mine = rows_at(c * 128, 128)

    load_cot = pltpu.make_async_copy(cot, cin, local_sems.at[0])
    load_cot.start()
    loads, loads_out = [], []
    for j in range(3):
        loads_out.append(pltpu.make_async_copy(act.at[3 * (1 - c) + j], aout.at[j], local_sems.at[1 + j]))
        loads.append(pltpu.make_async_copy(act.at[3 * c + j], actv.at[j, mine], local_sems.at[4 + j]))
        loads_out[j].start()
        loads[j].start()
    rows = rows_at(me.block * 32, 32)
    load_momentum = pltpu.make_async_copy(mom.at[:, rows, :], mb, local_sems.at[12])
    load_momentum.start()
    load_owners = pltpu.make_async_copy(owners_in, owners, local_sems.at[10])
    load_starts = pltpu.make_async_copy(starts_in, starts, local_sems.at[11])
    load_owners.start()
    load_starts.start()

    phase("r_greet")
    plane = [(dx, dy, dc) for dx in range(4) for dy in range(4) for dc in range(2) if dx or dy or dc]
    devices = [me.partner()]
    devices += [me.near(d, 0, 0, 0) for d in range(1, 4)]
    devices += [me.near(0, d, 0, 0) for d in range(1, 4)]
    devices += [me.near(0, 0, 0, d) for d in range(1, 8)]
    devices += [(x, yh, c, wrap(z + d, 8), 1 - yl) for d in range(1, 8)]
    signal_all(devices)

    def turn(source, store, inner_is_x):
        turned = source.T
        for bx in range(4):
            for by in range(2):
                for kv in range(2):
                    at = kv * 256 + (bx * 2 + by) * 32
                    to = (by * 256 + bx * 64 if inner_is_x else bx * 128 + by * 64) + kv * 32
                    store(to, turned[at : at + 32, :])

    def turn_layer(j):
        def store_out(to, value, j=j):
            cout[j, to : to + 32, :] = value

        def store_own(to, value, j=j):
            cott[j, to : to + 32, mine] = value

        turn(cin[3 * (1 - c) + j], store_out, j == 2)
        turn(cin[3 * c + j], store_own, j == 2)

    load_cot.wait()
    turn_layer(1)
    phase("r_greetw")
    pl.semaphore_wait(pltpu.get_barrier_semaphore(), len(devices))
    phase("r_swap")
    out_cot, out_act = wire.outlet(cout), wire.outlet(aout)
    out_x, out_y, out_z = wire.outlet(xs), wire.outlet(ys), wire.outlet(zs)
    swaps = {}
    for j in (1, 2, 0):
        if j != 1:
            turn_layer(j)
        loads_out[j].wait()
        swaps[j] = [wire.send(cout.at[j], cott.at[j, :, mine], me.partner(), out_cot)]
        parts = 2 if j else 1
        for k in range(parts):
            cols = pl.ds(k * (D // parts), D // parts)
            swaps[j].append(
                wire.send(aout.at[j, :, cols], actv.at[j, mine, cols], me.partner(), out_act)
            )

    def prepare(j):
        loads[j].wait()
        swaps[j][0].wait_recv()
        swaps[j][1].wait_recv()

    sent = {}

    def z_part(dest, half):
        columns = rows_at(dest * 256 + half * 128, 128)
        return jnp.dot(cott[0], actv[0, :, columns], preferred_element_type=f32)

    def z_send(half, d, n, k):
        part = z_part(wrap(z + d * (n + 1 - k), 8), half)
        slot = Z_BASE[half, d] + k - 1
        if k > 1:
            sent["z", half, d, k - 1].wait_recv()
            part += zr[slot - 1].astype(f32)
        zs[slot] = part.astype(bf16)
        sent["z", half, d, k] = wire.send(zs.at[slot], zr.at[slot], me.at(dz=d), out_z)

    def x_part(dest, half, i):
        columns = rows_at((4 * half + i) * 256, 256)
        return jnp.dot(cott[1, rows_at(dest * 128, 128), :], actv[1, :, columns], preferred_element_type=f32)

    def x_send(half, d, k):
        dest = wrap(x + d * (PAIR_STEPS[half, d] + 1 - k), 4)
        slot = PAIR_BASE[half, d] + k - 1
        if k > 1:
            sent["x", half, d, k - 1].wait_recv()

        def step(i, carry):
            part = x_part(dest, half, i)
            for t in range(2):
                value = part[:, t * 128 : (t + 1) * 128]
                if k > 1:
                    value += xr[slot - 1, 2 * i + t].astype(f32)
                xs[slot, 2 * i + t] = value.astype(bf16)
            return carry

        lax.fori_loop(0, 4, step, 0, unroll=True)
        sent["x", half, d, k] = wire.send(xs.at[slot], xr.at[slot], me.at(dx=d), out_x)

    def y_part(dest, half, i):
        columns = rows_at(((4 * half + i) * 2 + lax.rem(dest, 2)) * 128, 128)
        rows = rows_at(lax.div(dest, 2) * 256, 256)
        return jnp.dot(cott[2, rows, :], actv[2, :, columns], preferred_element_type=f32)

    def y_send(half, d, k):
        dest = wrap(y + d * (PAIR_STEPS[half, d] + 1 - k), 4)
        slot = PAIR_BASE[half, d] + k - 1
        if k > 1:
            sent["y", half, d, k - 1].wait_recv()

        def step(i, carry):
            value = y_part(dest, half, i)
            if k > 1:
                value += yr[slot - 1, i].astype(f32)
            ys[slot, i] = value.astype(bf16)
            return carry

        lax.fori_loop(0, 4, step, 0, unroll=True)
        sent["y", half, d, k] = wire.send(ys.at[slot], yr.at[slot], me.at_y(d), out_y)

    def z_round(k, long=None):
        for (half, d), n in Z_STEPS.items():
            if k <= n and long in (None, n == 4):
                z_send(half, d, n, k)

    phase("r_prep0")
    prepare(1)
    phase("r_x1")
    x_send(0, 1, 1)
    swaps[1][2].wait_recv()
    x_send(1, -1, 1)
    phase("r_y1")
    prepare(2)
    y_send(0, 1, 1)
    swaps[2][2].wait_recv()
    y_send(1, -1, 1)
    phase("r_z1")
    prepare(0)
    z_round(1)
    phase("r_xy1b")
    x_send(1, 1, 1)
    x_send(0, -1, 1)
    y_send(1, 1, 1)
    y_send(0, -1, 1)
    here = rows_at(me.column * 128, 128)

    def slot_matrix(p):
        found, seen, filled = jnp.int32(0), jnp.int32(0), jnp.int32(0)
        for m in range(MATS):
            named = (owners[m] == p).astype(jnp.int32)
            take = named * (seen == c).astype(jnp.int32)
            found, filled, seen = found + take * m, filled + take, seen + named
        return found, filled

    def note(p, carry):
        table[0, p], table[1, p] = slot_matrix(p)
        return carry

    def gather_columns(pieces, target):
        def choose(p, carry):
            found, filled = table[0, p], table[1, p]
            target[p] = (pieces[found].astype(f32) * filled.astype(f32)).astype(bf16)
            return carry

        lax.fori_loop(0, 16, choose, 0, unroll=2)

    phase("r_msend")
    load_momentum.wait()
    load_owners.wait()
    load_starts.wait()
    lax.fori_loop(0, 16, note, 0)
    gather_columns(mb, ms)
    own_half = rows_at(yh * 32, 32)
    mq[own_half, here] = ms[me.column]

    phase("r_z2")
    z_round(2, True)
    phase("r_x2")
    x_send(0, 1, 2)
    x_send(1, -1, 2)
    phase("r_y2")
    y_send(0, 1, 2)
    y_send(1, -1, 2)
    phase("r_z2b")
    z_round(2, False)
    phase("r_z3")
    z_round(3, True)
    z_round(3, False)
    phase("r_z4")
    z_round(4)
    copies = [(ms.at[p], mq.at[own_half, here], device) for device, p in me.columns()]
    momentum_to_owner = wire.group(copies, ms.at[:15])

    phase("r_xlast")
    def turned_z(to):
        return wrap(to - z - 2, 8)

    def third(second, buffer, arrived, here, store):
        for e in range(4 * second, 4 * second + 4):
            value = here(e).astype(f32)
            for d in range(3):
                value += arrived[second, d, e % 4].astype(f32)
            buffer[e] = value.astype(bf16)
        places = (2, 1, 3, 0) if second == 0 else (4, 7, 5)
        copies = [(buffer.at[e], store.at[e], me.at(dz=e + 2)) for e in places]
        return wire.group(copies, store.at[: len(places)])

    for half in range(2):
        sent["x", half, 1, PAIR_STEPS[half, 1]].wait_recv()
        sent["x", half, -1, PAIR_STEPS[half, -1]].wait_recv()
        up = PAIR_BASE[half, 1] + PAIR_STEPS[half, 1] - 1
        down = PAIR_BASE[half, -1] + PAIR_STEPS[half, -1] - 1

        def x_last(i, carry, half=half, up=up, down=down):
            part = x_part(x, half, i)
            for t in range(2):
                value = part[:, t * 128 : (t + 1) * 128]
                value += xr[up, 2 * i + t].astype(f32) + xr[down, 2 * i + t].astype(f32)
                x2s[t, turned_z(4 * half + i)] = value.astype(bf16)
            return carry

        lax.fori_loop(0, 4, x_last, 0, unroll=True)
    for second in range(2):
        copies = []
        for d in (2, 1, 3):
            to = wrap(y + d, 4)
            source = x2s.at[lax.rem(to, 2), pl.ds(4 * second, 4), rows_at(lax.div(to, 2) * 64, 64), :]
            copies.append((source, x2r.at[second, d - 1], me.at_y(d)))
        sent["x2", second] = wire.group(copies, x2r.at[second])

    phase("r_ylast")
    for half in range(2):
        sent["y", half, 1, PAIR_STEPS[half, 1]].wait_recv()
        sent["y", half, -1, PAIR_STEPS[half, -1]].wait_recv()
        up = PAIR_BASE[half, 1] + PAIR_STEPS[half, 1] - 1
        down = PAIR_BASE[half, -1] + PAIR_STEPS[half, -1] - 1

        def y_last(i, carry, half=half, up=up, down=down):
            value = y_part(y, half, i) + yr[up, i].astype(f32) + yr[down, i].astype(f32)
            y2s[turned_z(4 * half + i)] = value.astype(bf16)
            return carry

        lax.fori_loop(0, 4, y_last, 0, unroll=True)
    for second in range(2):
        copies = []
        for d in (2, 1, 3):
            source = y2s.at[pl.ds(4 * second, 4), rows_at(wrap(x + d, 4) * 64, 64), :]
            copies.append((source, y2r.at[second, d - 1], me.at(dx=d)))
        sent["y2", second] = wire.group(copies, y2r.at[second])

    phase("r_zlast")
    for half in range(2):
        last = []
        for d in (1, -1):
            n = Z_STEPS[half, d]
            sent["z", half, d, n].wait_recv()
            last.append(Z_BASE[half, d] + n - 1)
        value = z_part(z, half) + zr[last[0]].astype(f32) + zr[last[1]].astype(f32)
        z2s[half] = value.astype(bf16).reshape(4, 2, 64, 128)
    copies = []
    for d in (1, 3, 2):
        to = wrap(y + d, 4)
        copies.append((z2s.at[lax.rem(to, 2), :, lax.div(to, 2)], z2r.at[d - 1], me.at_y(d)))
    sent["z2"] = wire.group(copies, z2r)
    def z_second():
        phase("r_z3b")
        sent["z2"].wait_recv()
        for to in range(4):
            value = z2s[yl, to, yh].astype(f32)
            for d in range(3):
                value += z2r[d, to].astype(f32)
            z3s[to] = value.astype(bf16)
        copies = [(z3s.at[wrap(x + d, 4)], z3r.at[d - 1], me.at(dx=d)) for d in (2, 1, 3)]
        sent["z3"] = wire.group(copies, z3r)

    def x_here(e):
        return x2s[yl, e, rows_at(yh * 64, 64), :]

    def y_here(e):
        return y2s[e, rows_at(x * 64, 64), :]

    for second in range(2):
        phase("r_x3" + "ab"[second])
        sent["x2", second].wait_recv()
        sent["x3", second] = third(second, x3s, x2r, x_here, x3r)
        phase("r_y3" + "ab"[second])
        sent["y2", second].wait_recv()
        sent["y3", second] = third(second, y3s, y2r, y_here, y3r)
    z_second()
    momentum_to_owner.wait_recv()
    momentum_over = wire.send(mq.at[own_half], mq.at[own_half], me.near(0, 2, 0, 0))

    phase("r_xfin")
    inverse = 1.0 / math.sqrt(TOKENS)
    sqs[z] = jnp.zeros((8, 128), f32)

    def piece(j, value):
        value = value * inverse
        for kv in range(2):
            block = value[kv * 32 : (kv + 1) * 32]
            gb[6 * c + 2 * j + kv, rows, :] = block.astype(bf16)
            gp[6 * c + 2 * j + kv] = block.astype(bf16)
            total = jnp.sum(block * block, axis=(0, 1), keepdims=True)
            sqs[z, 2 * j + kv : 2 * j + kv + 1, :] = jnp.broadcast_to(total, (1, 128))

    sent["x3", 0].wait_recv()
    sent["x3", 1].wait_recv()
    value = x3s[6].astype(f32)
    for e in (0, 1, 2, 3, 4, 5, 7):
        value += x3r[e].astype(f32)
    piece(1, value)
    phase("r_yfin")
    sent["y3", 0].wait_recv()
    sent["y3", 1].wait_recv()
    value = y3s[6].astype(f32)
    for e in (0, 1, 2, 3, 4, 5, 7):
        value += y3r[e].astype(f32)
    piece(2, value)
    phase("r_zfin")
    sent["z3"].wait_recv()
    value = z3s[x].astype(f32)
    for d in range(3):
        value += z3r[d].astype(f32)
    piece(0, value)

    phase("r_sqsend")
    own = pl.ds(6 * c, 6)
    squares = wire.group([(sqs.at[z], sqs.at[z], me.at(dz=d)) for d in (4, 3, 5, 2, 6, 1, 7)], sqs.at[:7])
    swap = wire.send(gp.at[own], gp.at[own], me.partner())
    swap.wait_recv()
    gather_columns(gp, us)
    gq[own_half, here] = us[me.column]
    copies = []
    for dz in (4, 3, 5, 2, 6, 1, 7, 0):
        for dy in (2, 1, 3, 0):
            if dz or dy:
                device = me.near(0, dy, 0, dz)
                copies.append((us.at[2 * device[3] + device[4]], gq.at[own_half, here], device))
    to_owner = wire.group(copies, rb.at[:31])
    phase("r_sqw1b")
    squares.wait_recv()
    spot = c * 16 + 4 * x + y
    farthest = sorted(plane, key=lambda d: -min(d[0], 4 - d[0]) - min(d[1], 4 - d[1]))
    sq2[spot] = sum((sqs[i] for i in range(1, 8)), sqs[0])
    squares = wire.group(
        [(sq2.at[spot], sq2.at[spot], me.near(dx, dy, dc, 0)) for dx, dy, dc in farthest], sq2.at[:31]
    )
    phase("r_sqw2")
    squares.wait_recv()
    totals = [sum((sq2[k * 16 + i] for i in range(1, 16)), sq2[k * 16]) for k in range(2)]
    totals = jnp.concatenate(totals, axis=0)
    phase("o_a2a")
    momentum_over.wait_recv()
    to_owner.wait_recv()
    phase("o_choose")

    row = lax.broadcasted_iota(jnp.int32, (16, 128), 0)
    matrix = jnp.where(row >= 8, row - 2, row)
    held = (row < 6) | ((row >= 8) & (row < 14))
    bucket = (matrix >= starts[0]).astype(jnp.int32) + (matrix >= starts[1]).astype(jnp.int32)
    factors = jnp.ones((16, 128), f32)
    for b in range(3):
        inside = held & (bucket == b)
        total = jnp.sum(jnp.where(inside, totals, 0.0), axis=0, keepdims=True)
        members = jnp.sum(inside.astype(f32), axis=0, keepdims=True)
        root_mean = jnp.sqrt(total / (members * (KV * D)) + epsilon)
        factors = jnp.where(inside, jnp.minimum(1.0, clip_level / root_mean), factors)
    f_out[...] = factors
    fac[...] = factors
    mine_is = table[0, me.column]
    factor = fac[pl.ds(mine_is + 2 * (mine_is >= 6).astype(jnp.int32), 1), :]
    for k in range(4):
        cols = slice(k * 512, (k + 1) * 512)
        scaled = factor[:, :1] * gq[:, cols].astype(f32)
        value = scaled + momentum_rate * (momentum_rate * mq[:, cols].astype(f32) + scaled)
        gin[rows_at(x * 64, 64), cols] = value.astype(bf16)

    phase("o_ag")

    def part(dx, h):
        return gin.at[rows_at(wrap(x + dx, 4) * 64 + 32 * h, 32), :]

    ahead, behind = me.at(dx=1), me.at(dx=-1)
    out_u = wire.outlet(gin.at[:192])
    first_up = wire.send(part(0, 0), part(0, 0), ahead, out_u)
    first_down = wire.send(part(0, 1), part(0, 1), behind, out_u)
    second_up = wire.send(part(0, 1), part(0, 1), ahead, out_u)
    second_down = wire.send(part(0, 0), part(0, 0), behind, out_u)
    first_up.wait_recv()
    third_up = wire.send(part(-1, 0), part(-1, 0), ahead, out_u)
    first_down.wait_recv()
    third_down = wire.send(part(1, 1), part(1, 1), behind, out_u)
    for copy in (second_up, second_down, third_up, third_down):
        copy.wait_recv()
    pieces = wire.group(
        [(gb.at[own, rows, :], gb.at[own, rows, :], device) for device in me.replicas()], gb.at[:6, :224, :]
    )

    phase("o_ns")
    orthogonalize(gin, xw, gram)

    phase("o_back")
    copies = [
        (xw.at[rows, rows_at(p * 128, 128)], rb.at[c * 16 + me.column], device) for device, p in me.columns()
    ]
    back = wire.group(copies, rb.at[:15])
    rb[c * 16 + me.column] = xw[rows, here]
    pieces.wait_recv()
    over_g = wire.send(gb.at[own], gb.at[own], me.partner())
    whole = wire.send(xw, o_out.at[c], me.partner())
    store = pltpu.make_async_copy(xw, o_out.at[c], local_sems.at[7])
    store.start()
    back.wait_recv()
    phase("o_over")
    slots = pl.ds(c * 16, 16)
    over = wire.send(rb.at[slots], rb.at[slots], me.partner())
    over.wait_recv()
    for k in range(6):
        m = 6 * c + k
        owner = owners[m]
        slot = jnp.int32(0)
        for j in range(MATS):
            slot = slot + (owners[j] == owner).astype(jnp.int32) * (j < m).astype(jnp.int32)
        ob[m, rows, :] = rb[jnp.minimum(slot, 1) * 16 + owner]
    phase("o_ag2")
    out_pieces = wire.outlet(ob.at[:6, :224])
    gathered = [wire.send(ob.at[own, rows, :], ob.at[own, rows, :], device, out_pieces) for device in me.replicas()]
    onward = wire.opened(ob.at[:6])
    wire.join(onward, [(ob.at[own, rows, :], ob.at[own, rows, :], me.partner())])
    over_g.wait_recv()
    store_g = pltpu.make_async_copy(gb, g_out, local_sems.at[8])
    store_g.start()
    for copy, (dx, dyh) in zip(gathered, me.offsets(), strict=True):
        copy.wait_recv()
        block = 2 * wrap(x - dx, 4) + lax.rem(yh + dyh, 2)
        arrived = ob.at[own, rows_at(block * 32, 32), :]
        wire.join(onward, [(arrived, arrived, me.partner())])
    phase("o_over2")
    onward.wait_recv()
    out = pltpu.make_async_copy(ob, upd_out, local_sems.at[9])
    out.start()
    phase("o_finish")
    whole.wait_recv()
    store.wait()
    store_g.wait()
    out.wait()
    wire.finish()
    phase.end()


def orthogonalize(xin, xw, gram):
    def outer(value):
        return lax.dot_general(value, value, (((1,), (1,)), ((), ())), preferred_element_type=f32)

    def iteration(x_of, last):
        rounded = gram[...].astype(bf16)
        square = jnp.dot(rounded, rounded, preferred_element_type=f32)
        mixing = (coef_b * rounded.astype(f32) + coef_c * square).astype(bf16)
        total = None
        for k in range(4):
            cols = slice(k * 512, (k + 1) * 512)
            old = x_of(cols)
            product = jnp.dot(mixing, old, preferred_element_type=f32)
            new = (coef_a * old.astype(f32) + product).astype(bf16)
            xw[:, cols] = new
            if not last:
                total = outer(new) if k == 0 else total + outer(new)
        if not last:
            gram[...] = total

    first = outer(xin[...])
    diagonal = lax.broadcasted_iota(jnp.int32, (KV, KV), 0) == lax.broadcasted_iota(jnp.int32, (KV, KV), 1)
    norm = jnp.sqrt(jnp.sum(jnp.where(diagonal, first, 0.0), axis=(0, 1), keepdims=True))
    scale = 1.0 / (norm + epsilon)
    gram[...] = first * scale * scale
    iteration(lambda cols: (xin[:, cols].astype(f32) * scale).astype(bf16), False)

    def middle(i, carry):
        iteration(lambda cols: xw[:, cols], False)
        return carry

    lax.fori_loop(0, ITERS - 2, middle, 0)
    iteration(lambda cols: xw[:, cols], True)


def stepped(activations, cotangents, momentum, owners, bucket_starts):
    vm = pltpu.VMEM
    operands = (owners, bucket_starts, activations, cotangents, momentum)
    operands = [pltpu.with_memory_space_constraint(a, pltpu.HBM) for a in operands]
    return pl.pallas_call(
        step_kernel,
        out_shape=(
            jax.ShapeDtypeStruct((MATS, KV, 128), bf16),
            jax.ShapeDtypeStruct((16, 128), f32),
            jax.ShapeDtypeStruct((MATS, KV, 128), bf16),
            jax.ShapeDtypeStruct((2, KV, D), bf16),
        ),
        in_specs=[pl.BlockSpec(memory_space=pltpu.HBM)] * 5,
        out_specs=(
            pl.BlockSpec(memory_space=pl.ANY),
            pl.BlockSpec(memory_space=pltpu.VMEM),
            pl.BlockSpec(memory_space=pl.ANY),
            pl.BlockSpec(memory_space=pl.ANY),
        ),
        scratch_shapes=[
            vm((6, 128, 512), bf16), vm((3, 512, 128), bf16), vm((3, 128, D), bf16), vm((3, 256, D), bf16), vm((3, 512, 256), bf16),
            vm((14, 512, 128), bf16), vm((14, 512, 128), bf16),
            vm((6, 8, 128, 128), bf16), vm((6, 8, 128, 128), bf16),
            vm((6, 4, 256, 128), bf16), vm((6, 4, 256, 128), bf16),
            vm((2, 4, 2, 64, 128), bf16), vm((3, 4, 64, 128), bf16), vm((4, 64, 128), bf16), vm((3, 64, 128), bf16),
            vm((2, 8, 128, 128), bf16), vm((2, 3, 4, 64, 128), bf16), vm((8, 64, 128), bf16), vm((8, 64, 128), bf16),
            vm((8, 256, 128), bf16), vm((2, 3, 4, 64, 128), bf16), vm((8, 64, 128), bf16), vm((8, 64, 128), bf16),
            vm((MATS, KV, 128), bf16), vm((MATS, 32, 128), bf16), vm((8, 8, 128), f32), vm((32, 8, 128), f32),
            vm((MATS, 32, 128), f32), vm((16, 32, 128), bf16), vm((16, 32, 128), bf16), vm((16, 128), f32),
            vm((64, D), bf16), vm((64, D), bf16), vm((KV, D), bf16), vm((KV, D), bf16), vm((32, 32, 128), bf16), vm((MATS, KV, 128), bf16),
            vm((KV, KV), f32),
            pltpu.SMEM((MATS,), jnp.int32), pltpu.SMEM((2,), jnp.int32), pltpu.SMEM((2, 16), jnp.int32),
            pltpu.SemaphoreType.DMA((13,)),
            pltpu.SemaphoreType.DMA((OUTLETS,)),
            pltpu.SemaphoreType.DMA((ARRIVALS,)),
        ],
        compiler_params=pltpu.CompilerParams(
            collective_id=0, has_side_effects=True, vmem_limit_bytes=48 * 1024 * 1024
        ),
        name="step",
    )(*operands)


def finish_kernel(factors, g, mom, x, whole, mom_out, update, owned, mv, uv, ov, sems):
    scale = math.sqrt(max(KV, D))
    copies = []

    def store(source, target):
        copy = pltpu.make_async_copy(source, target, sems.at[len(copies)])
        copy.start()
        copies.append(copy)

    for i in range(4):
        rows, mats = pl.ds(64 * i, 64), pl.ds(3 * i, 3)
        ov[:, rows] = (scale * whole[:, rows].astype(f32)).astype(bf16)
        store(ov.at[:, rows], owned.at[:, rows])
        for m in range(3 * i, 3 * i + 3):
            r = m if m < 6 else m + 2
            mv[m] = momentum_rate * mom[m] + factors[r : r + 1, :] * g[m].astype(f32)
        store(mv.at[mats], mom_out.at[mats])
        uv[mats] = scale * x[mats].astype(f32)
        store(uv.at[mats], update.at[mats])
    for copy in copies:
        copy.wait()


def finished(factors, g, mom, x, whole):
    return pl.pallas_call(
        finish_kernel,
        out_shape=(
            jax.ShapeDtypeStruct((MATS, KV, 128), f32),
            jax.ShapeDtypeStruct((MATS, KV, 128), f32),
            jax.ShapeDtypeStruct((2, KV, D), bf16),
        ),
        in_specs=[pl.BlockSpec(memory_space=pltpu.VMEM)] * 5,
        out_specs=[pl.BlockSpec(memory_space=pltpu.HBM)] * 3,
        scratch_shapes=[
            pltpu.VMEM((MATS, KV, 128), f32),
            pltpu.VMEM((MATS, KV, 128), f32),
            pltpu.VMEM((2, KV, D), bf16),
            pltpu.SemaphoreType.DMA((12,)),
        ],
        compiler_params=pltpu.CompilerParams(vmem_limit_bytes=16 * 1024 * 1024),
        name="finish",
    )(factors, g, mom, x, whole)


def per_device(activations, cotangents, momentum, owners, bucket_starts):
    g, factors, x, whole = stepped(activations, cotangents, momentum, owners, bucket_starts)
    return finished(factors, g, momentum, x, whole)


def solution(mesh):
    torus = Mesh(
        mesh.devices.reshape(4, 2, 2, 8, 2), ("rep_0", "rep_1", "rep_2", "shard_0", "shard_1")
    )
    return jax.shard_map(
        per_device,
        mesh=torus,
        in_specs=(
            P(None, REP_SHARD, None),
            P(None, REP_SHARD, None),
            P(None, None, SHARD),
            P(),
            P(),
        ),
        out_specs=(P(None, None, SHARD), P(None, None, SHARD), P(SHARD, None, None)),
        check_vma=False,
    )
```
